128 devices in a mesh: rep: 16 (over x_hi, z, core), tp: 8 (over x_lo, y).
Axes of the slice: x: 4 (x_hi: 2, x_lo: 2; x = x_hi * 2 + x_lo), y: 4, z: 4, core: 2. Of those that a mesh axis runs over, the one named last changes fastest.
Arguments:
- hidden: bfloat16 [64, 4608], P('rep'), may hold values from -6 to 6
- positions: int32 [64], P('rep'), may hold values from 1 to 1023
- key_cache: bfloat16 [64, 16, 1024, 128], P('rep', 'tp'), may hold values from -6 to 6
- value_cache: bfloat16 [64, 16, 1024, 128], P('rep', 'tp'), may hold values from -6 to 6
- norm_gain: float32 [4608], replicated, may hold values from 0.1 to 1.9
- q_proj: bfloat16 [4096, 4608], P(('rep', 'tp')), may hold values from -0.09375 to 0.09375
- k_proj: bfloat16 [2048, 4608], P(('rep', 'tp')), may hold values from -0.09375 to 0.09375
- v_proj: bfloat16 [2048, 4608], P(('rep', 'tp')), may hold values from -0.09375 to 0.09375
- o_proj: bfloat16 [4608, 4096], P(('rep', 'tp')), may hold values from -0.09375 to 0.09375
- post_gain: float32 [4608], P('tp'), may hold values from 0.1 to 1.9
Outputs:
- joined_qkv: bfloat16 [4608, 8192], P(None, 'tp')
- wo_heads: bfloat16 [4096, 4608], P('tp')
- attn_out: bfloat16 [64, 4608], P('rep', 'tp')
The draws below stay inside these ranges and needn't reach their ends.
All inputs are finite; a program needn't handle non-finite values.
Results may differ from the reference program's by a relative error of at most 0.008.
Values may be sent and summed in bfloat16 or wider, within the bound.
A program may use at most 128 MiB of HBM per device.

```python
import jax
import jax.numpy as jnp
from jax import lax

D = 4608
HEADS = 32
KV_HEADS = 16
HEAD_DIM = 128
CTX = 1024
BATCH = 64
QKV_COLS = 8192
N_TP = 8


def touch_ends(entries, own_key, smallest, high):
    index_at = [jax.random.randint(jax.random.fold_in(own_key, axis), (), 0, length) for axis, length in enumerate(entries.shape)]
    main_axis = entries.shape.index(max(entries.shape))
    next_to = index_at[:main_axis] + [(index_at[main_axis] + 1) % entries.shape[main_axis]] + index_at[main_axis + 1:]
    return entries.at[tuple(index_at)].set(smallest).at[tuple(next_to)].set(high)


def block_scale(key, dims, pieces, low, high):
    def one(position, parts):
        draws = jax.random.uniform(jax.random.fold_in(jax.random.fold_in(key, 6), position), (parts,), jnp.float32, low / len(pieces), high / len(pieces))
        return jnp.repeat(jnp.exp(draws), dims[position] // parts).reshape((-1,) + (1,) * (len(dims) - position - 1))

    loudness = one(*pieces[0])
    for cut in pieces[1:]:
        loudness = loudness * one(*cut)
    return loudness


def normal_values(key, shape, deviation, limit, cuts=(), kind=jnp.bfloat16):
    entries = deviation * jax.random.normal(key, shape, jnp.float32)
    if cuts:
        entries = entries * block_scale(key, shape, cuts, -0.22, 0.18)
    return jnp.clip(entries, -limit, limit).astype(kind)


def setup_inputs(seed: int = 0) -> dict:
    arg_keys = jax.random.split(jax.random.key(seed), 11)
    return {
        "hidden": normal_values(arg_keys[0], (BATCH, D), 1.0, 6.0, ((0, 16),)),
        "positions": touch_ends(jax.random.randint(arg_keys[1], (BATCH,), 1, CTX), jax.random.fold_in(arg_keys[1], 1), 1, CTX - 1).astype(jnp.int32),
        "key_cache": normal_values(arg_keys[2], (BATCH, KV_HEADS, CTX, HEAD_DIM), 1.0, 6.0, ((0, 16), (1, 8))),
        "value_cache": normal_values(arg_keys[3], (BATCH, KV_HEADS, CTX, HEAD_DIM), 1.0, 6.0, ((0, 16), (1, 8))),
        "norm_gain": jnp.clip(1.0 + 0.18 * jax.random.normal(arg_keys[4], (D,), jnp.float32), 0.1, 1.9),
        "q_proj": normal_values(arg_keys[5], (HEADS * HEAD_DIM, D), D ** -0.5, 0.09375, ((0, 128),)),
        "k_proj": normal_values(arg_keys[6], (KV_HEADS * HEAD_DIM, D), D ** -0.5, 0.09375, ((0, 128),)),
        "v_proj": normal_values(arg_keys[7], (KV_HEADS * HEAD_DIM, D), D ** -0.5, 0.09375, ((0, 128),)),
        "o_proj": normal_values(arg_keys[8], (D, HEADS * HEAD_DIM), (HEADS * HEAD_DIM) ** -0.5, 0.09375, ((0, 128),)),
        "post_gain": jnp.clip(1.0 + 0.18 * jax.random.normal(arg_keys[9], (D,), jnp.float32), 0.1, 1.9),
    }


score_scale = 144.0 ** (-0.5)
soft_cap = 50.0

def rms_scale(values, gain):
    mean_square = lax.optimization_barrier(jnp.mean(values * values, axis=-1, keepdims=True))
    return values * lax.rsqrt(mean_square + 1e-06) * gain

def rotate(values, positions):
    half = values.shape[-1] // 2
    freq = 10000.0 ** (-2.0 * jnp.arange(half, dtype=jnp.float32) / values.shape[-1])
    angle = positions.astype(jnp.float32)[:, None] * freq[None, :]
    cosine = jnp.cos(angle)[:, None, :]
    sine = jnp.sin(angle)[:, None, :]
    first = values[..., :half]
    second = values[..., half:]
    return jnp.concatenate([first * cosine - second * sine, second * cosine + first * sine], axis=-1)

def reference(hidden, positions, key_cache, value_cache, norm_gain, q_proj, k_proj, v_proj, o_proj, post_gain):
    q_cols = jnp.transpose(q_proj).reshape(D, N_TP, -1)
    k_cols = jnp.transpose(k_proj).reshape(D, N_TP, -1)
    v_cols = jnp.transpose(v_proj).reshape(D, N_TP, -1)
    joined_qkv = jnp.concatenate([q_cols, k_cols, v_cols], axis=2).reshape(D, QKV_COLS)
    wo_heads = jnp.transpose(o_proj)
    normed = rms_scale(hidden.astype(jnp.float32), norm_gain).astype(jnp.bfloat16)
    query = jnp.dot(normed, jnp.transpose(q_proj), preferred_element_type=jnp.float32).reshape(BATCH, HEADS, HEAD_DIM)
    keys_new = jnp.dot(normed, jnp.transpose(k_proj), preferred_element_type=jnp.float32).reshape(BATCH, KV_HEADS, HEAD_DIM)
    values_new = jnp.dot(normed, jnp.transpose(v_proj), preferred_element_type=jnp.float32).reshape(BATCH, KV_HEADS, HEAD_DIM)
    query_rot = rotate(query, positions).astype(jnp.bfloat16)
    rotated_keys = rotate(keys_new, positions).astype(jnp.bfloat16)
    values_rot = values_new.astype(jnp.bfloat16)
    group = HEADS // KV_HEADS
    grouped_heads = query_rot.astype(jnp.float32).reshape(BATCH, KV_HEADS, group, HEAD_DIM)
    scores = jnp.einsum('bkgd,bkld->bkgl', grouped_heads, key_cache.astype(jnp.float32)) * score_scale
    capped = soft_cap * jnp.tanh(scores / soft_cap)
    valid = jnp.arange(CTX, dtype=jnp.int32)[None, :] < positions[:, None]
    weight_raw = jnp.where(valid[:, None, None, :], jnp.exp(capped), 0.0)
    self_score = lax.optimization_barrier(jnp.sum(grouped_heads * rotated_keys.astype(jnp.float32)[:, :, None, :], axis=-1)) * score_scale
    self_raw = jnp.exp(soft_cap * jnp.tanh(self_score / soft_cap))
    denom = lax.optimization_barrier(jnp.sum(weight_raw, axis=-1)) + self_raw
    weights = (weight_raw / denom[..., None]).astype(jnp.bfloat16)
    self_weight = (self_raw / denom).astype(jnp.bfloat16)
    attention = jnp.einsum('bkgl,bkld->bkgd', weights.astype(jnp.float32), value_cache.astype(jnp.float32))
    attention = attention + self_weight.astype(jnp.float32)[..., None] * values_rot.astype(jnp.float32)[:, :, None, :]
    attention = attention.reshape(BATCH, HEADS * HEAD_DIM).astype(jnp.bfloat16)
    projected = jnp.dot(attention, wo_heads, preferred_element_type=jnp.float32)
    attn_out = rms_scale(projected, post_gain).astype(jnp.bfloat16)
    return (joined_qkv, wo_heads, attn_out)
```

```python
import jax
import jax.numpy as jnp
from jax import lax
from jax.experimental import pallas as pl
from jax.experimental.pallas import tpu as pltpu
from jax.sharding import PartitionSpec as P

score_scale = 144.0 ** (-0.5)
soft_cap = 50.0


MESH = pl.DeviceIdType.MESH


def gather_kernel(q_ref, k_ref, v_ref, o_ref, outq_ref, outo_ref, s1q, s1o, so, gq, go,
                  s1_send, s1_recv, z_send, z_recv, x_send, x_recv, d_send, d_recv, out_sem):
    rep = lax.axis_index("rep")
    tp = lax.axis_index("tp")
    h = rep // 8
    z = (rep // 2) % 4
    core = rep % 2
    g = 2 * h + core
    gpar = 2 * (1 - h) + core
    zp = (z + 1) % 4
    zm = (z + 3) % 4
    zo = (z + 2) % 4
    gathered = (gq, go)
    halves = (gq.shape[2] // 2, go.shape[2] // 2)
    outs = (outq_ref, outo_ref)
    piece_z = (z, zm, zp, zo)
    piece_g = (g, gpar)

    def remote(src, dst, ssem, rsem, device):
        return pltpu.make_async_remote_copy(
            src_ref=src, dst_ref=dst, send_sem=ssem, recv_sem=rsem, device_id=device,
            device_id_type=MESH)

    def exchange(src, dst, dest_rep, dest_tp, ssem, rsem):
        own = jnp.logical_and(dest_rep == rep, dest_tp == tp)

        @pl.when(own)
        def _():
            pltpu.make_async_copy(src, dst, rsem).start()

        @pl.when(jnp.logical_not(own))
        def _():
            remote(src, dst, ssem, rsem, (dest_rep, dest_tp)).start()

    def exchange_done(src, dst, dest_rep, dest_tp, ssem, rsem):
        own = jnp.logical_and(dest_rep == rep, dest_tp == tp)

        @pl.when(jnp.logical_not(own))
        def _():
            remote(src, dst, ssem, rsem, (dest_rep, dest_tp)).wait_send()

    block = rep // 2
    kk = rep % 2
    width = s1q.shape[1]
    qrows, krows = q_ref.shape[0], k_ref.shape[0]
    sends = []
    for zd in range(4):
        cols = pl.ds(zd * width, width)
        sends.append((q_ref.at[:, cols], s1q.at[pl.ds(pl.multiple_of(tp * qrows, qrows), qrows)],
                      2 * zd + kk, block, s1_send.at[3 * zd], s1_recv.at[0]))
        row = pl.multiple_of(kk * 128 + tp * krows, krows)
        sends.append((k_ref.at[:, cols], s1q.at[pl.ds(row, krows)],
                      8 + 2 * zd, block, s1_send.at[3 * zd + 1], s1_recv.at[0]))
        sends.append((v_ref.at[:, cols], s1q.at[pl.ds(row, krows)],
                      9 + 2 * zd, block, s1_send.at[3 * zd + 2], s1_recv.at[0]))
    zdest = rep // 4
    slot = (rep % 4) * 8 + tp
    for p in range(8):
        for gd in range(4):
            sends.append((o_ref.at[:, pl.ds(p * 512 + gd * 128, 128)], s1o.at[slot],
                          (gd // 2) * 8 + zdest * 2 + gd % 2, p,
                          s1_send.at[12 + 4 * p + gd], s1_recv.at[1]))
    for item in sends:
        exchange(*item)

    def chunk(a, zs, gs, half):
        return gathered[a].at[zs, gs, pl.ds(half * halves[a], halves[a])]

    def out_slice(a, zs, gs, half):
        if a == 0:
            rows = pl.ds(pl.multiple_of(zs * 1152 + half * 576, 576), 576)
            return outs[a].at[rows, pl.ds(pl.multiple_of(gs * 256, 256), 256)]
        rows = pl.ds(pl.multiple_of(gs * 128 + half * 64, 64), 64)
        return outs[a].at[rows, pl.ds(pl.multiple_of(zs * 1152, 1152), 1152)]

    def write_out(a, zs, gs, half):
        pltpu.make_async_copy(chunk(a, zs, gs, half), out_slice(a, zs, gs, half), out_sem.at[a]).start()

    def d2d(a, xp, s):
        c = chunk(a, piece_z[s // 2], piece_g[xp], s % 2)
        i = (a * 2 + xp) * 8 + s
        return remote(c, c, d_send.at[i], d_recv.at[i], (rep + 1 - 2 * core, tp))

    def arrived(a, xp, s):
        d2d(a, xp, s).start()
        write_out(a, piece_z[s // 2], piece_g[xp], s % 2)

    def d2d_arrived(a, xp, s):
        d2d(a, xp, s).wait_recv()
        write_out(a, piece_z[s // 2], piece_g[xp] + 1 - 2 * core, s % 2)

    up = (h * 8 + zp * 2 + core, tp)
    down = (h * 8 + zm * 2 + core, tp)

    def zcopy(a, xp, i):
        zs, half, to = ((z, 0, up), (z, 1, up), (z, 0, down), (z, 1, down), (zm, 0, up), (zp, 1, down))[i]
        c = chunk(a, zs, piece_g[xp], half)
        j = (a * 2 + xp) * 6 + i
        return remote(c, c, z_send.at[j], z_recv.at[j], to)

    def xcopy(a, half):
        c = chunk(a, z, g, half)
        return remote(c, c, x_send.at[2 * a + half], x_recv.at[2 * a + half],
                      ((1 - h) * 8 + z * 2 + core, tp))

    def launch(a, xp):
        for i in (0, 3, 1, 2):
            zcopy(a, xp, i).start()
        arrived(a, xp, 0)
        arrived(a, xp, 1)

    def relay(a, xp):
        zcopy(a, xp, 0).wait_recv()
        zcopy(a, xp, 4).start()
        arrived(a, xp, 2)
        zcopy(a, xp, 3).wait_recv()
        zcopy(a, xp, 5).start()
        arrived(a, xp, 5)
        zcopy(a, xp, 1).wait_recv()
        arrived(a, xp, 3)
        zcopy(a, xp, 2).wait_recv()
        arrived(a, xp, 4)

    def finish(a, xp):
        zcopy(a, xp, 4).wait_recv()
        arrived(a, xp, 6)
        zcopy(a, xp, 5).wait_recv()
        arrived(a, xp, 7)

    pltpu.make_async_copy(s1q, s1q, s1_recv.at[0]).wait()
    for b in range(9):
        for c in range(2):
            tile = s1q[c * 128:(c + 1) * 128, b * 128:(b + 1) * 128].astype(jnp.float32)
            gq[z, g, b * 128:(b + 1) * 128, c * 128:(c + 1) * 128] = tile.T.astype(jnp.bfloat16)
    xcopy(0, 0).start()
    xcopy(0, 1).start()
    launch(0, 0)
    pltpu.make_async_copy(s1o, s1o, s1_recv.at[1]).wait()
    nrow = s1o.shape[1]
    for i in range(32):
        so[i * nrow:(i + 1) * nrow, :] = s1o[i].astype(jnp.float32)
    for b in range(9):
        go[z, g, :, b * 128:(b + 1) * 128] = so[b * 128:(b + 1) * 128, :].T.astype(jnp.bfloat16)
    xcopy(1, 0).start()
    xcopy(1, 1).start()
    launch(1, 0)
    relay(0, 0)
    relay(1, 0)
    xcopy(0, 0).wait_recv()
    xcopy(0, 1).wait_recv()
    launch(0, 1)
    for s in range(6):
        d2d_arrived(0, 0, s)
    finish(0, 0)
    for s in range(6):
        d2d_arrived(1, 0, s)
    finish(1, 0)
    xcopy(1, 0).wait_recv()
    xcopy(1, 1).wait_recv()
    launch(1, 1)
    for a in range(2):
        d2d_arrived(a, 0, 6)
        d2d_arrived(a, 0, 7)
        d2d_arrived(a, 1, 0)
        d2d_arrived(a, 1, 1)
    relay(0, 1)
    relay(1, 1)
    for s in range(2, 6):
        d2d_arrived(0, 1, s)
    finish(0, 1)
    for s in range(2, 6):
        d2d_arrived(1, 1, s)
    finish(1, 1)
    for a in range(2):
        d2d_arrived(a, 1, 6)
        d2d_arrived(a, 1, 7)
    for item in sends:
        exchange_done(*item)
    for a in range(2):
        xcopy(a, 0).wait_send()
        xcopy(a, 1).wait_send()
        for xp in range(2):
            for i in range(6):
                zcopy(a, xp, i).wait_send()
            for s in range(8):
                d2d(a, xp, s).wait_send()
        pltpu.make_async_copy(outs[a], outs[a], out_sem.at[a]).wait()


def gather_blocks(q, k, v, o):
    bf = jnp.bfloat16
    dma = pltpu.SemaphoreType.DMA
    return pl.pallas_call(
        gather_kernel,
        out_shape=(jax.ShapeDtypeStruct((4608, 1024), bf), jax.ShapeDtypeStruct((512, 4608), bf)),
        in_specs=[pl.BlockSpec(memory_space=pl.ANY)] * 4,
        out_specs=[pl.BlockSpec(memory_space=pl.ANY)] * 2,
        scratch_shapes=[
            pltpu.VMEM((256, 1152), bf),
            pltpu.VMEM((32, 36, 128), bf),
            pltpu.VMEM((1152, 128), jnp.float32),
            pltpu.VMEM((4, 4, 1152, 256), bf),
            pltpu.VMEM((4, 4, 128, 1152), bf),
            dma((44,)), dma((2,)), dma((24,)), dma((24,)), dma((4,)), dma((4,)),
            dma((32,)), dma((32,)), dma((2,)),
        ],
        compiler_params=pltpu.CompilerParams(
            has_side_effects=True, vmem_limit_bytes=48 * 1024 * 1024),
        name="gather_blocks",
    )(q, k, v, o)


def sent_to_all(shard, axis):
    size = lax.axis_size(axis)
    return lax.all_to_all(
        jnp.broadcast_to(shard[None], (size, *shard.shape)), axis, 0, 0, tiled=True
    )


def over_copies(shard, axis):
    return sent_to_all(shard, axis).sum(axis=0)


def rms_scale(values, gain):
    mean_square = jnp.mean(values * values, axis=-1, keepdims=True)
    return values * lax.rsqrt(mean_square + 1e-06) * gain


def rotate(values, positions):
    half = values.shape[-1] // 2
    freq = 10000.0 ** (-2.0 * jnp.arange(half, dtype=jnp.float32) / values.shape[-1])
    angle = positions.astype(jnp.float32)[:, None] * freq[None, :]
    cosine = jnp.cos(angle)[:, None, :]
    sine = jnp.sin(angle)[:, None, :]
    first = values[..., :half]
    second = values[..., half:]
    return jnp.concatenate(
        [first * cosine - second * sine, second * cosine + first * sine], axis=-1
    )


def body(
    hidden, positions, key_cache, value_cache, norm_gain, q_proj, k_proj, v_proj, o_proj, post_gain
):
    joined_block, out_block = gather_blocks(q_proj, k_proj, v_proj, o_proj)
    batch, kv_local, length, head_dim = key_cache.shape
    q_width = out_block.shape[0]
    kv_width = (joined_block.shape[1] - q_width) // 2
    q_local = q_width // head_dim
    group = q_local // kv_local
    normed = rms_scale(hidden.astype(jnp.float32), norm_gain).astype(jnp.bfloat16)
    query_key_value_projected = jnp.dot(normed, joined_block, preferred_element_type=jnp.float32)
    query = query_key_value_projected[:, :q_width].reshape(batch, q_local, head_dim)
    keys_new = query_key_value_projected[:, q_width : q_width + kv_width].reshape(
        batch, kv_local, head_dim
    )
    values_new = query_key_value_projected[:, q_width + kv_width :].reshape(
        batch, kv_local, head_dim
    )
    query_rot = rotate(query, positions).astype(jnp.bfloat16)
    rotated_keys = rotate(keys_new, positions).astype(jnp.bfloat16)
    values_rot = values_new.astype(jnp.bfloat16)
    grouped_heads = query_rot.reshape(batch, kv_local, group, head_dim)
    scores = (
        jnp.einsum("bkgd,bkld->bkgl", grouped_heads, key_cache, preferred_element_type=jnp.float32)
        * score_scale
    )
    capped = soft_cap * jnp.tanh(scores / soft_cap)
    valid = jnp.arange(length, dtype=jnp.int32)[None, :] < positions[:, None]
    weight_raw = jnp.where(valid[:, None, None, :], jnp.exp(capped), 0.0)
    self_score = (
        jnp.einsum("juzy,juy->juz", grouped_heads, rotated_keys, preferred_element_type=jnp.float32)
        * score_scale
    )
    self_raw = jnp.exp(soft_cap * jnp.tanh(self_score / soft_cap))
    denom = jnp.sum(weight_raw, axis=-1) + self_raw
    weights = (weight_raw / denom[..., None]).astype(jnp.bfloat16)
    self_weight = (self_raw / denom).astype(jnp.bfloat16)
    attention = jnp.einsum(
        "bkgl,bkld->bkgd", weights, value_cache, preferred_element_type=jnp.float32
    )
    attention = (
        attention
        + self_weight.astype(jnp.float32)[..., None] * values_rot.astype(jnp.float32)[:, :, None, :]
    )
    attention = attention.reshape(batch, q_width).astype(jnp.bfloat16)
    partial_out = jnp.dot(attention, out_block, preferred_element_type=jnp.float32)
    width_local = post_gain.shape[0]
    total = over_copies(partial_out, "tp")
    multiplier = lax.rsqrt(jnp.mean(total * total, axis=1) + 1e-06)
    share = lax.dynamic_slice_in_dim(total, lax.axis_index("tp") * width_local, width_local, 1)
    result = share * multiplier[:, None] * post_gain
    return (joined_block, out_block, result.astype(jnp.bfloat16))


def solution(mesh):
    in_specs = (
        P("rep", None),
        P("rep"),
        P("rep", "tp", None, None),
        P("rep", "tp", None, None),
        P(),
        P(("rep", "tp"), None),
        P(("rep", "tp"), None),
        P(("rep", "tp"), None),
        P(("rep", "tp"), None),
        P("tp"),
    )
    out_specs = (P(None, "tp"), P("tp", None), P("rep", "tp"))
    return jax.shard_map(body, mesh=mesh, in_specs=in_specs, out_specs=out_specs, check_vma=False)
```

```python
import jax
import jax.numpy as jnp
import numpy as np
from jax import lax
from jax.experimental import pallas as pl
from jax.experimental.pallas import tpu as pltpu
from jax.sharding import PartitionSpec as P

score_scale = 144.0 ** (-0.5)
soft_cap = 50.0
MESH = pl.DeviceIdType.MESH


def remote(src, dst, ssem, rsem, device):
    return pltpu.make_async_remote_copy(
        src_ref=src, dst_ref=dst, send_sem=ssem, recv_sem=rsem, device_id=device,
        device_id_type=MESH)


def gather_kernel(q_ref, k_ref, v_ref, o_ref, gq, go, s1a, s1q, s1o, so,
                  a_send, a_recv, b_send, q_recv, o_send, o_recv, z_send, z_recv, x_send, x_recv,
                  d_send, d_recv):
    rep = lax.axis_index("rep")
    tp = lax.axis_index("tp")
    h = rep // 8
    z = (rep // 2) % 4
    core = rep % 2
    lo = tp // 4
    g = 2 * h + core
    gpar = 2 * (1 - h) + core
    zp = (z + 1) % 4
    zm = (z + 3) % 4
    zo = (z + 2) % 4
    gathered = (gq, go)
    halves = (gq.shape[2] // 2, go.shape[2] // 2)
    piece_z = (z, zm, zp, zo)
    piece_g = (g, gpar)

    def place(h_, z_, c_):
        return h_ * 8 + z_ * 2 + c_

    width = s1q.shape[1]
    qrows, krows = q_ref.shape[0], k_ref.shape[0]
    parts = ((q_ref, 0, qrows), (k_ref, qrows, krows), (v_ref, qrows + krows, krows))

    def along_z(dist, part):
        zd = (z + dist) % 4
        ref, row, rows = parts[part]
        src = ref.at[:, pl.ds(pl.multiple_of(zd * width, width), width)]
        dst = s1a.at[z, pl.ds(row, rows)]
        if dist == 0:
            return pltpu.make_async_copy(src, dst, a_recv.at[0])
        return remote(src, dst, a_send.at[3 * dist + part], a_recv.at[dist], (place(h, zd, core), tp))

    for dist in (2, 1, 3, 0):
        for part in range(3):
            along_z(dist, part).start()

    zdest = rep // 4
    slot = (rep % 4) * 8 + tp

    def o_slice(p, gd):
        src = o_ref.at[:, pl.ds(p * 512 + gd * 128, 128)]
        return src, s1o.at[slot], place(gd // 2, zdest, gd % 2), p, o_send.at[4 * p + gd], o_recv

    def exchange(src, dst, dest_rep, dest_tp, ssem, rsem):
        own = jnp.logical_and(dest_rep == rep, dest_tp == tp)

        @pl.when(own)
        def _():
            pltpu.make_async_copy(src, dst, rsem).start()

        @pl.when(jnp.logical_not(own))
        def _():
            remote(src, dst, ssem, rsem, (dest_rep, dest_tp)).start()

    def exchange_done(src, dst, dest_rep, dest_tp, ssem, rsem):
        own = jnp.logical_and(dest_rep == rep, dest_tp == tp)

        @pl.when(jnp.logical_not(own))
        def _():
            remote(src, dst, ssem, rsem, (dest_rep, dest_tp)).wait_send()

    for p in range(8):
        for gd in range(4):
            exchange(*o_slice(p, gd))

    def to_owner(dist, part):
        zs = (z + dist) % 4
        _, row, rows = parts[part]
        src = s1a.at[zs, pl.ds(row, rows)]
        if part == 0:
            dest, first = place(0, z, core), tp * rows
        else:
            dest, first = place(1, z, part - 1), core * 128 + tp * rows
        dst = s1q.at[pl.ds(pl.multiple_of(first, rows), rows)]
        return src, dst, dest, h * 4 + zs, b_send.at[3 * dist + part], q_recv

    for dist in (0, 1, 3, 2):
        came = s1a.at[(z + dist) % 4]
        pltpu.make_async_copy(came, came, a_recv.at[(4 - dist) % 4]).wait()
        for part in range(3):
            exchange(*to_owner(dist, part))

    def chunk(a, zs, gs, half):
        return gathered[a].at[zs, gs, pl.ds(half * halves[a], halves[a])]

    def d2d(a, xp, s):
        c = chunk(a, piece_z[s // 2], piece_g[xp], s % 2)
        i = (a * 2 + xp) * 8 + s
        return remote(c, c, d_send.at[i], d_recv.at[i], (place(h, z, 1 - core), tp))

    up = (place(h, zp, core), tp)
    down = (place(h, zm, core), tp)

    def zcopy(a, xp, i):
        zs, half, to = ((z, 0, up), (z, 1, up), (z, 0, down), (z, 1, down), (zm, 0, up), (zp, 1, down))[i]
        c = chunk(a, zs, piece_g[xp], half)
        j = (a * 2 + xp) * 6 + i
        return remote(c, c, z_send.at[j], z_recv.at[j], to)

    def xcopy(a, s):
        c = chunk(a, piece_z[s // 2], g, s % 2)
        return remote(c, c, x_send.at[a * 8 + s], x_recv.at[a * 8 + s], (place(1 - h, z, core), tp))

    def arrived(a, xp, s):
        if a == 1:
            xcopy(1, s).start()
        d2d(a, xp, s).start()

    def launch(a, xp):
        for i in (0, 3, 1, 2):
            zcopy(a, xp, i).start()
        arrived(a, xp, 0)
        arrived(a, xp, 1)

    def relay(a, xp):
        zcopy(a, xp, 0).wait_recv()
        zcopy(a, xp, 4).start()
        arrived(a, xp, 2)
        zcopy(a, xp, 3).wait_recv()
        zcopy(a, xp, 5).start()
        arrived(a, xp, 5)
        zcopy(a, xp, 1).wait_recv()
        arrived(a, xp, 3)
        zcopy(a, xp, 2).wait_recv()
        arrived(a, xp, 4)

    def finish(a, xp):
        zcopy(a, xp, 4).wait_recv()
        arrived(a, xp, 6)
        zcopy(a, xp, 5).wait_recv()
        arrived(a, xp, 7)

    pltpu.make_async_copy(s1o, s1o, o_recv).wait()
    nrow = s1o.shape[1]
    for i in range(32):
        so[i * nrow:(i + 1) * nrow, :] = s1o[i].astype(jnp.float32)
    for b in range(9):
        go[z, g, :, b * 128:(b + 1) * 128] = so[b * 128:(b + 1) * 128, :].T.astype(jnp.bfloat16)
    launch(1, 0)
    pltpu.make_async_copy(s1q, s1q, q_recv).wait()
    for b in range(9):
        for c in range(2):
            tile = s1q[c * 128:(c + 1) * 128, b * 128:(b + 1) * 128].astype(jnp.float32)
            gq[z, g, b * 128:(b + 1) * 128, c * 128:(c + 1) * 128] = tile.T.astype(jnp.bfloat16)
    xcopy(0, 0).start()
    xcopy(0, 1).start()
    launch(0, 0)
    relay(1, 0)
    finish(1, 0)
    relay(0, 0)
    for s in range(2):
        xcopy(0, s).wait_recv()
    launch(0, 1)
    finish(0, 0)
    for s in range(8):
        xcopy(1, s).wait_recv()
        d2d(1, 1, s).start()
    relay(0, 1)
    finish(0, 1)
    for a, xp in ((1, 0), (0, 0), (1, 1), (0, 1)):
        for s in range(8):
            d2d(a, xp, s).wait_recv()
    for part in range(3):
        for dist in (1, 2, 3):
            along_z(dist, part).wait_send()
        for dist in range(4):
            exchange_done(*to_owner(dist, part))
    for p in range(8):
        for gd in range(4):
            exchange_done(*o_slice(p, gd))
    for s in range(2):
        xcopy(0, s).wait_send()
    for s in range(8):
        xcopy(1, s).wait_send()
    for a, xp in ((1, 0), (0, 0), (1, 1), (0, 1)):
        if (a, xp) != (1, 1):
            for i in range(6):
                zcopy(a, xp, i).wait_send()
        for s in range(8):
            d2d(a, xp, s).wait_send()


def gather_blocks(q, k, v, o):
    bf = jnp.bfloat16
    dma = pltpu.SemaphoreType.DMA
    return pl.pallas_call(
        gather_kernel,
        out_shape=(jax.ShapeDtypeStruct((4, 4, 1152, 256), bf),
                   jax.ShapeDtypeStruct((4, 4, 128, 1152), bf)),
        in_specs=[pl.BlockSpec(memory_space=pltpu.HBM)] * 4,
        out_specs=[pl.BlockSpec(memory_space=pltpu.VMEM)] * 2,
        scratch_shapes=[
            pltpu.VMEM((4, 64, 1152), bf),
            pltpu.VMEM((256, 1152), bf),
            pltpu.VMEM((32, 36, 128), bf),
            pltpu.VMEM((1152, 128), jnp.float32),
            dma((12,)), dma((4,)), dma((12,)), dma, dma((32,)), dma,
            dma((24,)), dma((24,)), dma((16,)), dma((16,)), dma((32,)), dma((32,)),
        ],
        compiler_params=pltpu.CompilerParams(
            has_side_effects=True, vmem_limit_bytes=8 * 1024 * 1024),
        name="gather_blocks",
    )(q, k, v, o)


def attend_kernel(pos_ref, gq, go, hidden_ref, gain_ref, freq_ref, kc, vc, joined_ref, wo_ref, part_ref,
                  out_sem):
    copies = []
    for zs in range(4):
        for gs in range(4):
            copies.append((gq.at[zs, gs], joined_ref.at[pl.ds(zs * 1152, 1152), pl.ds(gs * 256, 256)], 0))
            copies.append((go.at[zs, gs], wo_ref.at[pl.ds(gs * 128, 128), pl.ds(zs * 1152, 1152)], 1))
    for src, dst, i in copies:
        pltpu.make_async_copy(src, dst, out_sem.at[i]).start()
    f32, bf = jnp.float32, jnp.bfloat16
    hid = hidden_ref[...].astype(f32)
    mean_square = jnp.mean(hid * hid, axis=-1, keepdims=True)
    normed = (hid * lax.rsqrt(mean_square + 1e-06) * gain_ref[...]).astype(bf)
    proj = []
    for gs in range(4):
        acc = jnp.zeros((4, 256), f32)
        for zs in range(4):
            acc += jnp.dot(normed[:, zs * 1152:(zs + 1) * 1152], gq[zs, gs], preferred_element_type=f32)
        proj += [acc[:, :128], acc[:, 128:]]
    row = lax.broadcasted_iota(jnp.int32, (4, 128), 0)
    posf = jnp.zeros((4, 128), f32)
    for b in range(4):
        posf = jnp.where(row == b, pos_ref[b].astype(f32), posf)
    angle = posf * freq_ref[...]
    lane = lax.broadcasted_iota(jnp.int32, (4, 128), 1)
    cosine = jnp.cos(angle)
    sine = jnp.where(lane < 64, -jnp.sin(angle), jnp.sin(angle))

    def rotate(x):
        swapped = jnp.concatenate([x[:, 64:], x[:, :64]], axis=1)
        return (x * cosine + swapped * sine).astype(bf).astype(f32)

    query = jnp.concatenate([rotate(x) for x in proj[:4]], axis=0)
    keys = [rotate(x) for x in proj[4:6]]
    vals = [x.astype(bf).astype(f32) for x in proj[6:8]]
    keys_new = jnp.concatenate([keys[0], keys[0], keys[1], keys[1]], axis=0)
    values_new = jnp.concatenate([vals[0], vals[0], vals[1], vals[1]], axis=0)
    qb = query.astype(bf)
    length = kc.shape[2]
    r = lax.broadcasted_iota(jnp.int32, (16, length), 0)
    slot = lax.broadcasted_iota(jnp.int32, (16, length), 1)
    owner = (r // 8) * 4 + r % 4
    scores = jnp.zeros((16, length), f32)
    limit = jnp.zeros((16, length), jnp.int32)
    for kv in range(2):
        for b in range(4):
            s = lax.dot_general(qb, kc[b, kv], (((1,), (1,)), ((), ())), preferred_element_type=f32)
            scores = jnp.where(owner == kv * 4 + b, s, scores)
    for b in range(4):
        limit = jnp.where(r % 4 == b, pos_ref[b], limit)
    capped = soft_cap * jnp.tanh(scores * score_scale / soft_cap)
    raw = jnp.where(slot < limit, jnp.exp(capped), 0.0)
    self_score = jnp.sum(query * keys_new, axis=-1, keepdims=True) * score_scale
    self_raw = jnp.exp(soft_cap * jnp.tanh(self_score / soft_cap))
    denom = jnp.sum(raw, axis=-1, keepdims=True) + self_raw
    weights = (raw / denom).astype(bf).astype(f32)
    attention = (self_raw / denom).astype(bf).astype(f32) * values_new
    for kv in range(2):
        for b in range(4):
            w = jnp.where(owner == kv * 4 + b, weights, 0.0).astype(bf)
            attention += jnp.dot(w, vc[b, kv], preferred_element_type=f32)
    att = jnp.concatenate([attention[i * 4:(i + 1) * 4] for i in range(4)], axis=1).astype(bf)
    for zs in range(4):
        part = jnp.dot(att, go[zs].reshape(512, 1152), preferred_element_type=f32)
        part_ref[2 * zs] = part[:, :576]
        part_ref[2 * zs + 1] = part[:, 576:]
    pltpu.make_async_copy(joined_ref, joined_ref, out_sem.at[0]).wait()
    pltpu.make_async_copy(wo_ref, wo_ref, out_sem.at[1]).wait()


def attend(positions, gq, go, hidden, norm_gain, key_cache, value_cache):
    bf = jnp.bfloat16
    vmem = pl.BlockSpec(memory_space=pltpu.VMEM)
    hbm = pl.BlockSpec(memory_space=pltpu.HBM)
    freq = 10000.0 ** (-2.0 * np.arange(64, dtype=np.float64) / 128)
    freq = np.concatenate([freq, freq]).astype(np.float32)[None]
    return pl.pallas_call(
        attend_kernel,
        out_shape=(jax.ShapeDtypeStruct((4608, 1024), bf), jax.ShapeDtypeStruct((512, 4608), bf),
                   jax.ShapeDtypeStruct((8, 4, 576), jnp.float32)),
        in_specs=[pl.BlockSpec(memory_space=pltpu.SMEM)] + [vmem] * 7,
        out_specs=[hbm, hbm, vmem],
        scratch_shapes=[pltpu.SemaphoreType.DMA((2,))],
        compiler_params=pltpu.CompilerParams(vmem_limit_bytes=20 * 1024 * 1024),
        name="attend",
    )(positions, gq, go, hidden, norm_gain.reshape(1, -1), jnp.asarray(freq), key_cache, value_cache)


def norm_kernel(part_ref, gain_ref, out_ref, came, square, squares, p_send, p_recv, s_send, s_recv):
    rep = lax.axis_index("rep")
    tp = lax.axis_index("tp")
    barrier = pltpu.get_barrier_semaphore()
    for d in range(1, 8):
        pl.semaphore_signal(barrier, inc=1, device_id=(rep, (tp + d) % 8), device_id_type=MESH)
    pl.semaphore_wait(barrier, 7)

    def part(d):
        to = (tp + d) % 8
        return remote(part_ref.at[to], came.at[d - 1], p_send.at[d - 1], p_recv.at[d - 1], (rep, to))

    def sq(d):
        return remote(square, squares.at[d - 1], s_send.at[d - 1], s_recv.at[d - 1],
                      (rep, (tp + d) % 8))

    for d in range(1, 8):
        part(d).start()
    total = part_ref[tp]
    for d in range(1, 8):
        part(d).wait_recv()
        total += came[d - 1]
    square[...] = jnp.broadcast_to(jnp.sum(total * total, axis=-1, keepdims=True), square.shape)
    for d in range(1, 8):
        sq(d).start()
    whole = square[...]
    for d in range(1, 8):
        sq(d).wait_recv()
        whole += squares[d - 1]
    scale = lax.rsqrt(whole[:, :1] / 4608.0 + 1e-06)
    out_ref[...] = (total * scale * gain_ref[...]).astype(jnp.bfloat16)
    for d in range(1, 8):
        part(d).wait_send()
        sq(d).wait_send()


def norm_sums(part, post_gain):
    vmem = pl.BlockSpec(memory_space=pltpu.VMEM)
    dma = pltpu.SemaphoreType.DMA
    return pl.pallas_call(
        norm_kernel,
        out_shape=jax.ShapeDtypeStruct((4, 576), jnp.bfloat16),
        in_specs=[vmem, vmem],
        out_specs=vmem,
        scratch_shapes=[pltpu.VMEM((7, 4, 576), jnp.float32), pltpu.VMEM((4, 128), jnp.float32),
                        pltpu.VMEM((7, 4, 128), jnp.float32), dma((7,)), dma((7,)), dma((7,)), dma((7,))],
        compiler_params=pltpu.CompilerParams(has_side_effects=True, collective_id=1),
        name="norm_sums",
    )(part, post_gain.reshape(1, -1))


def body(
    hidden, positions, key_cache, value_cache, norm_gain, q_proj, k_proj, v_proj, o_proj, post_gain
):
    gq, go = gather_blocks(q_proj, k_proj, v_proj, o_proj)
    joined, wo, part = attend(positions, gq, go, hidden, norm_gain, key_cache, value_cache)
    return joined, wo, norm_sums(part, post_gain)


def solution(mesh):
    in_specs = (
        P("rep", None),
        P("rep"),
        P("rep", "tp", None, None),
        P("rep", "tp", None, None),
        P(),
        P(("rep", "tp"), None),
        P(("rep", "tp"), None),
        P(("rep", "tp"), None),
        P(("rep", "tp"), None),
        P("tp"),
    )
    out_specs = (P(None, "tp"), P("tp", None), P("rep", "tp"))
    return jax.shard_map(body, mesh=mesh, in_specs=in_specs, out_specs=out_specs, check_vma=False)
```

```python
import jax
import jax.numpy as jnp
import numpy as np
from jax import lax
from jax.experimental import pallas as pl
from jax.experimental.pallas import tpu as pltpu
from jax.sharding import PartitionSpec as P

score_scale = 144.0 ** (-0.5)
soft_cap = 50.0
MESH = pl.DeviceIdType.MESH


def remote(src, dst, ssem, rsem, device):
    return pltpu.make_async_remote_copy(
        src_ref=src, dst_ref=dst, send_sem=ssem, recv_sem=rsem, device_id=device,
        device_id_type=MESH)


def gather_kernel(q_ref, k_ref, v_ref, o_ref, hidden_ref, gain_ref, kc_ref, vc_ref,
                  gq, go, hidden_out, gain_out, kc_out, vc_out, s1a, s1q, s1o, so,
                  a_send, a_recv, b_send, q_recv, o_send, o_recv, z_send, z_recv, x_send, x_recv,
                  d_send, d_recv, plane_sem, in_sem):
    rep = lax.axis_index("rep")
    tp = lax.axis_index("tp")
    h = rep // 8
    z = (rep // 2) % 4
    core = rep % 2
    lo = tp // 4
    g = 2 * h + core
    gpar = 2 * (1 - h) + core
    rep_in_plane = g
    zp = (z + 1) % 4
    zm = (z + 3) % 4
    zo = (z + 2) % 4
    gathered = (gq, go)
    halves = (gq.shape[2] // 2, go.shape[2] // 2)
    piece_z = (z, zm, zp, zo)
    piece_g = (g, gpar)

    def place(h_, z_, c_):
        return h_ * 8 + z_ * 2 + c_

    width = s1q.shape[1]
    qrows, krows = q_ref.shape[0], k_ref.shape[0]
    parts = ((q_ref, 0, qrows), (k_ref, qrows, krows), (v_ref, qrows + krows, krows))

    def along_z(dist, part):
        zd = (z + dist) % 4
        ref, row, rows = parts[part]
        src = ref.at[:, pl.ds(pl.multiple_of(zd * width, width), width)]
        dst = s1a.at[z, pl.ds(row, rows)]
        if dist == 0:
            return pltpu.make_async_copy(src, dst, a_recv.at[0])
        return remote(src, dst, a_send.at[3 * dist + part], a_recv.at[dist], (place(h, zd, core), tp))

    for dist in (2, 1, 3, 0):
        for part in range(3):
            along_z(dist, part).start()

    local = [pltpu.make_async_copy(src, dst, in_sem.at[i]) for i, (src, dst) in enumerate(
        ((hidden_ref, hidden_out), (gain_ref, gain_out), (kc_ref, kc_out), (vc_ref, vc_out)))]
    for copy in local:
        copy.start()

    zdest = rep // 4
    slot = (rep % 4) * 8 + tp

    def o_slice(p, gd):
        src = o_ref.at[:, pl.ds(p * 512 + gd * 128, 128)]
        return src, s1o.at[slot], place(gd // 2, zdest, gd % 2), p, o_send.at[4 * p + gd], o_recv

    def exchange(src, dst, dest_rep, dest_tp, ssem, rsem):
        own = jnp.logical_and(dest_rep == rep, dest_tp == tp)

        @pl.when(own)
        def _():
            pltpu.make_async_copy(src, dst, rsem).start()

        @pl.when(jnp.logical_not(own))
        def _():
            remote(src, dst, ssem, rsem, (dest_rep, dest_tp)).start()

    def exchange_done(src, dst, dest_rep, dest_tp, ssem, rsem):
        own = jnp.logical_and(dest_rep == rep, dest_tp == tp)

        @pl.when(jnp.logical_not(own))
        def _():
            remote(src, dst, ssem, rsem, (dest_rep, dest_tp)).wait_send()

    for p in range(8):
        for gd in range(4):
            exchange(*o_slice(p, gd))

    def to_owner(dist, part):
        zs = (z + dist) % 4
        _, row, rows = parts[part]
        src = s1a.at[zs, pl.ds(row, rows)]
        if part == 0:
            dest, first = place(0, z, core), tp * rows
        else:
            dest, first = place(1, z, part - 1), core * 128 + tp * rows
        dst = s1q.at[pl.ds(pl.multiple_of(first, rows), rows)]
        return src, dst, dest, h * 4 + zs, b_send.at[3 * dist + part], q_recv

    for dist in (0, 1, 3, 2):
        came = s1a.at[(z + dist) % 4]
        pltpu.make_async_copy(came, came, a_recv.at[(4 - dist) % 4]).wait()
        for part in range(3):
            exchange(*to_owner(dist, part))

    def chunk(a, zs, gs, half):
        return gathered[a].at[zs, gs, pl.ds(half * halves[a], halves[a])]

    def d2d(a, xp, s):
        c = chunk(a, piece_z[s // 2], piece_g[xp], s % 2)
        i = (a * 2 + xp) * 8 + s
        return remote(c, c, d_send.at[i], d_recv.at[i], (place(h, z, 1 - core), tp))

    up = (place(h, zp, core), tp)
    down = (place(h, zm, core), tp)

    def zcopy(a, xp, i):
        zs, half, to = ((z, 0, up), (z, 1, up), (z, 0, down), (z, 1, down), (zm, 0, up), (zp, 1, down))[i]
        c = chunk(a, zs, piece_g[xp], half)
        j = (a * 2 + xp) * 6 + i
        return remote(c, c, z_send.at[j], z_recv.at[j], to)

    def xcopy(a, s):
        c = chunk(a, piece_z[s // 2], g, s % 2)
        return remote(c, c, x_send.at[a * 8 + s], x_recv.at[a * 8 + s], (place(1 - h, z, core), tp))

    def arrived(a, xp, s):
        d2d(a, xp, s).start()

    def launch(a, xp):
        for i in (0, 3, 1, 2):
            zcopy(a, xp, i).start()
        arrived(a, xp, 0)
        arrived(a, xp, 1)

    def relay(a, xp):
        zcopy(a, xp, 0).wait_recv()
        zcopy(a, xp, 4).start()
        arrived(a, xp, 2)
        zcopy(a, xp, 3).wait_recv()
        zcopy(a, xp, 5).start()
        arrived(a, xp, 5)
        zcopy(a, xp, 1).wait_recv()
        arrived(a, xp, 3)
        zcopy(a, xp, 2).wait_recv()
        arrived(a, xp, 4)

    def finish(a, xp):
        zcopy(a, xp, 4).wait_recv()
        arrived(a, xp, 6)
        zcopy(a, xp, 5).wait_recv()
        arrived(a, xp, 7)

    pltpu.make_async_copy(s1o, s1o, o_recv).wait()
    nrow = s1o.shape[1]
    for i in range(32):
        so[i * nrow:(i + 1) * nrow, :] = s1o[i].astype(jnp.float32)
    for b in range(9):
        go[z, g, :, b * 128:(b + 1) * 128] = so[b * 128:(b + 1) * 128, :].T.astype(jnp.bfloat16)
    launch(1, 0)
    pltpu.make_async_copy(s1q, s1q, q_recv).wait()
    for i in range(1, 32):
        peer = (rep_in_plane + i // 8) % 4
        pl.semaphore_signal(plane_sem, inc=1, device_id=(place(peer // 2, z, peer % 2), (tp + i) % 8),
                            device_id_type=MESH)
    for b in range(9):
        for c in range(2):
            tile = s1q[c * 128:(c + 1) * 128, b * 128:(b + 1) * 128].astype(jnp.float32)
            gq[z, g, b * 128:(b + 1) * 128, c * 128:(c + 1) * 128] = tile.T.astype(jnp.bfloat16)
    launch(0, 0)
    relay(1, 0)
    pl.semaphore_wait(plane_sem, 31)
    for s in range(2):
        xcopy(0, s).start()
    for s in (0, 1, 2, 5, 3, 4):
        xcopy(1, s).start()
    relay(0, 0)
    for s in range(2):
        xcopy(0, s).wait_recv()
    launch(0, 1)
    finish(1, 0)
    for s in (6, 7):
        xcopy(1, s).start()
    finish(0, 0)
    relay(0, 1)
    for s in (0, 1, 2, 5, 3, 4, 6, 7):
        xcopy(1, s).wait_recv()
        d2d(1, 1, s).start()
    finish(0, 1)
    for a, xp in ((1, 0), (0, 0), (1, 1), (0, 1)):
        for s in range(8):
            d2d(a, xp, s).wait_recv()
    for copy in local:
        copy.wait()
    for part in range(3):
        for dist in (1, 2, 3):
            along_z(dist, part).wait_send()
        for dist in range(4):
            exchange_done(*to_owner(dist, part))
    for p in range(8):
        for gd in range(4):
            exchange_done(*o_slice(p, gd))
    for s in range(2):
        xcopy(0, s).wait_send()
    for s in range(8):
        xcopy(1, s).wait_send()
    for a, xp in ((1, 0), (0, 0), (1, 1), (0, 1)):
        if (a, xp) != (1, 1):
            for i in range(6):
                zcopy(a, xp, i).wait_send()
        for s in range(8):
            d2d(a, xp, s).wait_send()


def in_hbm(x):
    return pltpu.with_memory_space_constraint(x, pltpu.HBM)


def gather_blocks(q, k, v, o, hidden, gain, key_cache, value_cache):
    bf = jnp.bfloat16
    dma = pltpu.SemaphoreType.DMA
    cache = jax.ShapeDtypeStruct(key_cache.shape, bf)
    return pl.pallas_call(
        gather_kernel,
        out_shape=(jax.ShapeDtypeStruct((4, 4, 1152, 256), bf),
                   jax.ShapeDtypeStruct((4, 4, 128, 1152), bf),
                   jax.ShapeDtypeStruct(hidden.shape, bf),
                   jax.ShapeDtypeStruct(gain.shape, jnp.float32), cache, cache),
        in_specs=[pl.BlockSpec(memory_space=pltpu.HBM)] * 8,
        out_specs=[pl.BlockSpec(memory_space=pltpu.VMEM)] * 6,
        scratch_shapes=[
            pltpu.VMEM((4, 64, 1152), bf),
            pltpu.VMEM((256, 1152), bf),
            pltpu.VMEM((32, 36, 128), bf),
            pltpu.VMEM((1152, 128), jnp.float32),
            dma((12,)), dma((4,)), dma((12,)), dma, dma((32,)), dma,
            dma((24,)), dma((24,)), dma((16,)), dma((16,)), dma((32,)), dma((32,)),
            pltpu.SemaphoreType.REGULAR, dma((4,)),
        ],
        compiler_params=pltpu.CompilerParams(
            has_side_effects=True, vmem_limit_bytes=8 * 1024 * 1024),
        name="gather_blocks",
    )(*(in_hbm(x) for x in (q, k, v, o, hidden, gain, key_cache, value_cache)))


def attend_kernel(pos_hbm, gq, go, hidden_ref, gain_ref, kc, vc, joined_ref, wo_ref, part_ref,
                  pos_ref, pos_sem, out_sem):
    pos_copy = pltpu.make_async_copy(pos_hbm, pos_ref, pos_sem)
    pos_copy.start()
    copies = []
    for zs in range(4):
        for gs in range(4):
            copies.append((gq.at[zs, gs], joined_ref.at[pl.ds(zs * 1152, 1152), pl.ds(gs * 256, 256)], 0))
            copies.append((go.at[zs, gs], wo_ref.at[pl.ds(gs * 128, 128), pl.ds(zs * 1152, 1152)], 1))
    for src, dst, i in copies:
        pltpu.make_async_copy(src, dst, out_sem.at[i]).start()
    f32, bf = jnp.float32, jnp.bfloat16
    hid = hidden_ref[...].astype(f32)
    mean_square = jnp.mean(hid * hid, axis=-1, keepdims=True)
    gain = gain_ref[...].reshape(1, -1)
    normed = (hid * lax.rsqrt(mean_square + 1e-06) * gain).astype(bf)
    proj = []
    for gs in range(4):
        acc = jnp.zeros((4, 256), f32)
        for zs in range(4):
            acc += jnp.dot(normed[:, zs * 1152:(zs + 1) * 1152], gq[zs, gs], preferred_element_type=f32)
        proj += [acc[:, :128], acc[:, 128:]]
    pos_copy.wait()
    row = lax.broadcasted_iota(jnp.int32, (4, 128), 0)
    posf = jnp.zeros((4, 128), f32)
    for b in range(4):
        posf = jnp.where(row == b, pos_ref[b].astype(f32), posf)
    lane = lax.broadcasted_iota(jnp.int32, (4, 128), 1)
    angle = posf * jnp.exp((lane % 64).astype(f32) * (-2.0 / 128 * np.log(10000.0)))
    cosine = jnp.cos(angle)
    sine = jnp.where(lane < 64, -jnp.sin(angle), jnp.sin(angle))

    def rotate(x):
        swapped = jnp.concatenate([x[:, 64:], x[:, :64]], axis=1)
        return (x * cosine + swapped * sine).astype(bf).astype(f32)

    query = jnp.concatenate([rotate(x) for x in proj[:4]], axis=0)
    keys = [rotate(x) for x in proj[4:6]]
    vals = [x.astype(bf).astype(f32) for x in proj[6:8]]
    keys_new = jnp.concatenate([keys[0], keys[0], keys[1], keys[1]], axis=0)
    values_new = jnp.concatenate([vals[0], vals[0], vals[1], vals[1]], axis=0)
    qb = query.astype(bf)
    length = kc.shape[2]
    r = lax.broadcasted_iota(jnp.int32, (16, length), 0)
    slot = lax.broadcasted_iota(jnp.int32, (16, length), 1)
    owner = (r // 8) * 4 + r % 4
    scores = jnp.zeros((16, length), f32)
    limit = jnp.zeros((16, length), jnp.int32)
    for kv in range(2):
        for b in range(4):
            s = lax.dot_general(qb, kc[b, kv], (((1,), (1,)), ((), ())), preferred_element_type=f32)
            scores = jnp.where(owner == kv * 4 + b, s, scores)
    for b in range(4):
        limit = jnp.where(r % 4 == b, pos_ref[b], limit)
    capped = soft_cap * jnp.tanh(scores * score_scale / soft_cap)
    raw = jnp.where(slot < limit, jnp.exp(capped), 0.0)
    self_score = jnp.sum(query * keys_new, axis=-1, keepdims=True) * score_scale
    self_raw = jnp.exp(soft_cap * jnp.tanh(self_score / soft_cap))
    denom = jnp.sum(raw, axis=-1, keepdims=True) + self_raw
    weights = (raw / denom).astype(bf).astype(f32)
    attention = (self_raw / denom).astype(bf).astype(f32) * values_new
    for kv in range(2):
        for b in range(4):
            w = jnp.where(owner == kv * 4 + b, weights, 0.0).astype(bf)
            attention += jnp.dot(w, vc[b, kv], preferred_element_type=f32)
    att = jnp.concatenate([attention[i * 4:(i + 1) * 4] for i in range(4)], axis=1).astype(bf)
    for zs in range(4):
        part = jnp.dot(att, go[zs].reshape(512, 1152), preferred_element_type=f32)
        part_ref[2 * zs] = part[:, :576]
        part_ref[2 * zs + 1] = part[:, 576:]
    pltpu.make_async_copy(joined_ref, joined_ref, out_sem.at[0]).wait()
    pltpu.make_async_copy(wo_ref, wo_ref, out_sem.at[1]).wait()


def attend(positions, gathered):
    bf = jnp.bfloat16
    vmem = pl.BlockSpec(memory_space=pltpu.VMEM)
    hbm = pl.BlockSpec(memory_space=pltpu.HBM)
    return pl.pallas_call(
        attend_kernel,
        out_shape=(jax.ShapeDtypeStruct((4608, 1024), bf), jax.ShapeDtypeStruct((512, 4608), bf),
                   jax.ShapeDtypeStruct((8, 4, 576), jnp.float32)),
        in_specs=[hbm] + [vmem] * 6,
        out_specs=[hbm, hbm, vmem],
        scratch_shapes=[pltpu.SMEM((4,), jnp.int32), pltpu.SemaphoreType.DMA,
                        pltpu.SemaphoreType.DMA((2,))],
        compiler_params=pltpu.CompilerParams(vmem_limit_bytes=20 * 1024 * 1024),
        name="attend",
    )(in_hbm(positions), *gathered)


def norm_kernel(part_ref, gain_ref, out_ref, came, square, squares, p_send, p_recv, s_send, s_recv):
    rep = lax.axis_index("rep")
    tp = lax.axis_index("tp")
    barrier = pltpu.get_barrier_semaphore()
    for d in range(1, 8):
        pl.semaphore_signal(barrier, inc=1, device_id=(rep, (tp + d) % 8), device_id_type=MESH)
    pl.semaphore_wait(barrier, 7)

    def part(d):
        to = (tp + d) % 8
        return remote(part_ref.at[to], came.at[d - 1], p_send.at[d - 1], p_recv.at[d - 1], (rep, to))

    def sq(d):
        return remote(square, squares.at[d - 1], s_send.at[d - 1], s_recv.at[d - 1],
                      (rep, (tp + d) % 8))

    for d in range(1, 8):
        part(d).start()
    total = part_ref[tp]
    for d in range(1, 8):
        part(d).wait_recv()
        total += came[d - 1]
    square[...] = jnp.broadcast_to(jnp.sum(total * total, axis=-1, keepdims=True), square.shape)
    for d in range(1, 8):
        sq(d).start()
    whole = square[...]
    for d in range(1, 8):
        sq(d).wait_recv()
        whole += squares[d - 1]
    scale = lax.rsqrt(whole[:, :1] / 4608.0 + 1e-06)
    out_ref[...] = (total * scale * gain_ref[...].reshape(1, -1)).astype(jnp.bfloat16)
    for d in range(1, 8):
        part(d).wait_send()
        sq(d).wait_send()


def norm_sums(part, post_gain):
    vmem = pl.BlockSpec(memory_space=pltpu.VMEM)
    dma = pltpu.SemaphoreType.DMA
    return pl.pallas_call(
        norm_kernel,
        out_shape=jax.ShapeDtypeStruct((4, 576), jnp.bfloat16),
        in_specs=[vmem, vmem],
        out_specs=vmem,
        scratch_shapes=[pltpu.VMEM((7, 4, 576), jnp.float32), pltpu.VMEM((4, 128), jnp.float32),
                        pltpu.VMEM((7, 4, 128), jnp.float32), dma((7,)), dma((7,)), dma((7,)), dma((7,))],
        compiler_params=pltpu.CompilerParams(
            has_side_effects=True, collective_id=1, vmem_limit_bytes=4 * 1024 * 1024),
        name="norm_sums",
    )(part, post_gain)


def body(
    hidden, positions, key_cache, value_cache, norm_gain, q_proj, k_proj, v_proj, o_proj, post_gain
):
    gathered = gather_blocks(q_proj, k_proj, v_proj, o_proj, hidden, norm_gain, key_cache, value_cache)
    joined, wo, part = attend(positions, gathered)
    return joined, wo, norm_sums(part, post_gain)


def solution(mesh):
    in_specs = (
        P("rep", None),
        P("rep"),
        P("rep", "tp", None, None),
        P("rep", "tp", None, None),
        P(),
        P(("rep", "tp"), None),
        P(("rep", "tp"), None),
        P(("rep", "tp"), None),
        P(("rep", "tp"), None),
        P("tp"),
    )
    out_specs = (P(None, "tp"), P("tp", None), P("rep", "tp"))
    return jax.shard_map(body, mesh=mesh, in_specs=in_specs, out_specs=out_specs, check_vma=False)
```

```python
import jax
import jax.numpy as jnp
import numpy as np
from jax import lax
from jax.experimental import pallas as pl
from jax.experimental.pallas import tpu as pltpu
from jax.sharding import PartitionSpec as P

score_scale = 144.0 ** (-0.5)
soft_cap = 50.0
MESH = pl.DeviceIdType.MESH
WO_SLICE = (0, 2, 3, 1)


def remote(src, dst, ssem, rsem, device):
    return pltpu.make_async_remote_copy(
        src_ref=src, dst_ref=dst, send_sem=ssem, recv_sem=rsem, device_id=device,
        device_id_type=MESH)


def gather_kernel(q_ref, k_ref, v_ref, o_ref, hidden_ref, gain_ref, kc_ref, vc_ref,
                  gq, go, hidden_out, gain_out, kc_out, vc_out, s1a, s1q, s1o, so,
                  a_send, a_recv, b_send, q_recv, o_send, o_recv, z_send, z_recv, x_send, x_recv,
                  d_send, d_recv, plane_sem, in_sem):
    rep = lax.axis_index("rep")
    tp = lax.axis_index("tp")
    h = rep // 8
    z = (rep // 2) % 4
    core = rep % 2
    lo = tp // 4
    g = 2 * h + core
    gpar = 2 * (1 - h) + core
    rep_in_plane = g
    zp = (z + 1) % 4
    zm = (z + 3) % 4
    zo = (z + 2) % 4
    gathered = (gq, go)
    halves = (gq.shape[2] // 2, go.shape[2] // 2)
    piece_z = (z, zm, zp, zo)
    piece_g = (g, gpar)

    def place(h_, z_, c_):
        return h_ * 8 + z_ * 2 + c_

    zdest = 2 * h + z // 2
    zdest = jnp.where(zdest == 0, 0, jnp.where(zdest == 1, 3, zdest - 1))
    slot = (rep % 4) * 8 + tp

    def o_slice(i, j):
        p = (tp + i) % 8
        gd = (g + j) % 4
        src = o_ref.at[:, pl.ds(pl.multiple_of(p * 512 + gd * 128, 128), 128)]
        return src, s1o.at[slot], place(gd // 2, zdest, gd % 2), p, o_send.at[4 * i + j], o_recv

    def exchange(src, dst, dest_rep, dest_tp, ssem, rsem):
        own = jnp.logical_and(dest_rep == rep, dest_tp == tp)

        @pl.when(own)
        def _():
            pltpu.make_async_copy(src, dst, rsem).start()

        @pl.when(jnp.logical_not(own))
        def _():
            remote(src, dst, ssem, rsem, (dest_rep, dest_tp)).start()

    def exchange_done(src, dst, dest_rep, dest_tp, ssem, rsem):
        own = jnp.logical_and(dest_rep == rep, dest_tp == tp)

        @pl.when(jnp.logical_not(own))
        def _():
            remote(src, dst, ssem, rsem, (dest_rep, dest_tp)).wait_send()

    for p in range(8):
        for gd in range(4):
            exchange(*o_slice(p, gd))

    width = s1q.shape[1]
    qrows, krows = q_ref.shape[0], k_ref.shape[0]
    parts = ((q_ref, 0, qrows), (k_ref, qrows, krows), (v_ref, qrows + krows, krows))

    first_x = jnp.logical_and(h == 0, lo == 0)
    last_x = jnp.logical_and(h == 1, lo == 1)

    def along_z(dist, part):
        zd = (z + dist) % 4
        ref, row, rows = parts[part]
        src = ref.at[:, pl.ds(pl.multiple_of(zd * width, width), width)]
        if part == 0:
            away, there, to_h, to_tp = last_x, qrows, 0, tp % 4
        else:
            away, there, to_h, to_tp = first_x, row - qrows, 1, 4 + tp % 4
        row = pl.multiple_of(jnp.where(away, there, row), krows)
        dst = s1a.at[z, pl.ds(row, rows)]
        device = (place(jnp.where(away, to_h, h), zd, core), jnp.where(away, to_tp, tp))
        return away, src, dst, remote(src, dst, a_send.at[3 * dist + part], a_recv.at[dist], device)

    for dist in (2, 1, 3, 0):
        for part in range(3):
            away, src, dst, copy = along_z(dist, part)
            if dist == 0:
                pl.when(away)(copy.start)
                pl.when(jnp.logical_not(away))(
                    pltpu.make_async_copy(src, dst, a_recv.at[0]).start)
            else:
                copy.start()

    local = [pltpu.make_async_copy(src, dst, in_sem.at[i]) for i, (src, dst) in enumerate(
        ((hidden_ref, hidden_out), (gain_ref, gain_out), (kc_ref, kc_out), (vc_ref, vc_out)))]
    for copy in local:
        copy.start()

    def to_owners(dist, act):
        zs = (tp + dist) % 4

        def message(when, index, row, rows, dest, first, block):
            dst = s1q.at[pl.ds(pl.multiple_of(first, rows), rows)]

            @pl.when(when)
            def _():
                act(s1a.at[zs, pl.ds(row, rows)], dst, dest, block, b_send.at[4 * dist + index], q_recv)

        y = tp % 4
        message(jnp.logical_not(last_x), 0, 0, qrows, place(0, z, core), tp * qrows, h * 4 + zs)
        message(first_x, 1, qrows, qrows, place(0, z, core), (4 + y) * qrows, 4 + zs)
        for i in range(2):
            message(jnp.logical_not(first_x), 1 + i, qrows + i * krows, krows, place(1, z, i),
                    core * 128 + tp * krows, h * 4 + zs)
            message(last_x, 3 * i, i * krows, krows, place(1, z, i), core * 128 + y * krows, zs)

    for dist in (0, 2, 1, 3):
        zs = (tp + dist) % 4
        came = s1a.at[zs]
        pltpu.make_async_copy(came, came, a_recv.at[(z + 4 - zs) % 4]).wait()
        to_owners(dist, exchange)

    def chunk(a, zs, gs, half):
        return gathered[a].at[zs, gs, pl.ds(half * halves[a], halves[a])]

    def d2d(a, xp, s):
        c = chunk(a, piece_z[s // 2], piece_g[xp], s % 2)
        i = (a * 2 + xp) * 8 + s
        return remote(c, c, d_send.at[i], d_recv.at[i], (place(h, z, 1 - core), tp))

    up = (place(h, zp, core), tp)
    down = (place(h, zm, core), tp)

    def zcopy(a, xp, i):
        zs, half, to = ((z, 0, up), (z, 1, up), (z, 0, down), (z, 1, down), (zm, 0, up), (zp, 1, down))[i]
        c = chunk(a, zs, piece_g[xp], half)
        j = (a * 2 + xp) * 6 + i
        return remote(c, c, z_send.at[j], z_recv.at[j], to)

    def xcopy(a, s):
        c = chunk(a, piece_z[s // 2], g, s % 2)
        return remote(c, c, x_send.at[a * 8 + s], x_recv.at[a * 8 + s], (place(1 - h, z, core), tp))

    def arrived(a, xp, s):
        d2d(a, xp, s).start()

    def launch(a, xp):
        for i in (0, 3, 1, 2):
            zcopy(a, xp, i).start()
        arrived(a, xp, 0)
        arrived(a, xp, 1)

    def relay(a, xp):
        zcopy(a, xp, 0).wait_recv()
        zcopy(a, xp, 4).start()
        arrived(a, xp, 2)
        zcopy(a, xp, 3).wait_recv()
        zcopy(a, xp, 5).start()
        arrived(a, xp, 5)
        zcopy(a, xp, 1).wait_recv()
        arrived(a, xp, 3)
        zcopy(a, xp, 2).wait_recv()
        arrived(a, xp, 4)

    def finish(a, xp):
        zcopy(a, xp, 4).wait_recv()
        arrived(a, xp, 6)
        zcopy(a, xp, 5).wait_recv()
        arrived(a, xp, 7)

    pltpu.make_async_copy(s1o, s1o, o_recv).wait()
    nrow = s1o.shape[1]
    for i in range(32):
        so[i * nrow:(i + 1) * nrow, :] = s1o[i].astype(jnp.float32)
    for b in range(9):
        go[z, g, :, b * 128:(b + 1) * 128] = so[b * 128:(b + 1) * 128, :].T.astype(jnp.bfloat16)
    launch(1, 0)
    pltpu.make_async_copy(s1q, s1q, q_recv).wait()
    for i in range(1, 32):
        peer = (rep_in_plane + i // 8) % 4
        pl.semaphore_signal(plane_sem, inc=1, device_id=(place(peer // 2, z, peer % 2), (tp + i) % 8),
                            device_id_type=MESH)
    for b in range(9):
        for c in range(2):
            tile = s1q[c * 128:(c + 1) * 128, b * 128:(b + 1) * 128].astype(jnp.float32)
            gq[z, g, b * 128:(b + 1) * 128, c * 128:(c + 1) * 128] = tile.T.astype(jnp.bfloat16)
    launch(0, 0)
    relay(1, 0)
    pl.semaphore_wait(plane_sem, 31)
    for s in range(2):
        xcopy(0, s).start()
    for s in (0, 1, 2, 5, 3, 4):
        xcopy(1, s).start()
    relay(0, 0)
    for s in range(2):
        xcopy(0, s).wait_recv()
    launch(0, 1)
    finish(1, 0)
    for s in (6, 7):
        xcopy(1, s).start()
    finish(0, 0)
    relay(0, 1)
    for s in (0, 1, 2, 5, 3, 4, 6, 7):
        xcopy(1, s).wait_recv()
        d2d(1, 1, s).start()
    finish(0, 1)
    for a, xp in ((1, 0), (0, 0), (1, 1), (0, 1)):
        for s in range(8):
            d2d(a, xp, s).wait_recv()
    for copy in local:
        copy.wait()
    for part in range(3):
        for dist in range(4):
            away, _, _, copy = along_z(dist, part)
            if dist == 0:
                pl.when(away)(copy.wait_send)
            else:
                copy.wait_send()
    for dist in range(4):
        to_owners(dist, exchange_done)
    for p in range(8):
        for gd in range(4):
            exchange_done(*o_slice(p, gd))
    for s in range(2):
        xcopy(0, s).wait_send()
    for s in range(8):
        xcopy(1, s).wait_send()
    for a, xp in ((1, 0), (0, 0), (1, 1), (0, 1)):
        if (a, xp) != (1, 1):
            for i in range(6):
                zcopy(a, xp, i).wait_send()
        for s in range(8):
            d2d(a, xp, s).wait_send()


def in_hbm(x):
    return pltpu.with_memory_space_constraint(x, pltpu.HBM)


def gather_blocks(q, k, v, o, hidden, gain, key_cache, value_cache):
    bf = jnp.bfloat16
    dma = pltpu.SemaphoreType.DMA
    cache = jax.ShapeDtypeStruct(key_cache.shape, bf)
    return pl.pallas_call(
        gather_kernel,
        out_shape=(jax.ShapeDtypeStruct((4, 4, 1152, 256), bf),
                   jax.ShapeDtypeStruct((4, 4, 128, 1152), bf),
                   jax.ShapeDtypeStruct(hidden.shape, bf),
                   jax.ShapeDtypeStruct(gain.shape, jnp.float32), cache, cache),
        in_specs=[pl.BlockSpec(memory_space=pltpu.HBM)] * 8,
        out_specs=[pl.BlockSpec(memory_space=pltpu.VMEM)] * 6,
        scratch_shapes=[
            pltpu.VMEM((4, 64, 1152), bf),
            pltpu.VMEM((256, 1152), bf),
            pltpu.VMEM((32, 36, 128), bf),
            pltpu.VMEM((1152, 128), jnp.float32),
            dma((12,)), dma((4,)), dma((16,)), dma, dma((32,)), dma,
            dma((24,)), dma((24,)), dma((16,)), dma((16,)), dma((32,)), dma((32,)),
            pltpu.SemaphoreType.REGULAR, dma((4,)),
        ],
        compiler_params=pltpu.CompilerParams(
            has_side_effects=True, vmem_limit_bytes=8 * 1024 * 1024),
        name="gather_blocks",
    )(*(in_hbm(x) for x in (q, k, v, o, hidden, gain, key_cache, value_cache)))


def attend_kernel(pos_hbm, gq, go, hidden_ref, gain_ref, kc, vc, joined_ref, wo_ref, part_ref,
                  pos_ref, pos_sem, out_sem):
    pos_copy = pltpu.make_async_copy(pos_hbm, pos_ref, pos_sem)
    pos_copy.start()
    copies = []
    for zs in range(4):
        for gs in range(4):
            copies.append((gq.at[zs, gs], joined_ref.at[pl.ds(zs * 1152, 1152), pl.ds(gs * 256, 256)], 0))
            copies.append((go.at[zs, gs], wo_ref.at[pl.ds(gs * 128, 128), pl.ds(WO_SLICE[zs] * 1152, 1152)], 1))
    for src, dst, i in copies:
        pltpu.make_async_copy(src, dst, out_sem.at[i]).start()
    f32, bf = jnp.float32, jnp.bfloat16
    hid = hidden_ref[...].astype(f32)
    mean_square = jnp.mean(hid * hid, axis=-1, keepdims=True)
    gain = gain_ref[...].reshape(1, -1)
    normed = (hid * lax.rsqrt(mean_square + 1e-06) * gain).astype(bf)
    proj = []
    for gs in range(4):
        acc = jnp.zeros((4, 256), f32)
        for zs in range(4):
            acc += jnp.dot(normed[:, zs * 1152:(zs + 1) * 1152], gq[zs, gs], preferred_element_type=f32)
        proj += [acc[:, :128], acc[:, 128:]]
    pos_copy.wait()
    row = lax.broadcasted_iota(jnp.int32, (4, 128), 0)
    posf = jnp.zeros((4, 128), f32)
    for b in range(4):
        posf = jnp.where(row == b, pos_ref[b].astype(f32), posf)
    lane = lax.broadcasted_iota(jnp.int32, (4, 128), 1)
    angle = posf * jnp.exp((lane % 64).astype(f32) * (-2.0 / 128 * np.log(10000.0)))
    cosine = jnp.cos(angle)
    sine = jnp.where(lane < 64, -jnp.sin(angle), jnp.sin(angle))

    def rotate(x):
        swapped = jnp.concatenate([x[:, 64:], x[:, :64]], axis=1)
        return (x * cosine + swapped * sine).astype(bf).astype(f32)

    query = jnp.concatenate([rotate(x) for x in proj[:4]], axis=0)
    keys = [rotate(x) for x in proj[4:6]]
    vals = [x.astype(bf).astype(f32) for x in proj[6:8]]
    keys_new = jnp.concatenate([keys[0], keys[0], keys[1], keys[1]], axis=0)
    values_new = jnp.concatenate([vals[0], vals[0], vals[1], vals[1]], axis=0)
    qb = query.astype(bf)
    length = kc.shape[2]
    r = lax.broadcasted_iota(jnp.int32, (16, length), 0)
    slot = lax.broadcasted_iota(jnp.int32, (16, length), 1)
    owner = (r // 8) * 4 + r % 4
    scores = jnp.zeros((16, length), f32)
    limit = jnp.zeros((16, length), jnp.int32)
    for kv in range(2):
        for b in range(4):
            s = lax.dot_general(qb, kc[b, kv], (((1,), (1,)), ((), ())), preferred_element_type=f32)
            scores = jnp.where(owner == kv * 4 + b, s, scores)
    for b in range(4):
        limit = jnp.where(r % 4 == b, pos_ref[b], limit)
    capped = soft_cap * jnp.tanh(scores * score_scale / soft_cap)
    raw = jnp.where(slot < limit, jnp.exp(capped), 0.0)
    self_score = jnp.sum(query * keys_new, axis=-1, keepdims=True) * score_scale
    self_raw = jnp.exp(soft_cap * jnp.tanh(self_score / soft_cap))
    denom = jnp.sum(raw, axis=-1, keepdims=True) + self_raw
    weights = (raw / denom).astype(bf).astype(f32)
    attention = (self_raw / denom).astype(bf).astype(f32) * values_new
    for kv in range(2):
        for b in range(4):
            w = jnp.where(owner == kv * 4 + b, weights, 0.0).astype(bf)
            attention += jnp.dot(w, vc[b, kv], preferred_element_type=f32)
    att = jnp.concatenate([attention[i * 4:(i + 1) * 4] for i in range(4)], axis=1).astype(bf)
    for zs in range(4):
        part = jnp.dot(att, go[zs].reshape(512, 1152), preferred_element_type=f32)
        part_ref[2 * WO_SLICE[zs]] = part[:, :576]
        part_ref[2 * WO_SLICE[zs] + 1] = part[:, 576:]
    pltpu.make_async_copy(joined_ref, joined_ref, out_sem.at[0]).wait()
    pltpu.make_async_copy(wo_ref, wo_ref, out_sem.at[1]).wait()


def attend(positions, gathered):
    bf = jnp.bfloat16
    vmem = pl.BlockSpec(memory_space=pltpu.VMEM)
    hbm = pl.BlockSpec(memory_space=pltpu.HBM)
    return pl.pallas_call(
        attend_kernel,
        out_shape=(jax.ShapeDtypeStruct((4608, 1024), bf), jax.ShapeDtypeStruct((512, 4608), bf),
                   jax.ShapeDtypeStruct((8, 4, 576), jnp.float32)),
        in_specs=[hbm] + [vmem] * 6,
        out_specs=[hbm, hbm, vmem],
        scratch_shapes=[pltpu.SMEM((4,), jnp.int32), pltpu.SemaphoreType.DMA,
                        pltpu.SemaphoreType.DMA((2,))],
        compiler_params=pltpu.CompilerParams(vmem_limit_bytes=20 * 1024 * 1024),
        name="attend",
    )(in_hbm(positions), *gathered)


def norm_kernel(part_ref, gain_ref, out_ref, came, square, squares, p_send, p_recv, s_send, s_recv):
    rep = lax.axis_index("rep")
    tp = lax.axis_index("tp")
    barrier = pltpu.get_barrier_semaphore()
    for d in range(1, 8):
        pl.semaphore_signal(barrier, inc=1, device_id=(rep, (tp + d) % 8), device_id_type=MESH)
    pl.semaphore_wait(barrier, 7)

    def part(d):
        to = (tp + d) % 8
        return remote(part_ref.at[to], came.at[d - 1], p_send.at[d - 1], p_recv.at[d - 1], (rep, to))

    def sq(d):
        return remote(square, squares.at[d - 1], s_send.at[d - 1], s_recv.at[d - 1],
                      (rep, (tp + d) % 8))

    for d in range(1, 8):
        part(d).start()
    total = part_ref[tp]
    for d in range(1, 8):
        part(d).wait_recv()
        total += came[d - 1]
    square[...] = jnp.broadcast_to(jnp.sum(total * total, axis=-1, keepdims=True), square.shape)
    for d in range(1, 8):
        sq(d).start()
    whole = square[...]
    for d in range(1, 8):
        sq(d).wait_recv()
        whole += squares[d - 1]
    scale = lax.rsqrt(whole[:, :1] / 4608.0 + 1e-06)
    out_ref[...] = (total * scale * gain_ref[...].reshape(1, -1)).astype(jnp.bfloat16)
    for d in range(1, 8):
        part(d).wait_send()
        sq(d).wait_send()


def norm_sums(part, post_gain):
    vmem = pl.BlockSpec(memory_space=pltpu.VMEM)
    dma = pltpu.SemaphoreType.DMA
    return pl.pallas_call(
        norm_kernel,
        out_shape=jax.ShapeDtypeStruct((4, 576), jnp.bfloat16),
        in_specs=[vmem, vmem],
        out_specs=vmem,
        scratch_shapes=[pltpu.VMEM((7, 4, 576), jnp.float32), pltpu.VMEM((4, 128), jnp.float32),
                        pltpu.VMEM((7, 4, 128), jnp.float32), dma((7,)), dma((7,)), dma((7,)), dma((7,))],
        compiler_params=pltpu.CompilerParams(
            has_side_effects=True, collective_id=1, vmem_limit_bytes=4 * 1024 * 1024),
        name="norm_sums",
    )(part, post_gain)


def body(
    hidden, positions, key_cache, value_cache, norm_gain, q_proj, k_proj, v_proj, o_proj, post_gain
):
    gathered = gather_blocks(q_proj, k_proj, v_proj, o_proj, hidden, norm_gain, key_cache, value_cache)
    joined, wo, part = attend(positions, gathered)
    return joined, wo, norm_sums(part, post_gain)


def solution(mesh):
    in_specs = (
        P("rep", None),
        P("rep"),
        P("rep", "tp", None, None),
        P("rep", "tp", None, None),
        P(),
        P(("rep", "tp"), None),
        P(("rep", "tp"), None),
        P(("rep", "tp"), None),
        P(("rep", "tp"), None),
        P("tp"),
    )
    out_specs = (P(None, "tp"), P("tp", None), P("rep", "tp"))
    return jax.shard_map(body, mesh=mesh, in_specs=in_specs, out_specs=out_specs, check_vma=False)
```

```python
import jax
import jax.numpy as jnp
import numpy as np
from jax import lax
from jax.experimental import pallas as pl
from jax.experimental.pallas import tpu as pltpu
from jax.sharding import PartitionSpec as P

score_scale = 144.0 ** (-0.5)
soft_cap = 50.0
MESH = pl.DeviceIdType.MESH
WO_SLICE = (0, 2, 3, 1)


def remote(src, dst, ssem, rsem, device):
    return pltpu.make_async_remote_copy(
        src_ref=src, dst_ref=dst, send_sem=ssem, recv_sem=rsem, device_id=device,
        device_id_type=MESH)


def gather_kernel(q_ref, k_ref, v_ref, o_ref, hidden_hbm, gain_hbm, kc_hbm, vc_hbm, pos_hbm, post_hbm,
                  gq, go, out_ref,
                  hidden_ref, gain_ref, kc, vc, pos_ref, post_ref, nrm, acc, rope, part_ref, parts_in, square,
                  squares, s1a, s1q, s1o, so,
                  a_send, a_recv, b_send, q_recv, o_send, o_recv, z_send, z_recv, x_send, x_recv,
                  d_send, d_recv, plane_sem, in_sem, p_send, p_recv, s_send, s_recv):
    rep = lax.axis_index("rep")
    tp = lax.axis_index("tp")
    h = rep // 8
    z = (rep // 2) % 4
    core = rep % 2
    lo = tp // 4
    g = 2 * h + core
    gpar = 2 * (1 - h) + core
    rep_in_plane = g
    zp = (z + 1) % 4
    zm = (z + 3) % 4
    zo = (z + 2) % 4
    gathered = (gq, go)
    halves = (gq.shape[2] // 2, go.shape[2] // 2)
    piece_z = (z, zm, zp, zo)
    piece_g = (g, gpar)

    def place(h_, z_, c_):
        return h_ * 8 + z_ * 2 + c_

    zdest = 2 * h + z // 2
    zdest = jnp.where(zdest == 0, 0, jnp.where(zdest == 1, 3, zdest - 1))
    slot = (rep % 4) * 8 + tp

    def o_slice(i, j):
        p = (tp + i) % 8
        gd = (g + j) % 4
        src = o_ref.at[:, pl.ds(pl.multiple_of(p * 512 + gd * 128, 128), 128)]
        return src, s1o.at[slot], place(gd // 2, zdest, gd % 2), p, o_send.at[4 * i + j], o_recv

    def exchange(src, dst, dest_rep, dest_tp, ssem, rsem):
        own = jnp.logical_and(dest_rep == rep, dest_tp == tp)

        @pl.when(own)
        def _():
            pltpu.make_async_copy(src, dst, rsem).start()

        @pl.when(jnp.logical_not(own))
        def _():
            remote(src, dst, ssem, rsem, (dest_rep, dest_tp)).start()

    def exchange_done(src, dst, dest_rep, dest_tp, ssem, rsem):
        own = jnp.logical_and(dest_rep == rep, dest_tp == tp)

        @pl.when(jnp.logical_not(own))
        def _():
            remote(src, dst, ssem, rsem, (dest_rep, dest_tp)).wait_send()

    for p in range(8):
        for gd in range(4):
            exchange(*o_slice(p, gd))

    width = s1q.shape[1]
    qrows, krows = q_ref.shape[0], k_ref.shape[0]
    parts = ((q_ref, 0, qrows), (k_ref, qrows, krows), (v_ref, qrows + krows, krows))

    first_x = jnp.logical_and(h == 0, lo == 0)
    last_x = jnp.logical_and(h == 1, lo == 1)

    def along_z(dist, part):
        zd = (z + dist) % 4
        ref, row, rows = parts[part]
        src = ref.at[:, pl.ds(pl.multiple_of(zd * width, width), width)]
        if part == 0:
            away, there, to_h, to_tp = last_x, qrows, 0, tp % 4
        else:
            away, there, to_h, to_tp = first_x, row - qrows, 1, 4 + tp % 4
        row = pl.multiple_of(jnp.where(away, there, row), krows)
        dst = s1a.at[z, pl.ds(row, rows)]
        device = (place(jnp.where(away, to_h, h), zd, core), jnp.where(away, to_tp, tp))
        return away, src, dst, remote(src, dst, a_send.at[3 * dist + part], a_recv.at[dist], device)

    for dist in (2, 1, 3, 0):
        for part in range(3):
            away, src, dst, copy = along_z(dist, part)
            if dist == 0:
                pl.when(away)(copy.start)
                pl.when(jnp.logical_not(away))(
                    pltpu.make_async_copy(src, dst, a_recv.at[0]).start)
            else:
                copy.start()

    local = [pltpu.make_async_copy(src, dst, in_sem.at[i]) for i, (src, dst) in enumerate(
        ((hidden_hbm, hidden_ref), (gain_hbm, gain_ref), (pos_hbm, pos_ref), (post_hbm, post_ref),
         (kc_hbm, kc), (vc_hbm, vc)))]
    for copy in local:
        copy.start()
    for copy in local:
        copy.wait()
    prepare(pos_ref, hidden_ref, gain_ref, nrm, acc, rope)

    def to_owners(dist, act):
        zs = (tp + dist) % 4

        def message(when, index, row, rows, dest, first, block):
            dst = s1q.at[pl.ds(pl.multiple_of(first, rows), rows)]

            @pl.when(when)
            def _():
                act(s1a.at[zs, pl.ds(row, rows)], dst, dest, block, b_send.at[4 * dist + index], q_recv)

        y = tp % 4
        message(jnp.logical_not(last_x), 0, 0, qrows, place(0, z, core), tp * qrows, h * 4 + zs)
        message(first_x, 1, qrows, qrows, place(0, z, core), (4 + y) * qrows, 4 + zs)
        for i in range(2):
            message(jnp.logical_not(first_x), 1 + i, qrows + i * krows, krows, place(1, z, i),
                    core * 128 + tp * krows, h * 4 + zs)
            message(last_x, 3 * i, i * krows, krows, place(1, z, i), core * 128 + y * krows, zs)

    for dist in (0, 2, 1, 3):
        zs = (tp + dist) % 4
        came = s1a.at[zs]
        pltpu.make_async_copy(came, came, a_recv.at[(z + 4 - zs) % 4]).wait()
        to_owners(dist, exchange)

    def chunk(a, zs, gs, half):
        return gathered[a].at[zs, gs, pl.ds(half * halves[a], halves[a])]

    def d2d(a, xp, s):
        c = chunk(a, piece_z[s // 2], piece_g[xp], s % 2)
        i = (a * 2 + xp) * 8 + s
        return remote(c, c, d_send.at[i], d_recv.at[i], (place(h, z, 1 - core), tp))

    up = (place(h, zp, core), tp)
    down = (place(h, zm, core), tp)

    def zcopy(a, xp, i):
        zs, half, to = ((z, 0, up), (z, 1, up), (z, 0, down), (z, 1, down), (zm, 0, up), (zp, 1, down))[i]
        c = chunk(a, zs, piece_g[xp], half)
        j = (a * 2 + xp) * 6 + i
        return remote(c, c, z_send.at[j], z_recv.at[j], to)

    def xcopy(a, s):
        c = chunk(a, piece_z[s // 2], g, s % 2)
        return remote(c, c, x_send.at[a * 8 + s], x_recv.at[a * 8 + s], (place(1 - h, z, core), tp))

    def arrived(a, xp, s):
        d2d(a, xp, s).start()

    def launch(a, xp):
        for i in (0, 3, 1, 2):
            zcopy(a, xp, i).start()
        arrived(a, xp, 0)
        arrived(a, xp, 1)

    def relay(a, xp):
        zcopy(a, xp, 0).wait_recv()
        zcopy(a, xp, 4).start()
        arrived(a, xp, 2)
        zcopy(a, xp, 3).wait_recv()
        zcopy(a, xp, 5).start()
        arrived(a, xp, 5)
        zcopy(a, xp, 1).wait_recv()
        arrived(a, xp, 3)
        zcopy(a, xp, 2).wait_recv()
        arrived(a, xp, 4)

    def finish(a, xp):
        zcopy(a, xp, 4).wait_recv()
        arrived(a, xp, 6)
        zcopy(a, xp, 5).wait_recv()
        arrived(a, xp, 7)

    pltpu.make_async_copy(s1o, s1o, o_recv).wait()
    nrow = s1o.shape[1]
    for i in range(32):
        so[i * nrow:(i + 1) * nrow, :] = s1o[i].astype(jnp.float32)
    for b in range(9):
        go[z, g, :, b * 128:(b + 1) * 128] = so[b * 128:(b + 1) * 128, :].T.astype(jnp.bfloat16)
    launch(1, 0)
    pltpu.make_async_copy(s1q, s1q, q_recv).wait()
    for i in range(1, 32):
        peer = (rep_in_plane + i // 8) % 4
        pl.semaphore_signal(plane_sem, inc=1, device_id=(place(peer // 2, z, peer % 2), (tp + i) % 8),
                            device_id_type=MESH)
    for b in range(9):
        for c in range(2):
            tile = s1q[c * 128:(c + 1) * 128, b * 128:(b + 1) * 128].astype(jnp.float32)
            gq[z, g, b * 128:(b + 1) * 128, c * 128:(c + 1) * 128] = tile.T.astype(jnp.bfloat16)
    launch(0, 0)
    relay(1, 0)
    pl.semaphore_wait(plane_sem, 31)
    for s in range(2):
        xcopy(0, s).start()
    for s in (0, 1, 2, 5, 3, 4):
        xcopy(1, s).start()
    relay(0, 0)
    for s in range(2):
        xcopy(0, s).wait_recv()
    launch(0, 1)
    finish(1, 0)
    for s in (6, 7):
        xcopy(1, s).start()
    finish(0, 0)

    def project(xp, i):
        zs = piece_z[i]
        for s in (2 * i, 2 * i + 1):
            d2d(0, xp, s).wait_recv()
        for gs in (piece_g[xp], piece_g[xp] + 1 - 2 * core):
            acc[gs] += jnp.dot(nrm[zs], gq[zs, gs], preferred_element_type=jnp.float32)

    for i in range(4):
        project(0, i)
    relay(0, 1)
    project(1, 0)
    for s in (0, 1, 2, 5, 3, 4, 6, 7):
        xcopy(1, s).wait_recv()
        d2d(1, 1, s).start()
    finish(0, 1)
    for i in range(1, 4):
        project(1, i)
    att = attention(pos_ref, kc, vc, acc, rope)
    for xp in range(2):
        for s in range(8):
            d2d(1, xp, s).wait_recv()
    for zs in range(4):
        part = jnp.dot(att, go[zs].reshape(512, 1152), preferred_element_type=jnp.float32)
        part_ref[2 * WO_SLICE[zs]] = part[:, :576]
        part_ref[2 * WO_SLICE[zs] + 1] = part[:, 576:]
    sum_and_norm(part_ref, post_ref, out_ref, parts_in, square, squares, p_send, p_recv, s_send, s_recv)
    for part in range(3):
        for dist in range(4):
            away, _, _, copy = along_z(dist, part)
            if dist == 0:
                pl.when(away)(copy.wait_send)
            else:
                copy.wait_send()
    for dist in range(4):
        to_owners(dist, exchange_done)
    for p in range(8):
        for gd in range(4):
            exchange_done(*o_slice(p, gd))
    for s in range(2):
        xcopy(0, s).wait_send()
    for s in range(8):
        xcopy(1, s).wait_send()
    for a, xp in ((1, 0), (0, 0), (1, 1), (0, 1)):
        if (a, xp) != (1, 1):
            for i in range(6):
                zcopy(a, xp, i).wait_send()
        for s in range(8):
            d2d(a, xp, s).wait_send()


def in_hbm(x):
    return pltpu.with_memory_space_constraint(x, pltpu.HBM)


def gather_and_attend(q, k, v, o, hidden, gain, key_cache, value_cache, positions, post_gain):
    bf, f32 = jnp.bfloat16, jnp.float32
    dma = pltpu.SemaphoreType.DMA
    vmem = pltpu.VMEM
    return pl.pallas_call(
        gather_kernel,
        out_shape=(jax.ShapeDtypeStruct((4, 4, 1152, 256), bf),
                   jax.ShapeDtypeStruct((4, 4, 128, 1152), bf),
                   jax.ShapeDtypeStruct((4, 576), bf)),
        in_specs=[pl.BlockSpec(memory_space=pltpu.HBM)] * 10,
        out_specs=[pl.BlockSpec(memory_space=vmem)] * 3,
        scratch_shapes=[
            vmem(hidden.shape, bf), vmem(gain.shape, f32), vmem(key_cache.shape, bf),
            vmem(value_cache.shape, bf), pltpu.SMEM((4,), jnp.int32), vmem(post_gain.shape, f32),
            vmem((4, 4, 1152), bf), vmem((4, 4, 256), f32), vmem((2, 4, 128), f32),
            vmem((8, 4, 576), f32), vmem((7, 4, 576), f32), vmem((4, 128), f32), vmem((7, 4, 128), f32),
            vmem((4, 64, 1152), bf), vmem((256, 1152), bf), vmem((32, 36, 128), bf),
            vmem((1152, 128), f32),
            dma((12,)), dma((4,)), dma((16,)), dma, dma((32,)), dma,
            dma((24,)), dma((24,)), dma((16,)), dma((16,)), dma((32,)), dma((32,)),
            pltpu.SemaphoreType.REGULAR, dma((6,)), dma((7,)), dma((7,)), dma((7,)), dma((7,)),
        ],
        compiler_params=pltpu.CompilerParams(
            has_side_effects=True, vmem_limit_bytes=16 * 1024 * 1024),
        name="gather_and_attend",
    )(*(in_hbm(x) for x in (q, k, v, o, hidden, gain, key_cache, value_cache, positions, post_gain)))


def prepare(pos_ref, hidden_ref, gain_ref, nrm, acc, rope):
    f32 = jnp.float32
    hid = hidden_ref[...].astype(f32)
    mean_square = jnp.mean(hid * hid, axis=-1, keepdims=True)
    gain = gain_ref[...].reshape(1, -1)
    normed = (hid * lax.rsqrt(mean_square + 1e-06) * gain).astype(jnp.bfloat16)
    for zs in range(4):
        nrm[zs] = normed[:, zs * 1152:(zs + 1) * 1152]
    acc[...] = jnp.zeros_like(acc)
    row = lax.broadcasted_iota(jnp.int32, (4, 128), 0)
    posf = jnp.zeros((4, 128), f32)
    for b in range(4):
        posf = jnp.where(row == b, pos_ref[b].astype(f32), posf)
    lane = lax.broadcasted_iota(jnp.int32, (4, 128), 1)
    angle = posf * jnp.exp((lane % 64).astype(f32) * (-2.0 / 128 * np.log(10000.0)))
    rope[0] = jnp.cos(angle)
    rope[1] = jnp.where(lane < 64, -jnp.sin(angle), jnp.sin(angle))


def attention(pos_ref, kc, vc, acc, rope):
    f32, bf = jnp.float32, jnp.bfloat16
    proj = []
    for gs in range(4):
        both = acc[gs]
        proj += [both[:, :128], both[:, 128:]]
    cosine, sine = rope[0], rope[1]

    def rotate(x):
        swapped = jnp.concatenate([x[:, 64:], x[:, :64]], axis=1)
        return (x * cosine + swapped * sine).astype(bf).astype(f32)

    query = jnp.concatenate([rotate(x) for x in proj[:4]], axis=0)
    keys = [rotate(x) for x in proj[4:6]]
    vals = [x.astype(bf).astype(f32) for x in proj[6:8]]
    keys_new = jnp.concatenate([keys[0], keys[0], keys[1], keys[1]], axis=0)
    values_new = jnp.concatenate([vals[0], vals[0], vals[1], vals[1]], axis=0)
    qb = query.astype(bf)
    length = kc.shape[2]
    r = lax.broadcasted_iota(jnp.int32, (16, length), 0)
    slot = lax.broadcasted_iota(jnp.int32, (16, length), 1)
    owner = (r // 8) * 4 + r % 4
    scores = jnp.zeros((16, length), f32)
    limit = jnp.zeros((16, length), jnp.int32)
    for kv in range(2):
        for b in range(4):
            s = lax.dot_general(qb, kc[b, kv], (((1,), (1,)), ((), ())), preferred_element_type=f32)
            scores = jnp.where(owner == kv * 4 + b, s, scores)
    for b in range(4):
        limit = jnp.where(r % 4 == b, pos_ref[b], limit)
    capped = soft_cap * jnp.tanh(scores * score_scale / soft_cap)
    raw = jnp.where(slot < limit, jnp.exp(capped), 0.0)
    self_score = jnp.sum(query * keys_new, axis=-1, keepdims=True) * score_scale
    self_raw = jnp.exp(soft_cap * jnp.tanh(self_score / soft_cap))
    denom = jnp.sum(raw, axis=-1, keepdims=True) + self_raw
    weights = (raw / denom).astype(bf).astype(f32)
    mixed = (self_raw / denom).astype(bf).astype(f32) * values_new
    for kv in range(2):
        for b in range(4):
            w = jnp.where(owner == kv * 4 + b, weights, 0.0).astype(bf)
            mixed += jnp.dot(w, vc[b, kv], preferred_element_type=f32)
    return jnp.concatenate([mixed[i * 4:(i + 1) * 4] for i in range(4)], axis=1).astype(bf)


def write_kernel(gq, go, joined_ref, wo_ref, out_sem):
    for zs in range(4):
        for gs in range(4):
            pltpu.make_async_copy(
                gq.at[zs, gs], joined_ref.at[pl.ds(zs * 1152, 1152), pl.ds(gs * 256, 256)],
                out_sem.at[0]).start()
            pltpu.make_async_copy(
                go.at[zs, gs], wo_ref.at[pl.ds(gs * 128, 128), pl.ds(WO_SLICE[zs] * 1152, 1152)],
                out_sem.at[1]).start()
    pltpu.make_async_copy(joined_ref, joined_ref, out_sem.at[0]).wait()
    pltpu.make_async_copy(wo_ref, wo_ref, out_sem.at[1]).wait()


def write_out(gq, go):
    bf = jnp.bfloat16
    vmem = pl.BlockSpec(memory_space=pltpu.VMEM)
    hbm = pl.BlockSpec(memory_space=pltpu.HBM)
    return pl.pallas_call(
        write_kernel,
        out_shape=(jax.ShapeDtypeStruct((4608, 1024), bf), jax.ShapeDtypeStruct((512, 4608), bf)),
        in_specs=[vmem, vmem],
        out_specs=[hbm, hbm],
        scratch_shapes=[pltpu.SemaphoreType.DMA((2,))],
        compiler_params=pltpu.CompilerParams(vmem_limit_bytes=16 * 1024 * 1024),
        name="write_out",
    )(gq, go)


def sum_and_norm(part_ref, gain_ref, out_ref, parts_in, square, squares, p_send, p_recv, s_send, s_recv):
    rep = lax.axis_index("rep")
    tp = lax.axis_index("tp")

    def part(d):
        to = (tp + d) % 8
        return remote(part_ref.at[to], parts_in.at[d - 1], p_send.at[d - 1], p_recv.at[d - 1], (rep, to))

    def sq(d):
        return remote(square, squares.at[d - 1], s_send.at[d - 1], s_recv.at[d - 1],
                      (rep, (tp + d) % 8))

    for d in range(1, 8):
        part(d).start()
    total = part_ref[tp]
    for d in range(1, 8):
        part(d).wait_recv()
        total += parts_in[d - 1]
    square[...] = jnp.broadcast_to(jnp.sum(total * total, axis=-1, keepdims=True), square.shape)
    for d in range(1, 8):
        sq(d).start()
    whole = square[...]
    for d in range(1, 8):
        sq(d).wait_recv()
        whole += squares[d - 1]
    scale = lax.rsqrt(whole[:, :1] / 4608.0 + 1e-06)
    out_ref[...] = (total * scale * gain_ref[...].reshape(1, -1)).astype(jnp.bfloat16)
    for d in range(1, 8):
        part(d).wait_send()
        sq(d).wait_send()


def body(
    hidden, positions, key_cache, value_cache, norm_gain, q_proj, k_proj, v_proj, o_proj, post_gain
):
    gq, go, attn_out = gather_and_attend(
        q_proj, k_proj, v_proj, o_proj, hidden, norm_gain, key_cache, value_cache, positions, post_gain)
    joined, wo = write_out(gq, go)
    return joined, wo, attn_out


def solution(mesh):
    in_specs = (
        P("rep", None),
        P("rep"),
        P("rep", "tp", None, None),
        P("rep", "tp", None, None),
        P(),
        P(("rep", "tp"), None),
        P(("rep", "tp"), None),
        P(("rep", "tp"), None),
        P(("rep", "tp"), None),
        P("tp"),
    )
    out_specs = (P(None, "tp"), P("tp", None), P("rep", "tp"))
    return jax.shard_map(body, mesh=mesh, in_specs=in_specs, out_specs=out_specs, check_vma=False)
```

```python
import jax
import jax.numpy as jnp
import numpy as np
from jax import lax
from jax.experimental import pallas as pl
from jax.experimental.pallas import tpu as pltpu
from jax.sharding import PartitionSpec as P

score_scale = 144.0 ** (-0.5)
soft_cap = 50.0
MESH = pl.DeviceIdType.MESH
WO_SLICE = (0, 2, 3, 1)


def remote(src, dst, ssem, rsem, device):
    return pltpu.make_async_remote_copy(
        src_ref=src, dst_ref=dst, send_sem=ssem, recv_sem=rsem, device_id=device,
        device_id_type=MESH)


def gather_kernel(q_ref, k_ref, v_ref, o_ref, hidden_hbm, gain_hbm, kc_hbm, vc_hbm, pos_hbm, post_hbm,
                  gq, go, out_ref,
                  hidden_ref, gain_ref, kc, vc, pos_ref, post_ref, nrm, acc, rope, part_ref, parts_in, square,
                  squares, s1a, s1q, s1o, so,
                  a_send, a_recv, b_send, q_recv, o_send, o_recv, z_send, z_recv, x_send, x_recv,
                  d_send, d_recv, row_sem, in_sem, p_send, p_recv, s_send, s_recv):
    rep = lax.axis_index("rep")
    tp = lax.axis_index("tp")
    h = rep // 8
    z = (rep // 2) % 4
    core = rep % 2
    lo = tp // 4
    g = 2 * h + core
    gpar = 2 * (1 - h) + core
    zp = (z + 1) % 4
    zm = (z + 3) % 4
    zo = (z + 2) % 4
    gathered = (gq, go)
    halves = (gq.shape[2] // 2, go.shape[2] // 2)
    piece_z = (z, zm, zp, zo)
    piece_g = (g, gpar)

    def place(h_, z_, c_):
        return h_ * 8 + z_ * 2 + c_

    barrier = pltpu.get_barrier_semaphore()
    pair = z + 1 - 2 * (z % 2)
    greeted = [((z_ + 2) % 4, h_, core, tp_) for z_ in (pair, z)
               for h_, tp_ in ((1 - h, (tp + 4) % 8), (h, tp))]
    greeted += [(z_, (g + a) % 4 // 2, (g + a) % 2, (tp + b) % 8) for z_ in (pair, z)
                for a in (2, 3, 1, 0) for b in (6, 2, 5, 7, 1, 3, 4, 0)][:-1]
    for z_, h_, c_, tp_ in greeted:
        pl.semaphore_signal(barrier, inc=1, device_id=(place(h_, z_, c_), tp_), device_id_type=MESH)
    pl.semaphore_wait(barrier, len(greeted))

    zdest = 2 * h + z // 2
    zdest = jnp.where(zdest == 0, 0, jnp.where(zdest == 1, 3, zdest - 1))
    slot = (rep % 4) * 8 + tp

    def o_slice(i, j):
        p = (tp + i) % 8
        gd = (g + j) % 4
        src = o_ref.at[:, pl.ds(pl.multiple_of(p * 512 + gd * 128, 128), 128)]
        return src, s1o.at[slot], place(gd // 2, zdest, gd % 2), p, o_send.at[4 * i + j], o_recv

    def exchange(src, dst, dest_rep, dest_tp, ssem, rsem):
        own = jnp.logical_and(dest_rep == rep, dest_tp == tp)

        @pl.when(own)
        def _():
            pltpu.make_async_copy(src, dst, rsem).start()

        @pl.when(jnp.logical_not(own))
        def _():
            remote(src, dst, ssem, rsem, (dest_rep, dest_tp)).start()

    def exchange_done(src, dst, dest_rep, dest_tp, ssem, rsem):
        own = jnp.logical_and(dest_rep == rep, dest_tp == tp)

        @pl.when(jnp.logical_not(own))
        def _():
            remote(src, dst, ssem, rsem, (dest_rep, dest_tp)).wait_send()

    for p in range(8):
        for gd in range(4):
            exchange(*o_slice(p, gd))

    width = s1q.shape[1]
    qrows, krows = q_ref.shape[0], k_ref.shape[0]
    parts = ((q_ref, 0, qrows), (k_ref, qrows, krows), (v_ref, qrows + krows, krows))

    first_x = jnp.logical_and(h == 0, lo == 0)
    last_x = jnp.logical_and(h == 1, lo == 1)

    def along_z(dist, part):
        zd = (z + dist) % 4
        ref, row, rows = parts[part]
        src = ref.at[:, pl.ds(pl.multiple_of(zd * width, width), width)]
        if part == 0:
            away, there, to_h, to_tp = last_x, qrows, 0, tp % 4
        else:
            away, there, to_h, to_tp = first_x, row - qrows, 1, 4 + tp % 4
        row = pl.multiple_of(jnp.where(away, there, row), krows)
        dst = s1a.at[z, pl.ds(row, rows)]
        device = (place(jnp.where(away, to_h, h), zd, core), jnp.where(away, to_tp, tp))
        return away, src, dst, remote(src, dst, a_send.at[3 * dist + part], a_recv.at[dist], device)

    for dist in (2, 1, 3, 0):
        for part in range(3):
            away, src, dst, copy = along_z(dist, part)
            if dist == 0:
                pl.when(away)(copy.start)
                pl.when(jnp.logical_not(away))(
                    pltpu.make_async_copy(src, dst, a_recv.at[0]).start)
            else:
                copy.start()

    local = [pltpu.make_async_copy(src, dst, in_sem.at[i]) for i, (src, dst) in enumerate(
        ((hidden_hbm, hidden_ref), (gain_hbm, gain_ref), (pos_hbm, pos_ref), (post_hbm, post_ref),
         (kc_hbm, kc), (vc_hbm, vc)))]
    for copy in local:
        copy.start()
    for copy in local:
        copy.wait()
    prepare(pos_ref, hidden_ref, gain_ref, nrm, acc, rope)

    def to_owners(dist, act):
        zs = (tp + dist) % 4

        def message(when, index, row, rows, dest, first, block):
            dst = s1q.at[pl.ds(pl.multiple_of(first, rows), rows)]

            @pl.when(when)
            def _():
                act(s1a.at[zs, pl.ds(row, rows)], dst, dest, block, b_send.at[4 * dist + index], q_recv)

        y = tp % 4
        message(jnp.logical_not(last_x), 0, 0, qrows, place(0, z, core), tp * qrows, h * 4 + zs)
        message(first_x, 1, qrows, qrows, place(0, z, core), (4 + y) * qrows, 4 + zs)
        for i in range(2):
            message(jnp.logical_not(first_x), 1 + i, qrows + i * krows, krows, place(1, z, i),
                    core * 128 + tp * krows, h * 4 + zs)
            message(last_x, 3 * i, i * krows, krows, place(1, z, i), core * 128 + y * krows, zs)

    for dist in (0, 2, 1, 3):
        zs = (tp + dist) % 4
        came = s1a.at[zs]
        pltpu.make_async_copy(came, came, a_recv.at[(z + 4 - zs) % 4]).wait()
        to_owners(dist, exchange)

    def chunk(a, zs, gs, half):
        return gathered[a].at[zs, gs, pl.ds(half * halves[a], halves[a])]

    def d2d(a, xp, s):
        c = chunk(a, piece_z[s // 2], piece_g[xp], s % 2)
        i = (a * 2 + xp) * 8 + s
        return remote(c, c, d_send.at[i], d_recv.at[i], (place(h, z, 1 - core), tp))

    up = (place(h, zp, core), tp)
    down = (place(h, zm, core), tp)

    def zcopy(a, xp, i):
        zs, half, to = ((z, 0, up), (z, 1, up), (z, 0, down), (z, 1, down), (zm, 0, up), (zp, 1, down))[i]
        c = chunk(a, zs, piece_g[xp], half)
        j = (a * 2 + xp) * 6 + i
        return remote(c, c, z_send.at[j], z_recv.at[j], to)

    def xcopy(a, s):
        c = chunk(a, piece_z[s // 2], g, s % 2)
        return remote(c, c, x_send.at[a * 8 + s], x_recv.at[a * 8 + s], (place(1 - h, z, core), tp))

    def arrived(a, xp, s):
        d2d(a, xp, s).start()

    def launch(a, xp):
        for i in (0, 3, 1, 2):
            zcopy(a, xp, i).start()
        arrived(a, xp, 0)
        arrived(a, xp, 1)

    def relay(a, xp):
        zcopy(a, xp, 0).wait_recv()
        zcopy(a, xp, 4).start()
        arrived(a, xp, 2)
        zcopy(a, xp, 3).wait_recv()
        zcopy(a, xp, 5).start()
        arrived(a, xp, 5)
        zcopy(a, xp, 1).wait_recv()
        arrived(a, xp, 3)
        zcopy(a, xp, 2).wait_recv()
        arrived(a, xp, 4)

    def finish(a, xp):
        zcopy(a, xp, 4).wait_recv()
        arrived(a, xp, 6)
        zcopy(a, xp, 5).wait_recv()
        arrived(a, xp, 7)

    pltpu.make_async_copy(s1o, s1o, o_recv).wait()
    nrow = s1o.shape[1]
    for i in range(32):
        so[i * nrow:(i + 1) * nrow, :] = s1o[i].astype(jnp.float32)
    for b in range(9):
        go[z, g, :, b * 128:(b + 1) * 128] = so[b * 128:(b + 1) * 128, :].T.astype(jnp.bfloat16)
    launch(1, 0)
    for dist in range(4):
        to_owners(dist, exchange_done)
    for i in range(1, 8):
        peer = (2 * h + lo + i // 2) % 4
        pl.semaphore_signal(
            row_sem, inc=1, device_id_type=MESH,
            device_id=(place(peer // 2, z, (core + i) % 2), (peer % 2) * 4 + tp % 4))
    pltpu.make_async_copy(s1q, s1q, q_recv).wait()
    for b in range(9):
        for c in range(2):
            tile = s1q[c * 128:(c + 1) * 128, b * 128:(b + 1) * 128].astype(jnp.float32)
            gq[z, g, b * 128:(b + 1) * 128, c * 128:(c + 1) * 128] = tile.T.astype(jnp.bfloat16)
    launch(0, 0)
    relay(1, 0)
    pl.semaphore_wait(row_sem, 7)
    for s in range(2):
        xcopy(0, s).start()
    for s in (0, 1, 2, 5, 3, 4):
        xcopy(1, s).start()
    relay(0, 0)
    for s in range(2):
        xcopy(0, s).wait_recv()
    launch(0, 1)
    finish(1, 0)
    for s in (6, 7):
        xcopy(1, s).start()
    finish(0, 0)

    def project(xp, i):
        zs = piece_z[i]
        for s in (2 * i, 2 * i + 1):
            d2d(0, xp, s).wait_recv()
        for gs in (piece_g[xp], piece_g[xp] + 1 - 2 * core):
            acc[gs] += jnp.dot(nrm[zs], gq[zs, gs], preferred_element_type=jnp.float32)

    for i in range(4):
        project(0, i)
    relay(0, 1)
    project(1, 0)
    for s in (0, 1, 2, 5, 3, 4, 6, 7):
        xcopy(1, s).wait_recv()
        d2d(1, 1, s).start()
    finish(0, 1)
    for i in range(1, 4):
        project(1, i)
    att = attention(pos_ref, kc, vc, acc, rope)
    for xp in range(2):
        for s in range(8):
            d2d(1, xp, s).wait_recv()
    for zs in range(4):
        part = jnp.dot(att, go[zs].reshape(512, 1152), preferred_element_type=jnp.float32)
        part_ref[2 * WO_SLICE[zs]] = part[:, :576]
        part_ref[2 * WO_SLICE[zs] + 1] = part[:, 576:]
    sum_and_norm(part_ref, post_ref, out_ref, parts_in, square, squares, p_send, p_recv, s_send, s_recv)
    for part in range(3):
        for dist in range(4):
            away, _, _, copy = along_z(dist, part)
            if dist == 0:
                pl.when(away)(copy.wait_send)
            else:
                copy.wait_send()
    for p in range(8):
        for gd in range(4):
            exchange_done(*o_slice(p, gd))
    for s in range(2):
        xcopy(0, s).wait_send()
    for s in range(8):
        xcopy(1, s).wait_send()
    for a, xp in ((1, 0), (0, 0), (1, 1), (0, 1)):
        if (a, xp) != (1, 1):
            for i in range(6):
                zcopy(a, xp, i).wait_send()
        for s in range(8):
            d2d(a, xp, s).wait_send()


def in_hbm(x):
    return pltpu.with_memory_space_constraint(x, pltpu.HBM)


def gather_and_attend(q, k, v, o, hidden, gain, key_cache, value_cache, positions, post_gain):
    bf, f32 = jnp.bfloat16, jnp.float32
    dma = pltpu.SemaphoreType.DMA
    vmem = pltpu.VMEM
    return pl.pallas_call(
        gather_kernel,
        out_shape=(jax.ShapeDtypeStruct((4, 4, 1152, 256), bf),
                   jax.ShapeDtypeStruct((4, 4, 128, 1152), bf),
                   jax.ShapeDtypeStruct((4, 576), bf)),
        in_specs=[pl.BlockSpec(memory_space=pltpu.HBM)] * 10,
        out_specs=[pl.BlockSpec(memory_space=vmem)] * 3,
        scratch_shapes=[
            vmem(hidden.shape, bf), vmem(gain.shape, f32), vmem(key_cache.shape, bf),
            vmem(value_cache.shape, bf), pltpu.SMEM((4,), jnp.int32), vmem(post_gain.shape, f32),
            vmem((4, 4, 1152), bf), vmem((4, 4, 256), f32), vmem((2, 4, 128), f32),
            vmem((8, 4, 576), f32), vmem((7, 4, 576), f32), vmem((4, 128), f32), vmem((7, 4, 128), f32),
            vmem((4, 64, 1152), bf), vmem((256, 1152), bf), vmem((32, 36, 128), bf),
            vmem((1152, 128), f32),
            dma((12,)), dma((4,)), dma((16,)), dma, dma((32,)), dma,
            dma((24,)), dma((24,)), dma((16,)), dma((16,)), dma((32,)), dma((32,)),
            pltpu.SemaphoreType.REGULAR, dma((6,)), dma((7,)), dma((7,)), dma((7,)), dma((7,)),
        ],
        compiler_params=pltpu.CompilerParams(
            has_side_effects=True, collective_id=0, vmem_limit_bytes=16 * 1024 * 1024),
        name="gather_and_attend",
    )(*(in_hbm(x) for x in (q, k, v, o, hidden, gain, key_cache, value_cache, positions, post_gain)))


def prepare(pos_ref, hidden_ref, gain_ref, nrm, acc, rope):
    f32 = jnp.float32
    hid = hidden_ref[...].astype(f32)
    mean_square = jnp.mean(hid * hid, axis=-1, keepdims=True)
    gain = gain_ref[...].reshape(1, -1)
    normed = (hid * lax.rsqrt(mean_square + 1e-06) * gain).astype(jnp.bfloat16)
    for zs in range(4):
        nrm[zs] = normed[:, zs * 1152:(zs + 1) * 1152]
    acc[...] = jnp.zeros_like(acc)
    row = lax.broadcasted_iota(jnp.int32, (4, 128), 0)
    posf = jnp.zeros((4, 128), f32)
    for b in range(4):
        posf = jnp.where(row == b, pos_ref[b].astype(f32), posf)
    lane = lax.broadcasted_iota(jnp.int32, (4, 128), 1)
    angle = posf * jnp.exp((lane % 64).astype(f32) * (-2.0 / 128 * np.log(10000.0)))
    rope[0] = jnp.cos(angle)
    rope[1] = jnp.where(lane < 64, -jnp.sin(angle), jnp.sin(angle))


def attention(pos_ref, kc, vc, acc, rope):
    f32, bf = jnp.float32, jnp.bfloat16
    proj = []
    for gs in range(4):
        both = acc[gs]
        proj += [both[:, :128], both[:, 128:]]
    cosine, sine = rope[0], rope[1]

    def rotate(x):
        swapped = jnp.concatenate([x[:, 64:], x[:, :64]], axis=1)
        return (x * cosine + swapped * sine).astype(bf).astype(f32)

    query = jnp.concatenate([rotate(x) for x in proj[:4]], axis=0)
    keys = [rotate(x) for x in proj[4:6]]
    vals = [x.astype(bf).astype(f32) for x in proj[6:8]]
    keys_new = jnp.concatenate([keys[0], keys[0], keys[1], keys[1]], axis=0)
    values_new = jnp.concatenate([vals[0], vals[0], vals[1], vals[1]], axis=0)
    qb = query.astype(bf)
    length = kc.shape[2]
    r = lax.broadcasted_iota(jnp.int32, (16, length), 0)
    slot = lax.broadcasted_iota(jnp.int32, (16, length), 1)
    owner = (r // 8) * 4 + r % 4
    scores = jnp.zeros((16, length), f32)
    limit = jnp.zeros((16, length), jnp.int32)
    for kv in range(2):
        for b in range(4):
            s = lax.dot_general(qb, kc[b, kv], (((1,), (1,)), ((), ())), preferred_element_type=f32)
            scores = jnp.where(owner == kv * 4 + b, s, scores)
    for b in range(4):
        limit = jnp.where(r % 4 == b, pos_ref[b], limit)
    capped = soft_cap * jnp.tanh(scores * score_scale / soft_cap)
    raw = jnp.where(slot < limit, jnp.exp(capped), 0.0)
    self_score = jnp.sum(query * keys_new, axis=-1, keepdims=True) * score_scale
    self_raw = jnp.exp(soft_cap * jnp.tanh(self_score / soft_cap))
    denom = jnp.sum(raw, axis=-1, keepdims=True) + self_raw
    weights = (raw / denom).astype(bf).astype(f32)
    mixed = (self_raw / denom).astype(bf).astype(f32) * values_new
    for kv in range(2):
        for b in range(4):
            w = jnp.where(owner == kv * 4 + b, weights, 0.0).astype(bf)
            mixed += jnp.dot(w, vc[b, kv], preferred_element_type=f32)
    return jnp.concatenate([mixed[i * 4:(i + 1) * 4] for i in range(4)], axis=1).astype(bf)


def write_kernel(gq, go, small, joined_ref, wo_ref, small_ref, out_sem):
    pltpu.make_async_copy(small, small_ref, out_sem.at[2]).start()
    for zs in range(4):
        for gs in range(4):
            pltpu.make_async_copy(
                gq.at[zs, gs], joined_ref.at[pl.ds(zs * 1152, 1152), pl.ds(gs * 256, 256)],
                out_sem.at[0]).start()
            pltpu.make_async_copy(
                go.at[zs, gs], wo_ref.at[pl.ds(gs * 128, 128), pl.ds(WO_SLICE[zs] * 1152, 1152)],
                out_sem.at[1]).start()
    pltpu.make_async_copy(joined_ref, joined_ref, out_sem.at[0]).wait()
    pltpu.make_async_copy(wo_ref, wo_ref, out_sem.at[1]).wait()
    pltpu.make_async_copy(small, small_ref, out_sem.at[2]).wait()


def write_out(gq, go, small):
    bf = jnp.bfloat16
    vmem = pl.BlockSpec(memory_space=pltpu.VMEM)
    hbm = pl.BlockSpec(memory_space=pltpu.HBM)
    return pl.pallas_call(
        write_kernel,
        out_shape=(jax.ShapeDtypeStruct((4608, 1024), bf), jax.ShapeDtypeStruct((512, 4608), bf),
                   jax.ShapeDtypeStruct(small.shape, bf)),
        in_specs=[vmem, vmem, vmem],
        out_specs=[hbm, hbm, hbm],
        scratch_shapes=[pltpu.SemaphoreType.DMA((3,))],
        compiler_params=pltpu.CompilerParams(vmem_limit_bytes=16 * 1024 * 1024),
        name="write_out",
    )(gq, go, small)


def sum_and_norm(part_ref, gain_ref, out_ref, parts_in, square, squares, p_send, p_recv, s_send, s_recv):
    rep = lax.axis_index("rep")
    tp = lax.axis_index("tp")

    def part(d):
        to = (tp + d) % 8
        return remote(part_ref.at[to], parts_in.at[d - 1], p_send.at[d - 1], p_recv.at[d - 1], (rep, to))

    def sq(d):
        return remote(square, squares.at[d - 1], s_send.at[d - 1], s_recv.at[d - 1],
                      (rep, (tp + d) % 8))

    for d in range(1, 8):
        part(d).start()
    total = part_ref[tp]
    for d in range(1, 8):
        part(d).wait_recv()
        total += parts_in[d - 1]
    square[...] = jnp.broadcast_to(jnp.sum(total * total, axis=-1, keepdims=True), square.shape)
    for d in range(1, 8):
        sq(d).start()
    whole = square[...]
    for d in range(1, 8):
        sq(d).wait_recv()
        whole += squares[d - 1]
    scale = lax.rsqrt(whole[:, :1] / 4608.0 + 1e-06)
    out_ref[...] = (total * scale * gain_ref[...].reshape(1, -1)).astype(jnp.bfloat16)
    for d in range(1, 8):
        part(d).wait_send()
        sq(d).wait_send()


def body(
    hidden, positions, key_cache, value_cache, norm_gain, q_proj, k_proj, v_proj, o_proj, post_gain
):
    gq, go, attn_out = gather_and_attend(
        q_proj, k_proj, v_proj, o_proj, hidden, norm_gain, key_cache, value_cache, positions, post_gain)
    return write_out(gq, go, attn_out)


def solution(mesh):
    in_specs = (
        P("rep", None),
        P("rep"),
        P("rep", "tp", None, None),
        P("rep", "tp", None, None),
        P(),
        P(("rep", "tp"), None),
        P(("rep", "tp"), None),
        P(("rep", "tp"), None),
        P(("rep", "tp"), None),
        P("tp"),
    )
    out_specs = (P(None, "tp"), P("tp", None), P("rep", "tp"))
    return jax.shard_map(body, mesh=mesh, in_specs=in_specs, out_specs=out_specs, check_vma=False)
```

```python
import jax
import jax.numpy as jnp
import numpy as np
from jax import lax
from jax.experimental import pallas as pl
from jax.experimental.pallas import tpu as pltpu
from jax.sharding import PartitionSpec as P

score_scale = 144.0 ** (-0.5)
soft_cap = 50.0
MESH = pl.DeviceIdType.MESH
WO_SLICE = (0, 2, 3, 1)


def remote(src, dst, ssem, rsem, device):
    return pltpu.make_async_remote_copy(
        src_ref=src, dst_ref=dst, send_sem=ssem, recv_sem=rsem, device_id=device,
        device_id_type=MESH)


def gather_kernel(q_ref, k_ref, v_ref, o_ref, hidden_hbm, gain_hbm, kc_hbm, vc_hbm, pos_hbm, post_hbm,
                  gq, go, out_ref,
                  hidden_ref, gain_ref, kc, vc, pos_ref, post_ref, nrm, acc, rope, part_ref, parts_in, s1a, s1q, s1o, so,
                  a_send, a_recv, b_send, q_recv, o_send, o_recv, z_send, z_recv, x_send, x_recv,
                  d_send, d_recv, row_sem, in_sem, p_send, p_recv):
    rep = lax.axis_index("rep")
    tp = lax.axis_index("tp")
    h = rep // 8
    z = (rep // 2) % 4
    core = rep % 2
    lo = tp // 4
    g = 2 * h + core
    gpar = 2 * (1 - h) + core
    zp = (z + 1) % 4
    zm = (z + 3) % 4
    zo = (z + 2) % 4
    gathered = (gq, go)
    halves = (gq.shape[2] // 2, go.shape[2] // 2)
    piece_z = (z, zm, zp, zo)
    piece_g = (g, gpar)

    def place(h_, z_, c_):
        return h_ * 8 + z_ * 2 + c_

    barrier = pltpu.get_barrier_semaphore()
    pair = z + 1 - 2 * (z % 2)
    greeted = [((z_ + 2) % 4, h_, core, tp_) for z_ in (pair, z)
               for h_, tp_ in ((1 - h, (tp + 4) % 8), (h, tp))]
    greeted += [(z_, (g + a) % 4 // 2, (g + a) % 2, (tp + b) % 8) for z_ in (pair, z)
                for a in (2, 3, 1, 0) for b in (6, 2, 5, 7, 1, 3, 4, 0)][:-1]
    for z_, h_, c_, tp_ in greeted:
        pl.semaphore_signal(barrier, inc=1, device_id=(place(h_, z_, c_), tp_), device_id_type=MESH)
    pl.semaphore_wait(barrier, len(greeted))

    zdest = 2 * h + z // 2
    zdest = jnp.where(zdest == 0, 0, jnp.where(zdest == 1, 3, zdest - 1))
    slot = (rep % 4) * 8 + tp

    def o_slice(i, j):
        p = (tp + i) % 8
        gd = (g + j) % 4
        src = o_ref.at[:, pl.ds(pl.multiple_of(p * 512 + gd * 128, 128), 128)]
        return src, s1o.at[slot], place(gd // 2, zdest, gd % 2), p, o_send.at[4 * i + j], o_recv

    def exchange(src, dst, dest_rep, dest_tp, ssem, rsem):
        own = jnp.logical_and(dest_rep == rep, dest_tp == tp)

        @pl.when(own)
        def _():
            pltpu.make_async_copy(src, dst, rsem).start()

        @pl.when(jnp.logical_not(own))
        def _():
            remote(src, dst, ssem, rsem, (dest_rep, dest_tp)).start()

    def exchange_done(src, dst, dest_rep, dest_tp, ssem, rsem):
        own = jnp.logical_and(dest_rep == rep, dest_tp == tp)

        @pl.when(jnp.logical_not(own))
        def _():
            remote(src, dst, ssem, rsem, (dest_rep, dest_tp)).wait_send()

    for p in range(8):
        for gd in range(4):
            exchange(*o_slice(p, gd))

    width = s1q.shape[1]
    qrows, krows = q_ref.shape[0], k_ref.shape[0]
    parts = ((q_ref, 0, qrows), (k_ref, qrows, krows), (v_ref, qrows + krows, krows))

    first_x = jnp.logical_and(h == 0, lo == 0)
    last_x = jnp.logical_and(h == 1, lo == 1)

    def along_z(dist, part):
        zd = (z + dist) % 4
        ref, row, rows = parts[part]
        src = ref.at[:, pl.ds(pl.multiple_of(zd * width, width), width)]
        if part == 0:
            away, there, to_h, to_tp = last_x, qrows, 0, tp % 4
        else:
            away, there, to_h, to_tp = first_x, row - qrows, 1, 4 + tp % 4
        row = pl.multiple_of(jnp.where(away, there, row), krows)
        dst = s1a.at[z, pl.ds(row, rows)]
        device = (place(jnp.where(away, to_h, h), zd, core), jnp.where(away, to_tp, tp))
        return away, src, dst, remote(src, dst, a_send.at[3 * dist + part], a_recv.at[dist], device)

    for dist in (2, 1, 3, 0):
        for part in range(3):
            away, src, dst, copy = along_z(dist, part)
            if dist == 0:
                pl.when(away)(copy.start)
                pl.when(jnp.logical_not(away))(
                    pltpu.make_async_copy(src, dst, a_recv.at[0]).start)
            else:
                copy.start()

    local = [pltpu.make_async_copy(src, dst, in_sem.at[i]) for i, (src, dst) in enumerate(
        ((hidden_hbm, hidden_ref), (gain_hbm, gain_ref), (pos_hbm, pos_ref), (post_hbm, post_ref),
         (kc_hbm, kc), (vc_hbm, vc)))]
    for copy in local:
        copy.start()
    for copy in local:
        copy.wait()
    prepare(pos_ref, hidden_ref, gain_ref, nrm, acc, rope)

    def to_owners(dist, act):
        zs = (tp + dist) % 4

        def message(when, index, row, rows, dest, first, block):
            dst = s1q.at[pl.ds(pl.multiple_of(first, rows), rows)]

            @pl.when(when)
            def _():
                act(s1a.at[zs, pl.ds(row, rows)], dst, dest, block, b_send.at[4 * dist + index], q_recv)

        y = tp % 4
        message(jnp.logical_not(last_x), 0, 0, qrows, place(0, z, core), tp * qrows, h * 4 + zs)
        message(first_x, 1, qrows, qrows, place(0, z, core), (4 + y) * qrows, 4 + zs)
        for i in range(2):
            message(jnp.logical_not(first_x), 1 + i, qrows + i * krows, krows, place(1, z, i),
                    core * 128 + tp * krows, h * 4 + zs)
            message(last_x, 3 * i, i * krows, krows, place(1, z, i), core * 128 + y * krows, zs)

    for dist in (0, 2, 1, 3):
        zs = (tp + dist) % 4
        came = s1a.at[zs]
        pltpu.make_async_copy(came, came, a_recv.at[(z + 4 - zs) % 4]).wait()
        to_owners(dist, exchange)

    def chunk(a, zs, gs, half):
        return gathered[a].at[zs, gs, pl.ds(half * halves[a], halves[a])]

    early = 192
    late = (gq.shape[2] - early) // 2

    def ring_chunk(a, xp, zs, half):
        if a == 0 and xp == 1:
            return gq.at[zs, gpar, pl.ds(early + half * late, late)]
        return chunk(a, zs, piece_g[xp], half)

    def early_rows(i, gs):
        return gq.at[piece_z[i], gs, pl.ds(0, early)]

    def xearly(i):
        c = early_rows(i, g)
        return remote(c, c, x_send.at[2 + i], x_recv.at[2 + i], (place(1 - h, z, core), tp))

    def dearly(i):
        c = early_rows(i, gpar)
        return remote(c, c, d_send.at[32 + i], d_recv.at[32 + i], (place(h, z, 1 - core), tp))

    def d2d(a, xp, s):
        if s < 2:
            c = chunk(a, z, piece_g[xp], s)
        else:
            c = ring_chunk(a, xp, piece_z[s // 2], s % 2)
        i = (a * 2 + xp) * 8 + s
        return remote(c, c, d_send.at[i], d_recv.at[i], (place(h, z, 1 - core), tp))

    up = (place(h, zp, core), tp)
    down = (place(h, zm, core), tp)

    def zcopy(a, xp, i):
        zs, half, to = ((z, 0, up), (z, 1, up), (z, 0, down), (z, 1, down), (zm, 0, up), (zp, 1, down))[i]
        c = ring_chunk(a, xp, zs, half)
        j = (a * 2 + xp) * 6 + i
        return remote(c, c, z_send.at[j], z_recv.at[j], to)

    def xcopy(a, s):
        c = chunk(a, piece_z[s // 2], g, s % 2)
        return remote(c, c, x_send.at[a * 8 + s], x_recv.at[a * 8 + s], (place(1 - h, z, core), tp))

    def arrived(a, xp, s):
        d2d(a, xp, s).start()

    def launch(a, xp):
        for i in (0, 3, 1, 2):
            zcopy(a, xp, i).start()
        arrived(a, xp, 0)
        arrived(a, xp, 1)

    def relay(a, xp):
        zcopy(a, xp, 0).wait_recv()
        zcopy(a, xp, 4).start()
        arrived(a, xp, 2)
        zcopy(a, xp, 3).wait_recv()
        zcopy(a, xp, 5).start()
        arrived(a, xp, 5)
        zcopy(a, xp, 1).wait_recv()
        arrived(a, xp, 3)
        zcopy(a, xp, 2).wait_recv()
        arrived(a, xp, 4)

    def finish(a, xp):
        zcopy(a, xp, 4).wait_recv()
        arrived(a, xp, 6)
        zcopy(a, xp, 5).wait_recv()
        arrived(a, xp, 7)

    pltpu.make_async_copy(s1o, s1o, o_recv).wait()
    nrow = s1o.shape[1]
    for i in range(32):
        so[i * nrow:(i + 1) * nrow, :] = s1o[i].astype(jnp.float32)
    for b in range(9):
        go[z, g, :, b * 128:(b + 1) * 128] = so[b * 128:(b + 1) * 128, :].T.astype(jnp.bfloat16)
    launch(1, 0)
    for dist in range(4):
        to_owners(dist, exchange_done)
    for i in range(1, 8):
        peer = (2 * h + lo + i // 2) % 4
        pl.semaphore_signal(
            row_sem, inc=1, device_id_type=MESH,
            device_id=(place(peer // 2, z, (core + i) % 2), (peer % 2) * 4 + tp % 4))
    for s in range(2):
        xcopy(1, s).start()
    pltpu.make_async_copy(s1q, s1q, q_recv).wait()
    for b in range(9):
        for c in range(2):
            tile = s1q[c * 128:(c + 1) * 128, b * 128:(b + 1) * 128].astype(jnp.float32)
            gq[z, g, b * 128:(b + 1) * 128, c * 128:(c + 1) * 128] = tile.T.astype(jnp.bfloat16)
    launch(0, 0)
    pl.semaphore_wait(row_sem, 7)
    for s in range(2):
        xcopy(0, s).start()
    relay(1, 0)
    for s in (2, 5, 3, 4):
        xcopy(1, s).start()
    relay(0, 0)
    for i in (1, 2):
        xearly(i).start()
    for s in range(2):
        xcopy(0, s).wait_recv()
    launch(0, 1)
    finish(1, 0)
    finish(0, 0)
    xearly(3).start()
    for s in (6, 7):
        xcopy(1, s).start()

    def project(xp, i):
        def add(gs):
            acc[gs] += jnp.dot(nrm[piece_z[i]], gq[piece_z[i], gs], preferred_element_type=jnp.float32)

        add(piece_g[xp])
        for s in (2 * i, 2 * i + 1):
            d2d(0, xp, s).wait_recv()
        if xp == 1 and i > 0:
            dearly(i).wait_recv()
        add(piece_g[xp] + 1 - 2 * core)

    for i in range(4):
        project(0, i)
    relay(0, 1)
    project(1, 0)
    for s in (0, 1, 2, 5, 3, 4):
        xcopy(1, s).wait_recv()
        d2d(1, 1, s).start()
    for i in (1, 2):
        xearly(i).wait_recv()
        dearly(i).start()
    project(1, 1)
    project(1, 2)
    xearly(3).wait_recv()
    dearly(3).start()
    finish(0, 1)
    project(1, 3)
    for s in (6, 7):
        xcopy(1, s).wait_recv()
        d2d(1, 1, s).start()
    att = attention(pos_ref, kc, vc, acc, rope)
    for xp in range(2):
        for s in range(8):
            d2d(1, xp, s).wait_recv()
    for zs in range(4):
        part = jnp.dot(att, go[zs].reshape(512, 1152), preferred_element_type=jnp.float32)
        part = part.astype(jnp.bfloat16)
        part_ref[2 * WO_SLICE[zs]] = part[:, :576]
        part_ref[2 * WO_SLICE[zs] + 1] = part[:, 576:]
    sum_and_norm(part_ref, post_ref, out_ref, parts_in, p_send, p_recv)
    for part in range(3):
        for dist in range(4):
            away, _, _, copy = along_z(dist, part)
            if dist == 0:
                pl.when(away)(copy.wait_send)
            else:
                copy.wait_send()
    for p in range(8):
        for gd in range(4):
            exchange_done(*o_slice(p, gd))
    for s in range(2):
        xcopy(0, s).wait_send()
    for s in range(8):
        xcopy(1, s).wait_send()
    for i in range(1, 4):
        xearly(i).wait_send()
        dearly(i).wait_send()
    for a, xp in ((1, 0), (0, 0), (1, 1), (0, 1)):
        if (a, xp) != (1, 1):
            for i in range(6):
                zcopy(a, xp, i).wait_send()
        for s in range(8):
            d2d(a, xp, s).wait_send()


def in_hbm(x):
    return pltpu.with_memory_space_constraint(x, pltpu.HBM)


def gather_and_attend(q, k, v, o, hidden, gain, key_cache, value_cache, positions, post_gain):
    bf, f32 = jnp.bfloat16, jnp.float32
    dma = pltpu.SemaphoreType.DMA
    vmem = pltpu.VMEM
    return pl.pallas_call(
        gather_kernel,
        out_shape=(jax.ShapeDtypeStruct((4, 4, 1152, 256), bf),
                   jax.ShapeDtypeStruct((4, 4, 128, 1152), bf),
                   jax.ShapeDtypeStruct((4, 576), bf)),
        in_specs=[pl.BlockSpec(memory_space=pltpu.HBM)] * 10,
        out_specs=[pl.BlockSpec(memory_space=vmem)] * 3,
        scratch_shapes=[
            vmem(hidden.shape, bf), vmem(gain.shape, f32), vmem(key_cache.shape, bf),
            vmem(value_cache.shape, bf), pltpu.SMEM((4,), jnp.int32), vmem(post_gain.shape, f32),
            vmem((4, 4, 1152), bf), vmem((4, 4, 256), f32), vmem((2, 4, 128), f32),
            vmem((8, 4, 576), bf), vmem((7, 8, 4, 576), bf),
            vmem((4, 64, 1152), bf), vmem((256, 1152), bf), vmem((32, 36, 128), bf),
            vmem((1152, 128), f32),
            dma((12,)), dma((4,)), dma((16,)), dma, dma((32,)), dma,
            dma((24,)), dma((24,)), dma((16,)), dma((16,)), dma((36,)), dma((36,)),
            pltpu.SemaphoreType.REGULAR, dma((6,)), dma((7,)), dma((7,)),
        ],
        compiler_params=pltpu.CompilerParams(
            has_side_effects=True, collective_id=0, vmem_limit_bytes=16 * 1024 * 1024),
        name="gather_and_attend",
    )(*(in_hbm(x) for x in (q, k, v, o, hidden, gain, key_cache, value_cache, positions, post_gain)))


def prepare(pos_ref, hidden_ref, gain_ref, nrm, acc, rope):
    f32 = jnp.float32
    hid = hidden_ref[...].astype(f32)
    mean_square = jnp.mean(hid * hid, axis=-1, keepdims=True)
    gain = gain_ref[...].reshape(1, -1)
    normed = (hid * lax.rsqrt(mean_square + 1e-06) * gain).astype(jnp.bfloat16)
    for zs in range(4):
        nrm[zs] = normed[:, zs * 1152:(zs + 1) * 1152]
    acc[...] = jnp.zeros_like(acc)
    row = lax.broadcasted_iota(jnp.int32, (4, 128), 0)
    posf = jnp.zeros((4, 128), f32)
    for b in range(4):
        posf = jnp.where(row == b, pos_ref[b].astype(f32), posf)
    lane = lax.broadcasted_iota(jnp.int32, (4, 128), 1)
    angle = posf * jnp.exp((lane % 64).astype(f32) * (-2.0 / 128 * np.log(10000.0)))
    rope[0] = jnp.cos(angle)
    rope[1] = jnp.where(lane < 64, -jnp.sin(angle), jnp.sin(angle))


def attention(pos_ref, kc, vc, acc, rope):
    f32, bf = jnp.float32, jnp.bfloat16
    proj = []
    for gs in range(4):
        both = acc[gs]
        proj += [both[:, :128], both[:, 128:]]
    cosine, sine = rope[0], rope[1]

    def rotate(x):
        swapped = jnp.concatenate([x[:, 64:], x[:, :64]], axis=1)
        return (x * cosine + swapped * sine).astype(bf).astype(f32)

    query = jnp.concatenate([rotate(x) for x in proj[:4]], axis=0)
    keys = [rotate(x) for x in proj[4:6]]
    vals = [x.astype(bf).astype(f32) for x in proj[6:8]]
    keys_new = jnp.concatenate([keys[0], keys[0], keys[1], keys[1]], axis=0)
    values_new = jnp.concatenate([vals[0], vals[0], vals[1], vals[1]], axis=0)
    qb = query.astype(bf)
    length = kc.shape[2]
    r = lax.broadcasted_iota(jnp.int32, (16, length), 0)
    slot = lax.broadcasted_iota(jnp.int32, (16, length), 1)
    owner = (r // 8) * 4 + r % 4
    scores = jnp.zeros((16, length), f32)
    limit = jnp.zeros((16, length), jnp.int32)
    for kv in range(2):
        for b in range(4):
            s = lax.dot_general(qb, kc[b, kv], (((1,), (1,)), ((), ())), preferred_element_type=f32)
            scores = jnp.where(owner == kv * 4 + b, s, scores)
    for b in range(4):
        limit = jnp.where(r % 4 == b, pos_ref[b], limit)
    capped = soft_cap * jnp.tanh(scores * score_scale / soft_cap)
    raw = jnp.where(slot < limit, jnp.exp(capped), 0.0)
    self_score = jnp.sum(query * keys_new, axis=-1, keepdims=True) * score_scale
    self_raw = jnp.exp(soft_cap * jnp.tanh(self_score / soft_cap))
    denom = jnp.sum(raw, axis=-1, keepdims=True) + self_raw
    weights = (raw / denom).astype(bf).astype(f32)
    mixed = (self_raw / denom).astype(bf).astype(f32) * values_new
    for kv in range(2):
        for b in range(4):
            w = jnp.where(owner == kv * 4 + b, weights, 0.0).astype(bf)
            mixed += jnp.dot(w, vc[b, kv], preferred_element_type=f32)
    return jnp.concatenate([mixed[i * 4:(i + 1) * 4] for i in range(4)], axis=1).astype(bf)


def write_kernel(gq, go, small, joined_ref, wo_ref, small_ref, out_sem):
    pltpu.make_async_copy(small, small_ref, out_sem.at[2]).start()
    for zs in range(4):
        for gs in range(4):
            pltpu.make_async_copy(
                gq.at[zs, gs], joined_ref.at[pl.ds(zs * 1152, 1152), pl.ds(gs * 256, 256)],
                out_sem.at[0]).start()
            pltpu.make_async_copy(
                go.at[zs, gs], wo_ref.at[pl.ds(gs * 128, 128), pl.ds(WO_SLICE[zs] * 1152, 1152)],
                out_sem.at[1]).start()
    pltpu.make_async_copy(joined_ref, joined_ref, out_sem.at[0]).wait()
    pltpu.make_async_copy(wo_ref, wo_ref, out_sem.at[1]).wait()
    pltpu.make_async_copy(small, small_ref, out_sem.at[2]).wait()


def write_out(gq, go, small):
    bf = jnp.bfloat16
    vmem = pl.BlockSpec(memory_space=pltpu.VMEM)
    hbm = pl.BlockSpec(memory_space=pltpu.HBM)
    return pl.pallas_call(
        write_kernel,
        out_shape=(jax.ShapeDtypeStruct((4608, 1024), bf), jax.ShapeDtypeStruct((512, 4608), bf),
                   jax.ShapeDtypeStruct(small.shape, bf)),
        in_specs=[vmem, vmem, vmem],
        out_specs=[hbm, hbm, hbm],
        scratch_shapes=[pltpu.SemaphoreType.DMA((3,))],
        compiler_params=pltpu.CompilerParams(vmem_limit_bytes=16 * 1024 * 1024),
        name="write_out",
    )(gq, go, small)


def sum_and_norm(part_ref, gain_ref, out_ref, parts_in, p_send, p_recv):
    f32 = jnp.float32
    rep = lax.axis_index("rep")
    tp = lax.axis_index("tp")

    def part(d):
        return remote(part_ref, parts_in.at[d - 1], p_send.at[d - 1], p_recv.at[d - 1],
                      (rep, (tp + d) % 8))

    for d in (6, 2, 5, 7, 1, 3, 4):
        part(d).start()
    total = part_ref[...].astype(f32)
    own = part_ref[tp].astype(f32)
    for d in (4, 1, 3, 7, 5, 2, 6):
        part(d).wait_recv()
        total += parts_in[d - 1].astype(f32)
        own += parts_in[d - 1, tp].astype(f32)
    square = jnp.sum(jnp.sum(total * total, axis=0), axis=-1, keepdims=True)
    scale = lax.rsqrt(square / 4608.0 + 1e-06)
    out_ref[...] = (own * scale * gain_ref[...].reshape(1, -1)).astype(jnp.bfloat16)
    for d in range(1, 8):
        part(d).wait_send()


def body(
    hidden, positions, key_cache, value_cache, norm_gain, q_proj, k_proj, v_proj, o_proj, post_gain
):
    gq, go, attn_out = gather_and_attend(
        q_proj, k_proj, v_proj, o_proj, hidden, norm_gain, key_cache, value_cache, positions, post_gain)
    return write_out(gq, go, attn_out)


def solution(mesh):
    in_specs = (
        P("rep", None),
        P("rep"),
        P("rep", "tp", None, None),
        P("rep", "tp", None, None),
        P(),
        P(("rep", "tp"), None),
        P(("rep", "tp"), None),
        P(("rep", "tp"), None),
        P(("rep", "tp"), None),
        P("tp"),
    )
    out_specs = (P(None, "tp"), P("tp", None), P("rep", "tp"))
    return jax.shard_map(body, mesh=mesh, in_specs=in_specs, out_specs=out_specs, check_vma=False)
```

```python
import jax
import jax.numpy as jnp
import numpy as np
from jax import lax
from jax.experimental import pallas as pl
from jax.experimental.pallas import tpu as pltpu
from jax.sharding import PartitionSpec as P

score_scale = 144.0 ** (-0.5)
soft_cap = 50.0
MESH = pl.DeviceIdType.MESH
WO_SLICE = (0, 2, 3, 1)


def remote(src, dst, ssem, rsem, device):
    return pltpu.make_async_remote_copy(
        src_ref=src, dst_ref=dst, send_sem=ssem, recv_sem=rsem, device_id=device,
        device_id_type=MESH)


def settle(ref, sem):
    pltpu.make_async_copy(ref, ref, sem).wait()


def gather_kernel(q_ref, k_ref, v_ref, o_ref, hidden_hbm, gain_hbm, kc_hbm, vc_hbm, pos_hbm, post_hbm,
                  gq, go, out_ref,
                  hidden_ref, gain_ref, kc, vc, pos_ref, post_ref, nrm, acc, rope, part_ref, parts_in, s1a, s1q, s1o, so,
                  a_send, a_recv, b_send, q_recv, o_send, o_recv, z_send, z_recv, x_send, x_recv,
                  d_send, d_recv, row_sem, in_sem, p_send, p_recv):
    rep = lax.axis_index("rep")
    tp = lax.axis_index("tp")
    h = rep // 8
    z = (rep // 2) % 4
    core = rep % 2
    lo = tp // 4
    g = 2 * h + core
    gpar = 2 * (1 - h) + core
    zp = (z + 1) % 4
    zm = (z + 3) % 4
    zo = (z + 2) % 4
    gathered = (gq, go)
    halves = (gq.shape[2] // 2, go.shape[2] // 2)
    piece_z = (z, zm, zp, zo)
    piece_g = (g, gpar)

    def place(h_, z_, c_):
        return h_ * 8 + z_ * 2 + c_

    barrier = pltpu.get_barrier_semaphore()
    pair = z + 1 - 2 * (z % 2)
    greeted = [((z_ + 2) % 4, h_, core, tp_) for z_ in (pair, z)
               for h_, tp_ in ((1 - h, (tp + 4) % 8), (h, tp))]
    greeted += [(z_, (g + a) % 4 // 2, (g + a) % 2, (tp + b) % 8) for z_ in (pair, z)
                for a in (2, 3, 1, 0) for b in (6, 2, 5, 7, 1, 3, 4, 0)][:-1]
    for z_, h_, c_, tp_ in greeted:
        pl.semaphore_signal(barrier, inc=1, device_id=(place(h_, z_, c_), tp_), device_id_type=MESH)
    pl.semaphore_wait(barrier, len(greeted))

    zdest = 2 * h + z // 2
    zdest = jnp.where(zdest == 0, 0, jnp.where(zdest == 1, 3, zdest - 1))
    slot = (rep % 4) * 8 + tp

    def o_slice(i, j):
        p = (tp + i) % 8
        gd = (g + j) % 4
        src = o_ref.at[:, pl.ds(pl.multiple_of(p * 512 + gd * 128, 128), 128)]
        return src, s1o.at[slot], place(gd // 2, zdest, gd % 2), p, o_send, o_recv

    def exchange(src, dst, dest_rep, dest_tp, ssem, rsem):
        own = jnp.logical_and(dest_rep == rep, dest_tp == tp)

        @pl.when(own)
        def _():
            pltpu.make_async_copy(src, dst, rsem).start()

        @pl.when(jnp.logical_not(own))
        def _():
            remote(src, dst, ssem, rsem, (dest_rep, dest_tp)).start()

    for p in range(8):
        for gd in range(4):
            exchange(*o_slice(p, gd))

    width = s1q.shape[1]
    qrows, krows = q_ref.shape[0], k_ref.shape[0]
    parts = ((q_ref, 0, qrows), (k_ref, qrows, krows), (v_ref, qrows + krows, krows))

    first_x = jnp.logical_and(h == 0, lo == 0)
    last_x = jnp.logical_and(h == 1, lo == 1)

    def along_z(dist, part):
        zd = (z + dist) % 4
        ref, row, rows = parts[part]
        src = ref.at[:, pl.ds(pl.multiple_of(zd * width, width), width)]
        if part == 0:
            away, there, to_h, to_tp = last_x, qrows, 0, tp % 4
        else:
            away, there, to_h, to_tp = first_x, row - qrows, 1, 4 + tp % 4
        row = pl.multiple_of(jnp.where(away, there, row), krows)
        dst = s1a.at[z, pl.ds(row, rows)]
        device = (place(jnp.where(away, to_h, h), zd, core), jnp.where(away, to_tp, tp))
        return away, src, dst, remote(src, dst, a_send.at[min(dist, 1)], a_recv.at[dist], device)

    for dist in (2, 1, 3, 0):
        for part in range(3):
            away, src, dst, copy = along_z(dist, part)
            if dist == 0:
                pl.when(away)(copy.start)
                pl.when(jnp.logical_not(away))(
                    pltpu.make_async_copy(src, dst, a_recv.at[0]).start)
            else:
                copy.start()

    local = [pltpu.make_async_copy(src, dst, in_sem.at[i]) for i, (src, dst) in enumerate(
        ((hidden_hbm, hidden_ref), (gain_hbm, gain_ref), (pos_hbm, pos_ref), (post_hbm, post_ref),
         (kc_hbm, kc), (vc_hbm, vc)))]
    for copy in local:
        copy.start()
    for copy in local:
        copy.wait()
    prepare(pos_ref, hidden_ref, gain_ref, nrm, acc, rope)

    def to_owners(dist):
        zs = (tp + dist) % 4

        def message(when, row, rows, dest, first, block):
            dst = s1q.at[pl.ds(pl.multiple_of(first, rows), rows)]

            @pl.when(when)
            def _():
                exchange(s1a.at[zs, pl.ds(row, rows)], dst, dest, block, b_send, q_recv)

        y = tp % 4
        message(jnp.logical_not(last_x), 0, qrows, place(0, z, core), tp * qrows, h * 4 + zs)
        message(first_x, qrows, qrows, place(0, z, core), (4 + y) * qrows, 4 + zs)
        for i in range(2):
            message(jnp.logical_not(first_x), qrows + i * krows, krows, place(1, z, i),
                    core * 128 + tp * krows, h * 4 + zs)
            message(last_x, i * krows, krows, place(1, z, i), core * 128 + y * krows, zs)

    for dist in (0, 2, 1, 3):
        zs = (tp + dist) % 4
        came = s1a.at[zs]
        pltpu.make_async_copy(came, came, a_recv.at[(z + 4 - zs) % 4]).wait()
        to_owners(dist)

    def chunk(a, zs, gs, half):
        return gathered[a].at[zs, gs, pl.ds(half * halves[a], halves[a])]

    early = 192
    late = (gq.shape[2] - early) // 2

    def ring_chunk(a, xp, zs, half):
        if a == 0 and xp == 1:
            return gq.at[zs, gpar, pl.ds(early + half * late, late)]
        return chunk(a, zs, piece_g[xp], half)

    def early_rows(i, gs):
        return gq.at[piece_z[i], gs, pl.ds(0, early)]

    def xearly(i):
        c = early_rows(i, g)
        return remote(c, c, x_send.at[2], x_recv.at[1 + i], (place(1 - h, z, core), tp))

    def dearly(i):
        c = early_rows(i, gpar)
        return remote(c, c, d_send.at[1], d_recv.at[4 + i], (place(h, z, 1 - core), tp))

    def d2d(a, xp, s):
        if s < 2:
            c = chunk(a, z, piece_g[xp], s)
        else:
            c = ring_chunk(a, xp, piece_z[s // 2], s % 2)
        i = a * 2 + xp
        return remote(c, c, d_send.at[i], d_recv.at[i * 4 + s // 2], (place(h, z, 1 - core), tp))

    def d2d_piece_done(a, xp, i):
        settle(gathered[a].at[piece_z[i], 0], d_recv.at[(a * 2 + xp) * 4 + i])

    up = (place(h, zp, core), tp)
    down = (place(h, zm, core), tp)

    ring = {(1, 0): 0, (0, 0): 1, (0, 1): 2}

    def zcopy(a, xp, i):
        zs, half, to = ((z, 0, up), (z, 1, up), (z, 0, down), (z, 1, down), (zm, 0, up), (zp, 1, down))[i]
        c = ring_chunk(a, xp, zs, half)
        j = ring[a, xp]
        return remote(c, c, z_send.at[j], z_recv.at[j * 6 + i], to)

    def xcopy(a, s):
        c = chunk(a, piece_z[s // 2], g, s % 2)
        return remote(c, c, x_send.at[a], x_recv.at[a * 5 + s], (place(1 - h, z, core), tp))

    def arrived(a, xp, s):
        d2d(a, xp, s).start()

    def launch(a, xp):
        for i in (0, 3, 1, 2):
            zcopy(a, xp, i).start()
        arrived(a, xp, 0)
        arrived(a, xp, 1)

    def relay(a, xp):
        zcopy(a, xp, 0).wait_recv()
        zcopy(a, xp, 4).start()
        arrived(a, xp, 2)
        zcopy(a, xp, 3).wait_recv()
        zcopy(a, xp, 5).start()
        arrived(a, xp, 5)
        zcopy(a, xp, 1).wait_recv()
        arrived(a, xp, 3)
        zcopy(a, xp, 2).wait_recv()
        arrived(a, xp, 4)

    def finish(a, xp):
        zcopy(a, xp, 4).wait_recv()
        arrived(a, xp, 6)
        zcopy(a, xp, 5).wait_recv()
        arrived(a, xp, 7)

    pltpu.make_async_copy(s1o, s1o, o_recv).wait()
    nrow = s1o.shape[1]
    for i in range(32):
        so[i * nrow:(i + 1) * nrow, :] = s1o[i].astype(jnp.float32)
    for b in range(9):
        go[z, g, :, b * 128:(b + 1) * 128] = so[b * 128:(b + 1) * 128, :].T.astype(jnp.bfloat16)
    launch(1, 0)
    for s in range(2):
        xcopy(1, s).start()
    def slices_left(when, rows):
        @pl.when(when)
        def _():
            settle(s1q.at[pl.ds(0, rows)], b_send)

    ends = jnp.logical_or(first_x, last_x)
    slices_left(first_x, s1q.shape[0] - qrows)
    slices_left(last_x, s1q.shape[0] - krows)
    slices_left(jnp.logical_not(ends), s1q.shape[0])
    for i in range(1, 8):
        peer = (2 * h + lo + i // 2) % 4
        pl.semaphore_signal(
            row_sem, inc=1, device_id_type=MESH,
            device_id=(place(peer // 2, z, (core + i) % 2), (peer % 2) * 4 + tp % 4))
    pltpu.make_async_copy(s1q, s1q, q_recv).wait()
    for b in range(9):
        for c in range(2):
            tile = s1q[c * 128:(c + 1) * 128, b * 128:(b + 1) * 128].astype(jnp.float32)
            gq[z, g, b * 128:(b + 1) * 128, c * 128:(c + 1) * 128] = tile.T.astype(jnp.bfloat16)
    launch(0, 0)
    pl.semaphore_wait(row_sem, 7)
    for s in range(2):
        xcopy(0, s).start()
    relay(1, 0)
    for s in (2, 5, 3, 4):
        xcopy(1, s).start()
    relay(0, 0)
    for i in (1, 2):
        xearly(i).start()
    for s in range(2):
        xcopy(0, s).wait_recv()
    launch(0, 1)
    finish(1, 0)
    finish(0, 0)
    xearly(3).start()
    for s in (6, 7):
        xcopy(1, s).start()

    def project(xp, i):
        def add(gs):
            acc[gs] += jnp.dot(nrm[piece_z[i]], gq[piece_z[i], gs], preferred_element_type=jnp.float32)

        add(piece_g[xp])
        d2d_piece_done(0, xp, i)
        add(piece_g[xp] + 1 - 2 * core)

    for i in range(4):
        project(0, i)
    relay(0, 1)
    project(1, 0)
    for s in (0, 1, 2, 5, 3, 4):
        xcopy(1, s).wait_recv()
        d2d(1, 1, s).start()
    for i in (1, 2):
        xearly(i).wait_recv()
        dearly(i).start()
    project(1, 1)
    project(1, 2)
    xearly(3).wait_recv()
    dearly(3).start()
    finish(0, 1)
    project(1, 3)
    for s in (6, 7):
        xcopy(1, s).wait_recv()
        d2d(1, 1, s).start()
    att = attention(pos_ref, kc, vc, acc, rope)
    def part_slices(i):
        zs = piece_z[i]
        j = jnp.where(zs == 0, 0, jnp.where(zs == 3, 1, zs + 1))
        return pl.ds(2 * j, 2)

    def part(i, d):
        return remote(part_ref.at[part_slices(i)], parts_in.at[d - 1, part_slices(i)],
                      p_send, p_recv, (rep, (tp + d) % 8))

    for i in range(4):
        for xp in range(2):
            d2d_piece_done(1, xp, i)
        both = jnp.dot(att, go[piece_z[i]].reshape(512, 1152), preferred_element_type=jnp.float32)
        both = both.astype(jnp.bfloat16)
        first = part_slices(i).start
        part_ref[first] = both[:, :576]
        part_ref[first + 1] = both[:, 576:]
        for d in (6, 2, 5, 7, 1, 3, 4):
            part(i, d).start()
    settle(parts_in, p_recv)
    sum_and_norm(part_ref, post_ref, out_ref, parts_in)
    settle(parts_in, p_send)
    settle(s1a.at[pl.ds(0, 3)], a_send.at[1])

    @pl.when(ends)
    def _():
        settle(s1a.at[0, pl.ds(0, qrows)], a_send.at[0])

    @pl.when(zdest == z)
    def _():
        settle(s1o.at[pl.ds(0, 31)], o_send)

    @pl.when(zdest != z)
    def _():
        settle(s1o, o_send)

    settle(go.at[0, pl.ds(0, 3)], z_send.at[0])
    settle(gq.at[0, pl.ds(0, 3)], z_send.at[1])
    settle(gq.at[0, pl.ds(0, 3), pl.ds(0, 2 * late)], z_send.at[2])
    settle(gq.at[0, 0], x_send.at[0])
    settle(go.at[0], x_send.at[1])
    settle(gq.at[0, pl.ds(0, 3), pl.ds(0, early)], x_send.at[2])
    for i in range(4):
        settle(gathered[i // 2].at[0], d_send.at[i])


def in_hbm(x):
    return pltpu.with_memory_space_constraint(x, pltpu.HBM)


def gather_and_attend(q, k, v, o, hidden, gain, key_cache, value_cache, positions, post_gain):
    bf, f32 = jnp.bfloat16, jnp.float32
    dma = pltpu.SemaphoreType.DMA
    vmem = pltpu.VMEM
    return pl.pallas_call(
        gather_kernel,
        out_shape=(jax.ShapeDtypeStruct((4, 4, 1152, 256), bf),
                   jax.ShapeDtypeStruct((4, 4, 128, 1152), bf),
                   jax.ShapeDtypeStruct((4, 576), bf)),
        in_specs=[pl.BlockSpec(memory_space=pltpu.HBM)] * 10,
        out_specs=[pl.BlockSpec(memory_space=vmem)] * 3,
        scratch_shapes=[
            vmem(hidden.shape, bf), vmem(gain.shape, f32), vmem(key_cache.shape, bf),
            vmem(value_cache.shape, bf), pltpu.SMEM((4,), jnp.int32), vmem(post_gain.shape, f32),
            vmem((4, 4, 1152), bf), vmem((4, 4, 256), f32), vmem((2, 4, 128), f32),
            vmem((8, 4, 576), bf), vmem((7, 8, 4, 576), bf),
            vmem((4, 64, 1152), bf), vmem((256, 1152), bf), vmem((32, 36, 128), bf),
            vmem((1152, 128), f32),
            dma((2,)), dma((4,)), dma, dma, dma, dma, dma((3,)), dma((18,)), dma((3,)), dma((13,)),
            dma((4,)), dma((16,)), pltpu.SemaphoreType.REGULAR, dma((6,)), dma, dma,
        ],
        compiler_params=pltpu.CompilerParams(
            has_side_effects=True, collective_id=0, vmem_limit_bytes=16 * 1024 * 1024),
        name="gather_and_attend",
    )(*(in_hbm(x) for x in (q, k, v, o, hidden, gain, key_cache, value_cache, positions, post_gain)))


def prepare(pos_ref, hidden_ref, gain_ref, nrm, acc, rope):
    f32 = jnp.float32
    hid = hidden_ref[...].astype(f32)
    mean_square = jnp.mean(hid * hid, axis=-1, keepdims=True)
    gain = gain_ref[...].reshape(1, -1)
    normed = (hid * lax.rsqrt(mean_square + 1e-06) * gain).astype(jnp.bfloat16)
    for zs in range(4):
        nrm[zs] = normed[:, zs * 1152:(zs + 1) * 1152]
    acc[...] = jnp.zeros_like(acc)
    row = lax.broadcasted_iota(jnp.int32, (4, 128), 0)
    posf = jnp.zeros((4, 128), f32)
    for b in range(4):
        posf = jnp.where(row == b, pos_ref[b].astype(f32), posf)
    lane = lax.broadcasted_iota(jnp.int32, (4, 128), 1)
    angle = posf * jnp.exp((lane % 64).astype(f32) * (-2.0 / 128 * np.log(10000.0)))
    rope[0] = jnp.cos(angle)
    rope[1] = jnp.where(lane < 64, -jnp.sin(angle), jnp.sin(angle))


def attention(pos_ref, kc, vc, acc, rope):
    f32, bf = jnp.float32, jnp.bfloat16
    proj = []
    for gs in range(4):
        both = acc[gs]
        proj += [both[:, :128], both[:, 128:]]
    cosine, sine = rope[0], rope[1]

    def rotate(x):
        swapped = jnp.concatenate([x[:, 64:], x[:, :64]], axis=1)
        return (x * cosine + swapped * sine).astype(bf).astype(f32)

    query = jnp.concatenate([rotate(x) for x in proj[:4]], axis=0)
    keys = [rotate(x) for x in proj[4:6]]
    vals = [x.astype(bf).astype(f32) for x in proj[6:8]]
    keys_new = jnp.concatenate([keys[0], keys[0], keys[1], keys[1]], axis=0)
    values_new = jnp.concatenate([vals[0], vals[0], vals[1], vals[1]], axis=0)
    qb = query.astype(bf)
    length = kc.shape[2]
    r = lax.broadcasted_iota(jnp.int32, (16, length), 0)
    slot = lax.broadcasted_iota(jnp.int32, (16, length), 1)
    owner = (r // 8) * 4 + r % 4
    scores = jnp.zeros((16, length), f32)
    limit = jnp.zeros((16, length), jnp.int32)
    for kv in range(2):
        for b in range(4):
            s = lax.dot_general(qb, kc[b, kv], (((1,), (1,)), ((), ())), preferred_element_type=f32)
            scores = jnp.where(owner == kv * 4 + b, s, scores)
    for b in range(4):
        limit = jnp.where(r % 4 == b, pos_ref[b], limit)
    capped = soft_cap * jnp.tanh(scores * score_scale / soft_cap)
    raw = jnp.where(slot < limit, jnp.exp(capped), 0.0)
    self_score = jnp.sum(query * keys_new, axis=-1, keepdims=True) * score_scale
    self_raw = jnp.exp(soft_cap * jnp.tanh(self_score / soft_cap))
    denom = jnp.sum(raw, axis=-1, keepdims=True) + self_raw
    weights = (raw / denom).astype(bf).astype(f32)
    mixed = (self_raw / denom).astype(bf).astype(f32) * values_new
    for kv in range(2):
        for b in range(4):
            w = jnp.where(owner == kv * 4 + b, weights, 0.0).astype(bf)
            mixed += jnp.dot(w, vc[b, kv], preferred_element_type=f32)
    return jnp.concatenate([mixed[i * 4:(i + 1) * 4] for i in range(4)], axis=1).astype(bf)


def write_kernel(gq, go, small, joined_ref, wo_ref, small_ref, out_sem):
    pltpu.make_async_copy(small, small_ref, out_sem.at[2]).start()
    for zs in range(4):
        for gs in range(4):
            pltpu.make_async_copy(
                gq.at[zs, gs], joined_ref.at[pl.ds(zs * 1152, 1152), pl.ds(gs * 256, 256)],
                out_sem.at[0]).start()
            pltpu.make_async_copy(
                go.at[zs, gs], wo_ref.at[pl.ds(gs * 128, 128), pl.ds(WO_SLICE[zs] * 1152, 1152)],
                out_sem.at[1]).start()
    pltpu.make_async_copy(joined_ref, joined_ref, out_sem.at[0]).wait()
    pltpu.make_async_copy(wo_ref, wo_ref, out_sem.at[1]).wait()
    pltpu.make_async_copy(small, small_ref, out_sem.at[2]).wait()


def write_out(gq, go, small):
    bf = jnp.bfloat16
    vmem = pl.BlockSpec(memory_space=pltpu.VMEM)
    hbm = pl.BlockSpec(memory_space=pltpu.HBM)
    return pl.pallas_call(
        write_kernel,
        out_shape=(jax.ShapeDtypeStruct((4608, 1024), bf), jax.ShapeDtypeStruct((512, 4608), bf),
                   jax.ShapeDtypeStruct(small.shape, bf)),
        in_specs=[vmem, vmem, vmem],
        out_specs=[hbm, hbm, hbm],
        scratch_shapes=[pltpu.SemaphoreType.DMA((3,))],
        compiler_params=pltpu.CompilerParams(vmem_limit_bytes=16 * 1024 * 1024),
        name="write_out",
    )(gq, go, small)


def sum_and_norm(part_ref, gain_ref, out_ref, parts_in):
    f32 = jnp.float32
    tp = lax.axis_index("tp")
    total = part_ref[...].astype(f32)
    own = part_ref[tp].astype(f32)
    for d in range(7):
        total += parts_in[d].astype(f32)
        own += parts_in[d, tp].astype(f32)
    square = jnp.sum(jnp.sum(total * total, axis=0), axis=-1, keepdims=True)
    scale = lax.rsqrt(square / 4608.0 + 1e-06)
    out_ref[...] = (own * scale * gain_ref[...].reshape(1, -1)).astype(jnp.bfloat16)


def body(
    hidden, positions, key_cache, value_cache, norm_gain, q_proj, k_proj, v_proj, o_proj, post_gain
):
    gq, go, attn_out = gather_and_attend(
        q_proj, k_proj, v_proj, o_proj, hidden, norm_gain, key_cache, value_cache, positions, post_gain)
    return write_out(gq, go, attn_out)


def solution(mesh):
    in_specs = (
        P("rep", None),
        P("rep"),
        P("rep", "tp", None, None),
        P("rep", "tp", None, None),
        P(),
        P(("rep", "tp"), None),
        P(("rep", "tp"), None),
        P(("rep", "tp"), None),
        P(("rep", "tp"), None),
        P("tp"),
    )
    out_specs = (P(None, "tp"), P("tp", None), P("rep", "tp"))
    return jax.shard_map(body, mesh=mesh, in_specs=in_specs, out_specs=out_specs, check_vma=False)
```

```python
import jax
import jax.numpy as jnp
import numpy as np
from jax import lax
from jax.experimental import pallas as pl
from jax.experimental.pallas import tpu as pltpu
from jax.sharding import PartitionSpec as P

score_scale = 144.0 ** (-0.5)
soft_cap = 50.0
MESH = pl.DeviceIdType.MESH
WO_SLICE = (0, 2, 3, 1)


def remote(src, dst, ssem, rsem, device):
    return pltpu.make_async_remote_copy(
        src_ref=src, dst_ref=dst, send_sem=ssem, recv_sem=rsem, device_id=device,
        device_id_type=MESH)


def settle(ref, sem):
    pltpu.make_async_copy(ref, ref, sem).wait()


def gather_kernel(q_ref, k_ref, v_ref, o_ref, hidden_hbm, gain_hbm, kc_hbm, vc_hbm, pos_hbm, post_hbm,
                  gq, go, out_ref,
                  hidden_ref, gain_ref, kc, vc, pos_ref, post_ref, nrm, acc, rope, part_ref, parts_in, s1a, s1q, s1o, so,
                  a_send, a_recv, b_send, q_recv, o_send, o_recv, z_send, z_recv, x_send, x_recv,
                  d_send, d_recv, row_sem, in_sem, p_send, p_recv):
    rep = lax.axis_index("rep")
    tp = lax.axis_index("tp")
    h = rep // 8
    z = (rep // 2) % 4
    core = rep % 2
    lo = tp // 4
    g = 2 * h + core
    gpar = 2 * (1 - h) + core
    zp = (z + 1) % 4
    zm = (z + 3) % 4
    zo = (z + 2) % 4
    gathered = (gq, go)
    halves = (gq.shape[2] // 2, go.shape[2] // 2)
    piece_z = (z, zm, zp, zo)
    piece_g = (g, gpar)

    def place(h_, z_, c_):
        return h_ * 8 + z_ * 2 + c_

    barrier = pltpu.get_barrier_semaphore()
    pair = z + 1 - 2 * (z % 2)
    greeted = [((z_ + 2) % 4, h_, core, tp_) for z_ in (pair, z)
               for h_, tp_ in ((1 - h, (tp + 4) % 8), (h, tp))]
    greeted += [(z_, (g + a) % 4 // 2, (g + a) % 2, (tp + b) % 8) for z_ in (pair, z)
                for a in (2, 3, 1, 0) for b in (6, 2, 5, 7, 1, 3, 4, 0)][:-1]
    for z_, h_, c_, tp_ in greeted:
        pl.semaphore_signal(barrier, inc=1, device_id=(place(h_, z_, c_), tp_), device_id_type=MESH)
    pl.semaphore_wait(barrier, len(greeted))

    zdest = 2 * h + z // 2
    zdest = jnp.where(zdest == 0, 0, jnp.where(zdest == 1, 3, zdest - 1))
    slot = (rep % 4) * 8 + tp

    def o_slice(i, j):
        p = (tp + i) % 8
        gd = (g + j) % 4
        src = o_ref.at[:, pl.ds(pl.multiple_of(p * 512 + gd * 128, 128), 128)]
        return src, s1o.at[slot], place(gd // 2, zdest, gd % 2), p, o_send, o_recv

    def exchange(first, src, dst, dest_rep, dest_tp, ssem, rsem):
        if not first:
            remote(src, dst, ssem, rsem, (dest_rep, dest_tp)).start()
            return
        own = jnp.logical_and(dest_rep == rep, dest_tp == tp)

        @pl.when(own)
        def _():
            pltpu.make_async_copy(src, dst, rsem).start()

        @pl.when(jnp.logical_not(own))
        def _():
            remote(src, dst, ssem, rsem, (dest_rep, dest_tp)).start()

    for p in range(8):
        for gd in range(4):
            exchange(p == 0 and gd == 0, *o_slice(p, gd))

    width = s1q.shape[1]
    qrows, krows = q_ref.shape[0], k_ref.shape[0]
    parts = ((q_ref, 0, qrows), (k_ref, qrows, krows), (v_ref, qrows + krows, krows))

    first_x = jnp.logical_and(h == 0, lo == 0)
    last_x = jnp.logical_and(h == 1, lo == 1)

    def along_z(dist, part):
        zd = (z + dist) % 4
        ref, row, rows = parts[part]
        src = ref.at[:, pl.ds(pl.multiple_of(zd * width, width), width)]
        if part == 0:
            away, there, to_h, to_tp = last_x, qrows, 0, tp % 4
        else:
            away, there, to_h, to_tp = first_x, row - qrows, 1, 4 + tp % 4
        row = pl.multiple_of(jnp.where(away, there, row), krows)
        dst = s1a.at[z, pl.ds(row, rows)]
        device = (place(jnp.where(away, to_h, h), zd, core), jnp.where(away, to_tp, tp))
        return away, src, dst, remote(src, dst, a_send.at[min(dist, 1)], a_recv.at[dist], device)

    for dist in (2, 1, 3, 0):
        for part in range(3):
            away, src, dst, copy = along_z(dist, part)
            if dist == 0:
                pl.when(away)(copy.start)
                pl.when(jnp.logical_not(away))(
                    pltpu.make_async_copy(src, dst, a_recv.at[0]).start)
            else:
                copy.start()

    local = [pltpu.make_async_copy(src, dst, in_sem.at[i]) for i, (src, dst) in enumerate(
        ((hidden_hbm, hidden_ref), (gain_hbm, gain_ref), (pos_hbm, pos_ref), (post_hbm, post_ref),
         (kc_hbm, kc), (vc_hbm, vc)))]
    for copy in local:
        copy.start()
    for copy in local:
        copy.wait()
    prepare(pos_ref, hidden_ref, gain_ref, nrm, acc, rope)

    def to_owners(dist):
        zs = (tp + dist) % 4

        def message(when, row, rows, dest, first, block):
            dst = s1q.at[pl.ds(pl.multiple_of(first, rows), rows)]

            @pl.when(when)
            def _():
                exchange(dist == 0, s1a.at[zs, pl.ds(row, rows)], dst, dest, block, b_send, q_recv)

        y = tp % 4
        message(jnp.logical_not(last_x), 0, qrows, place(0, z, core), tp * qrows, h * 4 + zs)
        message(first_x, qrows, qrows, place(0, z, core), (4 + y) * qrows, 4 + zs)
        for i in range(2):
            message(jnp.logical_not(first_x), qrows + i * krows, krows, place(1, z, i),
                    core * 128 + tp * krows, h * 4 + zs)
            message(last_x, i * krows, krows, place(1, z, i), core * 128 + y * krows, zs)

    for dist in (0, 2, 1, 3):
        zs = (tp + dist) % 4
        came = s1a.at[zs]
        pltpu.make_async_copy(came, came, a_recv.at[(z + 4 - zs) % 4]).wait()
        to_owners(dist)

    def chunk(a, zs, gs, half):
        return gathered[a].at[zs, gs, pl.ds(half * halves[a], halves[a])]

    early = 128
    late = (gq.shape[2] - early) // 2

    def ring_chunk(a, xp, zs, half):
        if a == 0 and xp == 1:
            return gq.at[zs, gpar, pl.ds(early + half * late, late)]
        return chunk(a, zs, piece_g[xp], half)

    def early_rows(i, gs):
        return gq.at[piece_z[i], gs, pl.ds(0, early)]

    def xearly(i):
        c = early_rows(i, g)
        return remote(c, c, x_send.at[2], x_recv.at[1 + i], (place(1 - h, z, core), tp))

    def dearly(i):
        c = early_rows(i, gpar)
        return remote(c, c, d_send.at[1], d_recv.at[4 + i], (place(h, z, 1 - core), tp))

    def d2d(a, xp, s):
        if s < 2:
            c = chunk(a, z, piece_g[xp], s)
        else:
            c = ring_chunk(a, xp, piece_z[s // 2], s % 2)
        i = a * 2 + xp
        return remote(c, c, d_send.at[i], d_recv.at[i * 4 + s // 2], (place(h, z, 1 - core), tp))

    def d2d_piece_done(a, xp, i):
        settle(gathered[a].at[piece_z[i], 0], d_recv.at[(a * 2 + xp) * 4 + i])

    up = (place(h, zp, core), tp)
    down = (place(h, zm, core), tp)

    ring = {(1, 0): 0, (0, 0): 1, (0, 1): 2}

    def zcopy(a, xp, i):
        zs, half, to = ((z, 0, up), (z, 1, up), (z, 0, down), (z, 1, down), (zm, 0, up), (zp, 1, down))[i]
        c = ring_chunk(a, xp, zs, half)
        j = ring[a, xp]
        return remote(c, c, z_send.at[j], z_recv.at[j * 6 + i], to)

    def xcopy(a, s):
        c = chunk(a, piece_z[s // 2], g, s % 2)
        return remote(c, c, x_send.at[a], x_recv.at[a * 5 + s], (place(1 - h, z, core), tp))

    def arrived(a, xp, s):
        d2d(a, xp, s).start()

    def launch(a, xp):
        for i in (0, 3, 1, 2):
            zcopy(a, xp, i).start()
        arrived(a, xp, 0)
        arrived(a, xp, 1)

    def forward(a, xp):
        zcopy(a, xp, 0).wait_recv()
        zcopy(a, xp, 4).start()
        arrived(a, xp, 2)
        zcopy(a, xp, 3).wait_recv()
        zcopy(a, xp, 5).start()
        arrived(a, xp, 5)

    def take(a, xp):
        zcopy(a, xp, 1).wait_recv()
        arrived(a, xp, 3)
        zcopy(a, xp, 2).wait_recv()
        arrived(a, xp, 4)

    def finish(a, xp):
        zcopy(a, xp, 4).wait_recv()
        arrived(a, xp, 6)
        zcopy(a, xp, 5).wait_recv()
        arrived(a, xp, 7)

    pltpu.make_async_copy(s1o, s1o, o_recv).wait()
    nrow = s1o.shape[1]
    for i in range(32):
        so[i * nrow:(i + 1) * nrow, :] = s1o[i].astype(jnp.float32)
    for b in range(9):
        go[z, g, :, b * 128:(b + 1) * 128] = so[b * 128:(b + 1) * 128, :].T.astype(jnp.bfloat16)
    launch(1, 0)
    for s in range(2):
        xcopy(1, s).start()
    def slices_left(when, rows):
        @pl.when(when)
        def _():
            settle(s1q.at[pl.ds(0, rows)], b_send)

    ends = jnp.logical_or(first_x, last_x)
    slices_left(first_x, s1q.shape[0] - qrows)
    slices_left(last_x, s1q.shape[0] - krows)
    slices_left(jnp.logical_not(ends), s1q.shape[0])
    for i in range(1, 8):
        peer = (2 * h + lo + i // 2) % 4
        pl.semaphore_signal(
            row_sem, inc=1, device_id_type=MESH,
            device_id=(place(peer // 2, z, (core + i) % 2), (peer % 2) * 4 + tp % 4))
    forward(1, 0)
    pltpu.make_async_copy(s1q, s1q, q_recv).wait()
    for b in range(9):
        for c in range(2):
            tile = s1q[c * 128:(c + 1) * 128, b * 128:(b + 1) * 128].astype(jnp.float32)
            gq[z, g, b * 128:(b + 1) * 128, c * 128:(c + 1) * 128] = tile.T.astype(jnp.bfloat16)
    launch(0, 0)
    pl.semaphore_wait(row_sem, 7)
    for s in range(2):
        xcopy(0, s).start()
    take(1, 0)
    for s in (2, 5, 3, 4):
        xcopy(1, s).start()
    forward(0, 0)
    take(0, 0)
    for i in (1, 2):
        xearly(i).start()
    for s in range(2):
        xcopy(0, s).wait_recv()
    launch(0, 1)
    finish(1, 0)
    finish(0, 0)
    xearly(3).start()
    for s in (6, 7):
        xcopy(1, s).start()

    def project(xp, i):
        def add(gs):
            acc[gs] += jnp.dot(nrm[piece_z[i]], gq[piece_z[i], gs], preferred_element_type=jnp.float32)

        add(piece_g[xp])
        d2d_piece_done(0, xp, i)
        add(piece_g[xp] + 1 - 2 * core)

    for i in range(4):
        project(0, i)
    forward(0, 1)
    take(0, 1)
    project(1, 0)
    for s in (0, 1, 2, 5, 3, 4):
        xcopy(1, s).wait_recv()
        d2d(1, 1, s).start()
    for i in (1, 2):
        xearly(i).wait_recv()
        dearly(i).start()
    project(1, 1)
    project(1, 2)
    xearly(3).wait_recv()
    dearly(3).start()
    finish(0, 1)
    project(1, 3)
    for s in (6, 7):
        xcopy(1, s).wait_recv()
        d2d(1, 1, s).start()
    att = attention(pos_ref, kc, vc, acc, rope)
    def part_slices(i):
        zs = piece_z[i]
        j = jnp.where(zs == 0, 0, jnp.where(zs == 3, 1, zs + 1))
        return pl.ds(2 * j, 2)

    def part(i, d):
        return remote(part_ref.at[part_slices(i)], parts_in.at[d - 1, part_slices(i)],
                      p_send, p_recv, (rep, (tp + d) % 8))

    for i in range(4):
        for xp in range(2):
            d2d_piece_done(1, xp, i)
        both = jnp.dot(att, go[piece_z[i]].reshape(512, 1152), preferred_element_type=jnp.float32)
        both = both.astype(jnp.bfloat16)
        first = part_slices(i).start
        part_ref[first] = both[:, :576]
        part_ref[first + 1] = both[:, 576:]
        for d in (6, 2, 5, 7, 1, 3, 4):
            part(i, d).start()
    settle(parts_in, p_recv)
    sum_and_norm(part_ref, post_ref, out_ref, parts_in)
    settle(parts_in, p_send)
    settle(s1a.at[pl.ds(0, 3)], a_send.at[1])

    @pl.when(ends)
    def _():
        settle(s1a.at[0, pl.ds(0, qrows)], a_send.at[0])

    @pl.when(zdest == z)
    def _():
        settle(s1o.at[pl.ds(0, 31)], o_send)

    @pl.when(zdest != z)
    def _():
        settle(s1o, o_send)

    settle(go.at[0, pl.ds(0, 3)], z_send.at[0])
    settle(gq.at[0, pl.ds(0, 3)], z_send.at[1])
    settle(gq.at[0, pl.ds(0, 3), pl.ds(0, 2 * late)], z_send.at[2])
    settle(gq.at[0, 0], x_send.at[0])
    settle(go.at[0], x_send.at[1])
    settle(gq.at[0, pl.ds(0, 3), pl.ds(0, early)], x_send.at[2])
    for i in range(4):
        settle(gathered[i // 2].at[0], d_send.at[i])


def in_hbm(x):
    return pltpu.with_memory_space_constraint(x, pltpu.HBM)


def gather_and_attend(q, k, v, o, hidden, gain, key_cache, value_cache, positions, post_gain):
    bf, f32 = jnp.bfloat16, jnp.float32
    dma = pltpu.SemaphoreType.DMA
    vmem = pltpu.VMEM
    return pl.pallas_call(
        gather_kernel,
        out_shape=(jax.ShapeDtypeStruct((4, 4, 1152, 256), bf),
                   jax.ShapeDtypeStruct((4, 4, 128, 1152), bf),
                   jax.ShapeDtypeStruct((4, 576), bf)),
        in_specs=[pl.BlockSpec(memory_space=pltpu.HBM)] * 10,
        out_specs=[pl.BlockSpec(memory_space=vmem)] * 3,
        scratch_shapes=[
            vmem(hidden.shape, bf), vmem(gain.shape, f32), vmem(key_cache.shape, bf),
            vmem(value_cache.shape, bf), pltpu.SMEM((4,), jnp.int32), vmem(post_gain.shape, f32),
            vmem((4, 4, 1152), bf), vmem((4, 4, 256), f32), vmem((2, 4, 128), f32),
            vmem((8, 4, 576), bf), vmem((7, 8, 4, 576), bf),
            vmem((4, 64, 1152), bf), vmem((256, 1152), bf), vmem((32, 36, 128), bf),
            vmem((1152, 128), f32),
            dma((2,)), dma((4,)), dma, dma, dma, dma, dma((3,)), dma((18,)), dma((3,)), dma((13,)),
            dma((4,)), dma((16,)), pltpu.SemaphoreType.REGULAR, dma((6,)), dma, dma,
        ],
        compiler_params=pltpu.CompilerParams(
            has_side_effects=True, collective_id=0, vmem_limit_bytes=16 * 1024 * 1024),
        name="gather_and_attend",
    )(*(in_hbm(x) for x in (q, k, v, o, hidden, gain, key_cache, value_cache, positions, post_gain)))


def prepare(pos_ref, hidden_ref, gain_ref, nrm, acc, rope):
    f32 = jnp.float32
    hid = hidden_ref[...].astype(f32)
    mean_square = jnp.mean(hid * hid, axis=-1, keepdims=True)
    gain = gain_ref[...].reshape(1, -1)
    normed = (hid * lax.rsqrt(mean_square + 1e-06) * gain).astype(jnp.bfloat16)
    for zs in range(4):
        nrm[zs] = normed[:, zs * 1152:(zs + 1) * 1152]
    acc[...] = jnp.zeros_like(acc)
    row = lax.broadcasted_iota(jnp.int32, (4, 128), 0)
    posf = jnp.zeros((4, 128), f32)
    for b in range(4):
        posf = jnp.where(row == b, pos_ref[b].astype(f32), posf)
    lane = lax.broadcasted_iota(jnp.int32, (4, 128), 1)
    angle = posf * jnp.exp((lane % 64).astype(f32) * (-2.0 / 128 * np.log(10000.0)))
    rope[0] = jnp.cos(angle)
    rope[1] = jnp.where(lane < 64, -jnp.sin(angle), jnp.sin(angle))


def attention(pos_ref, kc, vc, acc, rope):
    f32, bf = jnp.float32, jnp.bfloat16
    proj = []
    for gs in range(4):
        both = acc[gs]
        proj += [both[:, :128], both[:, 128:]]
    cosine, sine = rope[0], rope[1]

    def rotate(x):
        swapped = jnp.concatenate([x[:, 64:], x[:, :64]], axis=1)
        return (x * cosine + swapped * sine).astype(bf).astype(f32)

    query = jnp.concatenate([rotate(x) for x in proj[:4]], axis=0)
    keys = [rotate(x) for x in proj[4:6]]
    vals = [x.astype(bf).astype(f32) for x in proj[6:8]]
    keys_new = jnp.concatenate([keys[0], keys[0], keys[1], keys[1]], axis=0)
    values_new = jnp.concatenate([vals[0], vals[0], vals[1], vals[1]], axis=0)
    qb = query.astype(bf)
    length = kc.shape[2]
    r = lax.broadcasted_iota(jnp.int32, (16, length), 0)
    slot = lax.broadcasted_iota(jnp.int32, (16, length), 1)
    owner = (r // 8) * 4 + r % 4
    scores = jnp.zeros((16, length), f32)
    limit = jnp.zeros((16, length), jnp.int32)
    for kv in range(2):
        for b in range(4):
            s = lax.dot_general(qb, kc[b, kv], (((1,), (1,)), ((), ())), preferred_element_type=f32)
            scores = jnp.where(owner == kv * 4 + b, s, scores)
    for b in range(4):
        limit = jnp.where(r % 4 == b, pos_ref[b], limit)
    capped = soft_cap * jnp.tanh(scores * score_scale / soft_cap)
    raw = jnp.where(slot < limit, jnp.exp(capped), 0.0)
    self_score = jnp.sum(query * keys_new, axis=-1, keepdims=True) * score_scale
    self_raw = jnp.exp(soft_cap * jnp.tanh(self_score / soft_cap))
    denom = jnp.sum(raw, axis=-1, keepdims=True) + self_raw
    weights = (raw / denom).astype(bf).astype(f32)
    mixed = (self_raw / denom).astype(bf).astype(f32) * values_new
    for kv in range(2):
        for b in range(4):
            w = jnp.where(owner == kv * 4 + b, weights, 0.0).astype(bf)
            mixed += jnp.dot(w, vc[b, kv], preferred_element_type=f32)
    return jnp.concatenate([mixed[i * 4:(i + 1) * 4] for i in range(4)], axis=1).astype(bf)


def write_kernel(gq, go, small, joined_ref, wo_ref, small_ref, out_sem):
    pltpu.make_async_copy(small, small_ref, out_sem.at[2]).start()
    for zs in range(4):
        for gs in range(4):
            pltpu.make_async_copy(
                gq.at[zs, gs], joined_ref.at[pl.ds(zs * 1152, 1152), pl.ds(gs * 256, 256)],
                out_sem.at[0]).start()
            pltpu.make_async_copy(
                go.at[zs, gs], wo_ref.at[pl.ds(gs * 128, 128), pl.ds(WO_SLICE[zs] * 1152, 1152)],
                out_sem.at[1]).start()
    pltpu.make_async_copy(joined_ref, joined_ref, out_sem.at[0]).wait()
    pltpu.make_async_copy(wo_ref, wo_ref, out_sem.at[1]).wait()
    pltpu.make_async_copy(small, small_ref, out_sem.at[2]).wait()


def write_out(gq, go, small):
    bf = jnp.bfloat16
    vmem = pl.BlockSpec(memory_space=pltpu.VMEM)
    hbm = pl.BlockSpec(memory_space=pltpu.HBM)
    return pl.pallas_call(
        write_kernel,
        out_shape=(jax.ShapeDtypeStruct((4608, 1024), bf), jax.ShapeDtypeStruct((512, 4608), bf),
                   jax.ShapeDtypeStruct(small.shape, bf)),
        in_specs=[vmem, vmem, vmem],
        out_specs=[hbm, hbm, hbm],
        scratch_shapes=[pltpu.SemaphoreType.DMA((3,))],
        compiler_params=pltpu.CompilerParams(vmem_limit_bytes=16 * 1024 * 1024),
        name="write_out",
    )(gq, go, small)


def sum_and_norm(part_ref, gain_ref, out_ref, parts_in):
    f32 = jnp.float32
    tp = lax.axis_index("tp")
    total = part_ref[...].astype(f32)
    own = part_ref[tp].astype(f32)
    for d in range(7):
        total += parts_in[d].astype(f32)
        own += parts_in[d, tp].astype(f32)
    square = jnp.sum(jnp.sum(total * total, axis=0), axis=-1, keepdims=True)
    scale = lax.rsqrt(square / 4608.0 + 1e-06)
    out_ref[...] = (own * scale * gain_ref[...].reshape(1, -1)).astype(jnp.bfloat16)


def body(
    hidden, positions, key_cache, value_cache, norm_gain, q_proj, k_proj, v_proj, o_proj, post_gain
):
    gq, go, attn_out = gather_and_attend(
        q_proj, k_proj, v_proj, o_proj, hidden, norm_gain, key_cache, value_cache, positions, post_gain)
    return write_out(gq, go, attn_out)


def solution(mesh):
    in_specs = (
        P("rep", None),
        P("rep"),
        P("rep", "tp", None, None),
        P("rep", "tp", None, None),
        P(),
        P(("rep", "tp"), None),
        P(("rep", "tp"), None),
        P(("rep", "tp"), None),
        P(("rep", "tp"), None),
        P("tp"),
    )
    out_specs = (P(None, "tp"), P("tp", None), P("rep", "tp"))
    return jax.shard_map(body, mesh=mesh, in_specs=in_specs, out_specs=out_specs, check_vma=False)
```

```python
import jax
import jax.numpy as jnp
import numpy as np
from jax import lax
from jax.experimental import pallas as pl
from jax.experimental.pallas import tpu as pltpu
from jax.sharding import PartitionSpec as P

score_scale = 144.0 ** (-0.5)
soft_cap = 50.0
MESH = pl.DeviceIdType.MESH
WO_SLICE = (0, 2, 3, 1)


def remote(src, dst, ssem, rsem, device):
    return pltpu.make_async_remote_copy(
        src_ref=src, dst_ref=dst, send_sem=ssem, recv_sem=rsem, device_id=device,
        device_id_type=MESH)


def settle(ref, sem):
    pltpu.make_async_copy(ref, ref, sem).wait()


def gather_kernel(q_ref, k_ref, v_ref, o_ref, hidden_hbm, gain_hbm, kc_hbm, vc_hbm, pos_hbm, post_hbm,
                  gq, go, out_ref,
                  hidden_ref, gain_ref, kc, vc, pos_ref, post_ref, nrm, acc, rope, part_ref, parts_in, s1a, s1q, s1o, so,
                  a_send, a_recv, b_send, q_recv, o_send, o_recv, z_send, z_recv, x_send, x_recv,
                  d_send, d_recv, row_sem, in_sem, p_send, p_recv):
    rep = lax.axis_index("rep")
    tp = lax.axis_index("tp")
    h = rep // 8
    z = (rep // 2) % 4
    core = rep % 2
    lo = tp // 4
    g = 2 * h + core
    gpar = 2 * (1 - h) + core
    zp = (z + 1) % 4
    zm = (z + 3) % 4
    zo = (z + 2) % 4
    gathered = (gq, go)
    halves = (gq.shape[2] // 2, go.shape[2] // 2)
    piece_z = (z, zm, zp, zo)
    piece_g = (g, gpar)

    def place(h_, z_, c_):
        return h_ * 8 + z_ * 2 + c_

    barrier = pltpu.get_barrier_semaphore()
    pair = z + 1 - 2 * (z % 2)
    greeted = [((z_ + 2) % 4, h_, core, tp_) for z_ in (pair, z)
               for h_, tp_ in ((1 - h, (tp + 4) % 8), (h, tp))]
    greeted += [(z_, (g + a) % 4 // 2, (g + a) % 2, (tp + b) % 8) for z_ in (pair, z)
                for a in (2, 3, 1, 0) for b in (6, 2, 5, 7, 1, 3, 4, 0)][:-1]
    for z_, h_, c_, tp_ in greeted:
        pl.semaphore_signal(barrier, inc=1, device_id=(place(h_, z_, c_), tp_), device_id_type=MESH)
    pl.semaphore_wait(barrier, len(greeted))

    zdest = 2 * h + z // 2
    zdest = jnp.where(zdest == 0, 0, jnp.where(zdest == 1, 3, zdest - 1))
    slot = (rep % 4) * 8 + tp

    def o_slice(i, j):
        p = (tp + i) % 8
        gd = (g + j) % 4
        src = o_ref.at[:, pl.ds(pl.multiple_of(p * 512 + gd * 128, 128), 128)]
        return src, s1o.at[slot], place(gd // 2, zdest, gd % 2), p, o_send, o_recv

    def exchange(first, src, dst, dest_rep, dest_tp, ssem, rsem):
        if not first:
            remote(src, dst, ssem, rsem, (dest_rep, dest_tp)).start()
            return
        own = jnp.logical_and(dest_rep == rep, dest_tp == tp)

        @pl.when(own)
        def _():
            pltpu.make_async_copy(src, dst, rsem).start()

        @pl.when(jnp.logical_not(own))
        def _():
            remote(src, dst, ssem, rsem, (dest_rep, dest_tp)).start()

    for p in range(8):
        for gd in range(4):
            exchange(p == 0 and gd == 0, *o_slice(p, gd))

    width = s1q.shape[1]
    qrows, krows = q_ref.shape[0], k_ref.shape[0]
    parts = ((q_ref, 0, qrows), (k_ref, qrows, krows), (v_ref, qrows + krows, krows))

    first_x = jnp.logical_and(h == 0, lo == 0)
    last_x = jnp.logical_and(h == 1, lo == 1)

    def along_z(dist, part):
        zd = (z + dist) % 4
        ref, row, rows = parts[part]
        src = ref.at[:, pl.ds(pl.multiple_of(zd * width, width), width)]
        if part == 0:
            away, there, to_h, to_tp = last_x, qrows, 0, tp % 4
        else:
            away, there, to_h, to_tp = first_x, row - qrows, 1, 4 + tp % 4
        row = pl.multiple_of(jnp.where(away, there, row), krows)
        dst = s1a.at[z, pl.ds(row, rows)]
        device = (place(jnp.where(away, to_h, h), zd, core), jnp.where(away, to_tp, tp))
        return away, src, dst, remote(src, dst, a_send.at[min(dist, 1)], a_recv.at[dist], device)

    for dist in (2, 1, 3, 0):
        for part in range(3):
            away, src, dst, copy = along_z(dist, part)
            if dist == 0:
                pl.when(away)(copy.start)
                pl.when(jnp.logical_not(away))(
                    pltpu.make_async_copy(src, dst, a_recv.at[0]).start)
            else:
                copy.start()

    local = [pltpu.make_async_copy(src, dst, in_sem.at[i]) for i, (src, dst) in enumerate(
        ((hidden_hbm, hidden_ref), (gain_hbm, gain_ref), (pos_hbm, pos_ref), (post_hbm, post_ref),
         (kc_hbm, kc), (vc_hbm, vc)))]
    for copy in local:
        copy.start()
    for copy in local:
        copy.wait()
    prepare(pos_ref, hidden_ref, gain_ref, nrm, acc, rope)

    def to_owners(dist):
        zs = (tp + dist) % 4

        def message(when, row, rows, dest, first, block):
            dst = s1q.at[pl.ds(pl.multiple_of(first, rows), rows)]

            @pl.when(when)
            def _():
                exchange(dist == 0, s1a.at[zs, pl.ds(row, rows)], dst, dest, block, b_send, q_recv)

        y = tp % 4
        message(jnp.logical_not(last_x), 0, qrows, place(0, z, core), tp * qrows, h * 4 + zs)
        message(first_x, qrows, qrows, place(0, z, core), (4 + y) * qrows, 4 + zs)
        for i in range(2):
            message(jnp.logical_not(first_x), qrows + i * krows, krows, place(1, z, i),
                    core * 128 + tp * krows, h * 4 + zs)
            message(last_x, i * krows, krows, place(1, z, i), core * 128 + y * krows, zs)

    for dist in (0, 2, 1, 3):
        zs = (tp + dist) % 4
        came = s1a.at[zs]
        pltpu.make_async_copy(came, came, a_recv.at[(z + 4 - zs) % 4]).wait()
        to_owners(dist)

    def chunk(a, zs, gs, half):
        return gathered[a].at[zs, gs, pl.ds(half * halves[a], halves[a])]

    early = 128
    late = (gq.shape[2] - early) // 2

    def ring_chunk(a, xp, zs, half):
        if a == 0 and xp == 1:
            return gq.at[zs, gpar, pl.ds(early + half * late, late)]
        return chunk(a, zs, piece_g[xp], half)

    def early_rows(i, gs):
        return gq.at[piece_z[i], gs, pl.ds(0, early)]

    def xearly(i):
        c = early_rows(i, g)
        return remote(c, c, x_send.at[2], x_recv.at[1 + i], (place(1 - h, z, core), tp))

    def dearly(i):
        c = early_rows(i, gpar)
        return remote(c, c, d_send.at[0], d_recv.at[4 + i], (place(h, z, 1 - core), tp))

    def d2d(a, xp, s):
        if s < 2:
            c = chunk(a, z, piece_g[xp], s)
        else:
            c = ring_chunk(a, xp, piece_z[s // 2], s % 2)
        i = s // 2 + (8 if a else 4 * xp)
        return remote(c, c, d_send.at[a], d_recv.at[i], (place(h, z, 1 - core), tp))

    def d2d_piece_done(xp, i):
        settle(gq.at[piece_z[i], 0], d_recv.at[4 * xp + i])

    up = (place(h, zp, core), tp)
    down = (place(h, zm, core), tp)

    ring = {(1, 0): 0, (0, 0): 1, (0, 1): 2}

    def zcopy(a, xp, i):
        zs, half, to = ((z, 0, up), (z, 1, up), (z, 0, down), (z, 1, down), (zm, 0, up), (zp, 1, down))[i]
        c = ring_chunk(a, xp, zs, half)
        j = ring[a, xp]
        return remote(c, c, z_send.at[j], z_recv.at[j * 6 + i], to)

    def xcopy(a, s):
        c = chunk(a, piece_z[s // 2], g, s % 2)
        return remote(c, c, x_send.at[a], x_recv.at[a * 5 + s], (place(1 - h, z, core), tp))

    def arrived(a, xp, s):
        d2d(a, xp, s).start()

    def launch(a, xp):
        for i in (0, 3, 1, 2):
            zcopy(a, xp, i).start()
        arrived(a, xp, 0)
        arrived(a, xp, 1)

    def forward(a, xp):
        zcopy(a, xp, 0).wait_recv()
        zcopy(a, xp, 4).start()
        arrived(a, xp, 2)
        zcopy(a, xp, 3).wait_recv()
        zcopy(a, xp, 5).start()
        arrived(a, xp, 5)

    def take(a, xp):
        zcopy(a, xp, 1).wait_recv()
        arrived(a, xp, 3)
        zcopy(a, xp, 2).wait_recv()
        arrived(a, xp, 4)

    def finish(a, xp):
        zcopy(a, xp, 4).wait_recv()
        arrived(a, xp, 6)
        zcopy(a, xp, 5).wait_recv()
        arrived(a, xp, 7)

    pltpu.make_async_copy(s1o, s1o, o_recv).wait()
    nrow = s1o.shape[1]
    for i in range(32):
        so[i * nrow:(i + 1) * nrow, :] = s1o[i].astype(jnp.float32)
    for b in range(9):
        go[z, g, :, b * 128:(b + 1) * 128] = so[b * 128:(b + 1) * 128, :].T.astype(jnp.bfloat16)
    launch(1, 0)
    for s in range(2):
        xcopy(1, s).start()
    def slices_left(when, rows):
        @pl.when(when)
        def _():
            settle(s1q.at[pl.ds(0, rows)], b_send)

    ends = jnp.logical_or(first_x, last_x)
    slices_left(first_x, s1q.shape[0] - qrows)
    slices_left(last_x, s1q.shape[0] - krows)
    slices_left(jnp.logical_not(ends), s1q.shape[0])
    for i in range(1, 8):
        peer = (2 * h + lo + i // 2) % 4
        pl.semaphore_signal(
            row_sem, inc=1, device_id_type=MESH,
            device_id=(place(peer // 2, z, (core + i) % 2), (peer % 2) * 4 + tp % 4))
    forward(1, 0)
    pltpu.make_async_copy(s1q, s1q, q_recv).wait()
    for b in range(9):
        for c in range(2):
            tile = s1q[c * 128:(c + 1) * 128, b * 128:(b + 1) * 128].astype(jnp.float32)
            gq[z, g, b * 128:(b + 1) * 128, c * 128:(c + 1) * 128] = tile.T.astype(jnp.bfloat16)
    launch(0, 0)
    pl.semaphore_wait(row_sem, 7)
    for s in range(2):
        xcopy(0, s).start()
    take(1, 0)
    for s in (2, 5, 3, 4):
        xcopy(1, s).start()
    forward(0, 0)
    take(0, 0)
    for i in (1, 2):
        xearly(i).start()
    for s in range(2):
        xcopy(0, s).wait_recv()
    launch(0, 1)
    finish(1, 0)
    finish(0, 0)
    xearly(3).start()
    for s in (6, 7):
        xcopy(1, s).start()

    def project(xp, i):
        def add(gs):
            acc[gs] += jnp.dot(nrm[piece_z[i]], gq[piece_z[i], gs], preferred_element_type=jnp.float32)

        add(piece_g[xp])
        d2d_piece_done(xp, i)
        add(piece_g[xp] + 1 - 2 * core)

    for i in range(4):
        project(0, i)
    forward(0, 1)
    take(0, 1)
    project(1, 0)
    for s in (0, 1, 2, 5, 3, 4):
        xcopy(1, s).wait_recv()
        d2d(1, 1, s).start()
    for i in (1, 2):
        xearly(i).wait_recv()
        dearly(i).start()
    project(1, 1)
    project(1, 2)
    xearly(3).wait_recv()
    dearly(3).start()
    finish(0, 1)
    project(1, 3)
    for s in (6, 7):
        xcopy(1, s).wait_recv()
        d2d(1, 1, s).start()
    att = attention(pos_ref, kc, vc, acc, rope)
    def part_slices(i):
        zs = piece_z[i]
        j = jnp.where(zs == 0, 0, jnp.where(zs == 3, 1, zs + 1))
        return pl.ds(2 * j, 2)

    def part(i, d):
        return remote(part_ref.at[part_slices(i)], parts_in.at[d - 1, part_slices(i)],
                      p_send, p_recv, (rep, (tp + d) % 8))

    for i in range(4):
        settle(go.at[piece_z[i], pl.ds(0, 2)], d_recv.at[8 + i])
        both = jnp.dot(att, go[piece_z[i]].reshape(512, 1152), preferred_element_type=jnp.float32)
        both = both.astype(jnp.bfloat16)
        first = part_slices(i).start
        part_ref[first] = both[:, :576]
        part_ref[first + 1] = both[:, 576:]
        for d in (6, 2, 5, 7, 1, 3, 4):
            part(i, d).start()
    settle(parts_in, p_recv)
    sum_and_norm(part_ref, post_ref, out_ref, parts_in)
    settle(parts_in, p_send)
    settle(s1a.at[pl.ds(0, 3)], a_send.at[1])

    @pl.when(ends)
    def _():
        settle(s1a.at[0, pl.ds(0, qrows)], a_send.at[0])

    @pl.when(zdest == z)
    def _():
        settle(s1o.at[pl.ds(0, 31)], o_send)

    @pl.when(zdest != z)
    def _():
        settle(s1o, o_send)

    settle(go.at[0, pl.ds(0, 3)], z_send.at[0])
    settle(gq.at[0, pl.ds(0, 3)], z_send.at[1])
    settle(gq.at[0, pl.ds(0, 3), pl.ds(0, 2 * late)], z_send.at[2])
    settle(gq.at[0, 0], x_send.at[0])
    settle(go.at[0], x_send.at[1])
    settle(gq.at[0, pl.ds(0, 3), pl.ds(0, early)], x_send.at[2])
    for i in range(2):
        settle(gathered[i].at[pl.ds(0, 2)], d_send.at[i])


def in_hbm(x):
    return pltpu.with_memory_space_constraint(x, pltpu.HBM)


def gather_and_attend(q, k, v, o, hidden, gain, key_cache, value_cache, positions, post_gain):
    bf, f32 = jnp.bfloat16, jnp.float32
    dma = pltpu.SemaphoreType.DMA
    vmem = pltpu.VMEM
    return pl.pallas_call(
        gather_kernel,
        out_shape=(jax.ShapeDtypeStruct((4, 4, 1152, 256), bf),
                   jax.ShapeDtypeStruct((4, 4, 128, 1152), bf),
                   jax.ShapeDtypeStruct((4, 576), bf)),
        in_specs=[pl.BlockSpec(memory_space=pltpu.HBM)] * 10,
        out_specs=[pl.BlockSpec(memory_space=vmem)] * 3,
        scratch_shapes=[
            vmem(hidden.shape, bf), vmem(gain.shape, f32), vmem(key_cache.shape, bf),
            vmem(value_cache.shape, bf), pltpu.SMEM((4,), jnp.int32), vmem(post_gain.shape, f32),
            vmem((4, 4, 1152), bf), vmem((4, 4, 256), f32), vmem((2, 4, 128), f32),
            vmem((8, 4, 576), bf), vmem((7, 8, 4, 576), bf),
            vmem((4, 64, 1152), bf), vmem((256, 1152), bf), vmem((32, 36, 128), bf),
            vmem((1152, 128), f32),
            dma((2,)), dma((4,)), dma, dma, dma, dma, dma((3,)), dma((18,)), dma((3,)), dma((13,)),
            dma((2,)), dma((12,)), pltpu.SemaphoreType.REGULAR, dma((6,)), dma, dma,
        ],
        compiler_params=pltpu.CompilerParams(
            has_side_effects=True, collective_id=0, vmem_limit_bytes=16 * 1024 * 1024),
        name="gather_and_attend",
    )(*(in_hbm(x) for x in (q, k, v, o, hidden, gain, key_cache, value_cache, positions, post_gain)))


def prepare(pos_ref, hidden_ref, gain_ref, nrm, acc, rope):
    f32 = jnp.float32
    hid = hidden_ref[...].astype(f32)
    mean_square = jnp.mean(hid * hid, axis=-1, keepdims=True)
    gain = gain_ref[...].reshape(1, -1)
    normed = (hid * lax.rsqrt(mean_square + 1e-06) * gain).astype(jnp.bfloat16)
    for zs in range(4):
        nrm[zs] = normed[:, zs * 1152:(zs + 1) * 1152]
    acc[...] = jnp.zeros_like(acc)
    row = lax.broadcasted_iota(jnp.int32, (4, 128), 0)
    posf = jnp.zeros((4, 128), f32)
    for b in range(4):
        posf = jnp.where(row == b, pos_ref[b].astype(f32), posf)
    lane = lax.broadcasted_iota(jnp.int32, (4, 128), 1)
    angle = posf * jnp.exp((lane % 64).astype(f32) * (-2.0 / 128 * np.log(10000.0)))
    rope[0] = jnp.cos(angle)
    rope[1] = jnp.where(lane < 64, -jnp.sin(angle), jnp.sin(angle))


def attention(pos_ref, kc, vc, acc, rope):
    f32, bf = jnp.float32, jnp.bfloat16
    proj = []
    for gs in range(4):
        both = acc[gs]
        proj += [both[:, :128], both[:, 128:]]
    cosine, sine = rope[0], rope[1]

    def rotate(x):
        swapped = jnp.concatenate([x[:, 64:], x[:, :64]], axis=1)
        return (x * cosine + swapped * sine).astype(bf).astype(f32)

    query = jnp.concatenate([rotate(x) for x in proj[:4]], axis=0)
    keys = [rotate(x) for x in proj[4:6]]
    vals = [x.astype(bf).astype(f32) for x in proj[6:8]]
    keys_new = jnp.concatenate([keys[0], keys[0], keys[1], keys[1]], axis=0)
    values_new = jnp.concatenate([vals[0], vals[0], vals[1], vals[1]], axis=0)
    qb = query.astype(bf)
    length = kc.shape[2]
    r = lax.broadcasted_iota(jnp.int32, (16, length), 0)
    slot = lax.broadcasted_iota(jnp.int32, (16, length), 1)
    owner = (r // 8) * 4 + r % 4
    scores = jnp.zeros((16, length), f32)
    limit = jnp.zeros((16, length), jnp.int32)
    for kv in range(2):
        for b in range(4):
            s = lax.dot_general(qb, kc[b, kv], (((1,), (1,)), ((), ())), preferred_element_type=f32)
            scores = jnp.where(owner == kv * 4 + b, s, scores)
    for b in range(4):
        limit = jnp.where(r % 4 == b, pos_ref[b], limit)
    capped = soft_cap * jnp.tanh(scores * score_scale / soft_cap)
    raw = jnp.where(slot < limit, jnp.exp(capped), 0.0)
    self_score = jnp.sum(query * keys_new, axis=-1, keepdims=True) * score_scale
    self_raw = jnp.exp(soft_cap * jnp.tanh(self_score / soft_cap))
    denom = jnp.sum(raw, axis=-1, keepdims=True) + self_raw
    weights = (raw / denom).astype(bf).astype(f32)
    mixed = (self_raw / denom).astype(bf).astype(f32) * values_new
    for kv in range(2):
        for b in range(4):
            w = jnp.where(owner == kv * 4 + b, weights, 0.0).astype(bf)
            mixed += jnp.dot(w, vc[b, kv], preferred_element_type=f32)
    return jnp.concatenate([mixed[i * 4:(i + 1) * 4] for i in range(4)], axis=1).astype(bf)


def write_kernel(gq, go, small, joined_ref, wo_ref, small_ref, out_sem):
    pltpu.make_async_copy(small, small_ref, out_sem.at[2]).start()
    for zs in range(4):
        for gs in range(4):
            pltpu.make_async_copy(
                gq.at[zs, gs], joined_ref.at[pl.ds(zs * 1152, 1152), pl.ds(gs * 256, 256)],
                out_sem.at[0]).start()
            pltpu.make_async_copy(
                go.at[zs, gs], wo_ref.at[pl.ds(gs * 128, 128), pl.ds(WO_SLICE[zs] * 1152, 1152)],
                out_sem.at[1]).start()
    pltpu.make_async_copy(joined_ref, joined_ref, out_sem.at[0]).wait()
    pltpu.make_async_copy(wo_ref, wo_ref, out_sem.at[1]).wait()
    pltpu.make_async_copy(small, small_ref, out_sem.at[2]).wait()


def write_out(gq, go, small):
    bf = jnp.bfloat16
    vmem = pl.BlockSpec(memory_space=pltpu.VMEM)
    hbm = pl.BlockSpec(memory_space=pltpu.HBM)
    return pl.pallas_call(
        write_kernel,
        out_shape=(jax.ShapeDtypeStruct((4608, 1024), bf), jax.ShapeDtypeStruct((512, 4608), bf),
                   jax.ShapeDtypeStruct(small.shape, bf)),
        in_specs=[vmem, vmem, vmem],
        out_specs=[hbm, hbm, hbm],
        scratch_shapes=[pltpu.SemaphoreType.DMA((3,))],
        compiler_params=pltpu.CompilerParams(vmem_limit_bytes=16 * 1024 * 1024),
        name="write_out",
    )(gq, go, small)


def sum_and_norm(part_ref, gain_ref, out_ref, parts_in):
    f32 = jnp.float32
    tp = lax.axis_index("tp")
    total = part_ref[...].astype(f32)
    own = part_ref[tp].astype(f32)
    for d in range(7):
        total += parts_in[d].astype(f32)
        own += parts_in[d, tp].astype(f32)
    square = jnp.sum(jnp.sum(total * total, axis=0), axis=-1, keepdims=True)
    scale = lax.rsqrt(square / 4608.0 + 1e-06)
    out_ref[...] = (own * scale * gain_ref[...].reshape(1, -1)).astype(jnp.bfloat16)


def body(
    hidden, positions, key_cache, value_cache, norm_gain, q_proj, k_proj, v_proj, o_proj, post_gain
):
    gq, go, attn_out = gather_and_attend(
        q_proj, k_proj, v_proj, o_proj, hidden, norm_gain, key_cache, value_cache, positions, post_gain)
    return write_out(gq, go, attn_out)


def solution(mesh):
    in_specs = (
        P("rep", None),
        P("rep"),
        P("rep", "tp", None, None),
        P("rep", "tp", None, None),
        P(),
        P(("rep", "tp"), None),
        P(("rep", "tp"), None),
        P(("rep", "tp"), None),
        P(("rep", "tp"), None),
        P("tp"),
    )
    out_specs = (P(None, "tp"), P("tp", None), P("rep", "tp"))
    return jax.shard_map(body, mesh=mesh, in_specs=in_specs, out_specs=out_specs, check_vma=False)
```
